128 devices in a mesh: dp: 128 (over x, z, y, core).
Axes of the slice: x: 4, y: 4, z: 4, core: 2. Of those that a mesh axis runs over, the one named last changes fastest.
Arguments:
- token_ids: int32 [131072], P('dp'), may hold values from 0 to 31999, as said below
- tokens: bfloat16 [131072, 4096], P('dp'), may hold values from -64 to 64
- frozen_weight: bfloat16 [4096, 1024], replicated, may hold values from -0.09375 to 0.09375
- adapter_down: bfloat16 [4096, 128], replicated, may hold values from -0.09375 to 0.09375
- adapter_up: bfloat16 [128, 1024], replicated, may hold values from -1.5 to 1.5
- gate_weight: bfloat16 [4096, 8], replicated, may hold values from -1 to 1
- upstream: bfloat16 [131072, 1024], P('dp'), may hold values from -6 to 6
Outputs:
- projected: bfloat16 [131072, 1024], P('dp')
- input_grad: bfloat16 [131072, 4096], P('dp')
- clipped_down: float32 [4096, 128], replicated
- clipped_up: float32 [128, 1024], replicated
- clipped_gate: float32 [4096, 8], replicated
- load: float32 [8], replicated
- entropy: float32 [], replicated
The draws below stay inside these ranges and needn't reach their ends.
Inputs may be any that keep to these rules, and one draw needn't show every extreme that they name: `token_ids`: within each device's block of 1024 tokens the live tokens (id not 0) come first, 256 or more of them, and padding (id 0) fills the rest; the last block is wholly live.
All inputs are finite; a program needn't handle non-finite values.
Results may differ from the reference program's by a relative error of at most 0.0095.
Values sent between devices are 32-bit elements; how exact they have to be, the bound alone decides.
A program may use at most 192 MiB of HBM per device.

```python
import math
import jax
import jax.numpy as jnp
from jax import lax

D = 4096
DOUT = 1024
EXPERTS = 8
RANK = 16
VOCAB = 32000
TOK_DEV = 1024
TOKENS = 131072


def gate_table(key):
    return jax.random.normal(jax.random.fold_in(key, 7), (D, EXPERTS), jnp.float32) * (2.0 / math.sqrt(D))


def draw_gate_weight(key, part):
    return jnp.clip(gate_table(key), -1.0, 1.0).astype(jnp.bfloat16)


def draw_tokens(key, part):
    base_key = jax.random.fold_in(key, 11)
    noise = jax.random.normal(jax.random.fold_in(base_key, 1), (TOKENS, D), jnp.float32)
    scales = jnp.exp(jax.random.uniform(jax.random.fold_in(base_key, 2), (TOKENS, 1), jnp.float32, -math.log(2.0), math.log(2.0)))
    rows = noise * scales
    return jnp.clip(rows, -64.0, 64.0).astype(jnp.bfloat16)


def draw_token_ids(key, part):
    blocks = TOKENS // TOK_DEV
    block_ids = jnp.arange(blocks, dtype=jnp.int32)
    lowest = TOK_DEV // 4
    rising = (TOK_DEV - lowest) * block_ids // max(blocks - 1, 1)
    jitter = jax.random.randint(jax.random.fold_in(key, 21), (blocks,), 0, TOK_DEV // 8 + 1, dtype=jnp.int32)
    length = jnp.clip(lowest + rising - jitter, lowest, TOK_DEV)
    length = length.at[blocks - 1].set(TOK_DEV)
    position = jnp.arange(TOK_DEV, dtype=jnp.int32)
    alive = position[None, :] < length[:, None]
    values = jax.random.randint(jax.random.fold_in(key, 22), (blocks, TOK_DEV), 1, VOCAB, dtype=jnp.int32)
    return jnp.where(alive, values, 0).reshape(TOKENS).astype(jnp.int32)


def level_of(rng, dims, shards, smallest, high):
    level = 1.0
    for axis_at, shards_of in shards:
        steps = jax.random.uniform(jax.random.fold_in(jax.random.fold_in(rng, 6), axis_at), (shards_of,), jnp.float32, smallest / len(shards), high / len(shards))
        level = level * jnp.repeat(jnp.exp(steps), dims[axis_at] // shards_of).reshape((-1,) + (1,) * (len(dims) - 1 - axis_at))
    return level


def normal_values(stream_key, extent, scale, most, cuts=(), kind=jnp.bfloat16):
    values = jax.random.normal(stream_key, extent, jnp.float32) * scale
    if len(cuts) > 0:
        values = level_of(stream_key, extent, cuts, -0.22, 0.18) * values
    return jnp.clip(values, min=-most, max=most).astype(kind)


def setup_inputs(seed: int = 0) -> dict:
    streams_of = jax.random.split(jax.random.key(seed), 8)
    token_ids = draw_token_ids(jax.random.fold_in(streams_of[7], 71), 0)
    tokens = draw_tokens(jax.random.fold_in(streams_of[7], 71), 0)
    frozen_weight = normal_values(streams_of[2], (D, DOUT), D ** -0.5, 0.09375)
    adapter_down = normal_values(streams_of[3], (D, EXPERTS * RANK), D ** -0.5, 0.09375)
    adapter_up = normal_values(streams_of[4], (EXPERTS * RANK, DOUT), RANK ** -0.5, 1.5)
    gate_weight = draw_gate_weight(jax.random.fold_in(streams_of[7], 71), 0)
    upstream = normal_values(streams_of[6], (TOKENS, DOUT), 1.0, 6.0, ((0, 128),))
    return dict(token_ids=token_ids, tokens=tokens, frozen_weight=frozen_weight, adapter_down=adapter_down, adapter_up=adapter_up, gate_weight=gate_weight, upstream=upstream)


def reference(token_ids, tokens, frozen_weight, adapter_down, adapter_up, gate_weight, upstream):
    live = (token_ids != 0).astype(jnp.float32)
    base = jnp.dot(tokens, frozen_weight, preferred_element_type=jnp.float32)
    logits = jnp.dot(tokens, gate_weight, preferred_element_type=jnp.float32)
    prob = jax.nn.softmax(logits, axis=1)
    logp = jax.nn.log_softmax(logits, axis=1)
    low = jnp.dot(tokens, adapter_down, preferred_element_type=jnp.float32).astype(jnp.bfloat16)
    spread = jnp.repeat(prob, RANK, axis=1)
    weighted = (low.astype(jnp.float32) * spread).astype(jnp.bfloat16)
    projected = (base + 2.0 * jnp.dot(weighted, adapter_up, preferred_element_type=jnp.float32)).astype(jnp.bfloat16)
    masked = upstream * live.astype(jnp.bfloat16)[:, None]
    grad_up = 2.0 * jnp.dot(weighted.T, masked, preferred_element_type=jnp.float32)
    back = jnp.dot(masked, adapter_up.T, preferred_element_type=jnp.float32)
    gate_task = 2.0 * lax.optimization_barrier(jnp.sum((low.astype(jnp.float32) * back).reshape(-1, EXPERTS, RANK), axis=2))
    low_grad = (2.0 * spread * back).astype(jnp.bfloat16)
    grad_down = jnp.dot(tokens.T, low_grad, preferred_element_type=jnp.float32)
    ent_tok = -lax.optimization_barrier(jnp.sum(prob * logp, axis=1))
    load_sum = lax.optimization_barrier(jnp.sum(live[:, None] * prob, axis=0))
    ent_sum = jnp.sum(live * ent_tok)
    live_sum = jnp.sum(live)

    def jac(v):
        return prob * (v - lax.optimization_barrier(jnp.sum(prob * v, axis=1, keepdims=True)))
    gate_z = jac(gate_task) + 50.0 * live[:, None] * prob * (logp + ent_tok[:, None])
    gate_z = gate_z + 2.0 * EXPERTS * 100.0 / live_sum * live[:, None] * jac(load_sum[None, :])
    grad_gate = jnp.dot(tokens.astype(jnp.float32).T, gate_z, precision=lax.Precision.HIGHEST)
    input_grad = jnp.dot(masked, frozen_weight.T, preferred_element_type=jnp.float32)
    input_grad = input_grad + jnp.dot(low_grad, adapter_down.T, preferred_element_type=jnp.float32)
    input_grad = input_grad + jnp.dot(gate_z, gate_weight.astype(jnp.float32).T, precision=lax.Precision.HIGHEST)
    total = jnp.sum(grad_down * grad_down) + jnp.sum(grad_up * grad_up) + jnp.sum(grad_gate * grad_gate)
    count = D * EXPERTS * RANK + EXPERTS * RANK * DOUT + D * EXPERTS
    clip = jnp.minimum(1.0, math.sqrt(count) / jnp.sqrt(total))
    return (projected, input_grad.astype(jnp.bfloat16), grad_down * clip, grad_up * clip, grad_gate * clip, load_sum / live_sum, ent_sum / live_sum)
```

```python
import functools
import math

import jax
import jax.numpy as jnp
from jax import lax
from jax.experimental import pallas as pl
from jax.experimental.pallas import tpu as pltpu
from jax.sharding import Mesh
from jax.sharding import PartitionSpec as P

AXES = ("dp_0", "dp_1", "dp_2")
CORE = "dp_3"
DP = AXES + (CORE,)
MESH = pl.DeviceIdType.MESH
SIDE = 4
COLOURS = 3
LANES = 128


def left_dot(first, second):
    return lax.dot_general(
        first, second, (((0,), (0,)), ((), ())), preferred_element_type=jnp.float32
    )


def right_dot(first, second):
    return lax.dot_general(
        first, second, (((1,), (1,)), ((), ())), preferred_element_type=jnp.float32
    )


def exact_left(tokens, matrix):
    upper = matrix.astype(jnp.bfloat16)
    lower = (matrix - upper.astype(jnp.float32)).astype(jnp.bfloat16)
    return left_dot(tokens, upper) + left_dot(tokens, lower)


def ring_peer(axis, distance):
    return {axis: lax.rem(lax.axis_index(axis) + distance, SIDE)}


class Exchange:
    def __init__(self, rows, part, total, halves, firsts, seconds, thirds, send, recv):
        self.part, self.total = part, total
        self.halves, self.firsts, self.seconds, self.thirds = halves, firsts, seconds, thirds
        self.send, self.recv = send, recv
        self.colour_rows = rows // COLOURS
        self.half = self.colour_rows // 2
        self.quarter = self.half // SIDE
        self.last = self.quarter // SIDE
        self.core = lax.axis_index(CORE)

    def order(self, colour):
        return tuple(AXES[(colour + step) % 3] for step in range(3))

    def half_at(self, colour, core):
        return colour * self.colour_rows + core * self.half

    def quarter_at(self, colour, place):
        return self.half_at(colour, self.core) + place * self.quarter

    def last_at(self, colour, place, second):
        return self.quarter_at(colour, place) + second * self.last

    def copy(self, source, target, phase, colour, slot, device):
        return pltpu.make_async_remote_copy(
            src_ref=source,
            dst_ref=target,
            send_sem=self.send.at[phase, colour, slot],
            recv_sem=self.recv.at[phase, colour, slot],
            device_id=device,
            device_id_type=MESH,
        )

    def rows_of(self, ref, start, size):
        return ref.at[pl.ds(pl.multiple_of(start, 8), size)]

    def copies(self, phase, colour):
        first, second, third = self.order(colour)
        one, two = lax.axis_index(first), lax.axis_index(second)
        made = []
        if phase == 0:
            source = self.rows_of(self.part, self.half_at(colour, 1 - self.core), self.half)
            made.append(self.copy(source, self.halves.at[colour], 0, colour, 0, {CORE: 1 - self.core}))
        elif phase == 6:
            here = self.half_at(colour, self.core)
            made.append(
                self.copy(
                    self.rows_of(self.total, here, self.half),
                    self.rows_of(self.total, here, self.half),
                    6, colour, 0, {CORE: 1 - self.core},
                )
            )
        else:
            for distance in (1, 2, 3):
                slot = distance - 1
                if phase == 1:
                    place = lax.rem(one + distance, SIDE)
                    source = self.rows_of(self.part, self.quarter_at(colour, place), self.quarter)
                    target, axis = self.firsts.at[colour, slot], first
                elif phase == 2:
                    place = lax.rem(two + distance, SIDE)
                    source = self.rows_of(self.part, self.last_at(colour, one, place), self.last)
                    target, axis = self.seconds.at[colour, slot], second
                elif phase == 3:
                    source = self.rows_of(self.part, self.last_at(colour, one, two), self.last)
                    target, axis = self.thirds.at[colour, lax.axis_index(third)], third
                elif phase == 4:
                    source = self.rows_of(self.total, self.last_at(colour, one, two), self.last)
                    target, axis = source, second
                else:
                    source = self.rows_of(self.total, self.quarter_at(colour, one), self.quarter)
                    target, axis = source, first
                made.append(self.copy(source, target, phase, colour, slot, ring_peer(axis, distance)))
        return made

    def start(self, phase, colour):
        for copy in self.copies(phase, colour):
            copy.start()

    def finish(self, phase, colour):
        for copy in self.copies(phase, colour):
            copy.wait()
        first, second, third = self.order(colour)
        one, two = lax.axis_index(first), lax.axis_index(second)
        if phase == 0:
            here = pl.ds(pl.multiple_of(self.half_at(colour, self.core), 8), self.half)
            self.part[here] = self.part[here] + self.halves[colour]
        elif phase == 1:
            here = pl.ds(pl.multiple_of(self.quarter_at(colour, one), 8), self.quarter)
            got = self.firsts
            self.part[here] = self.part[here] + got[colour, 0] + got[colour, 1] + got[colour, 2]
        elif phase == 2:
            here = pl.ds(pl.multiple_of(self.last_at(colour, one, two), 8), self.last)
            got = self.seconds
            mine = self.part[here] + got[colour, 0] + got[colour, 1] + got[colour, 2]
            self.part[here] = mine
        elif phase == 3:
            here = pl.ds(pl.multiple_of(self.last_at(colour, one, two), 8), self.last)
            got = self.thirds
            got[colour, lax.axis_index(third)] = self.part[here]
            self.total[here] = (got[colour, 0] + got[colour, 1]) + (got[colour, 2] + got[colour, 3])

    def greet(self):
        barrier = pltpu.get_barrier_semaphore()
        peers = [{CORE: 1 - self.core}]
        peers += [ring_peer(axis, distance) for axis in AXES for distance in (1, 2, 3)]
        for peer in peers:
            pl.semaphore_signal(barrier, inc=1, device_id=peer, device_id_type=MESH)
        pl.semaphore_wait(barrier, len(peers))


def reduce_kernel(limit, down_rows, up_blocks, gate_rows, part_ref, down_ref, up_ref, gate_ref, part, total, halves, firsts, seconds, thirds, send, recv):
    rows = part.shape[0]
    part[...] = part_ref[...]
    exchange = Exchange(rows, part, total, halves, firsts, seconds, thirds, send, recv)
    exchange.greet()
    for colour in range(COLOURS):
        exchange.start(0, colour)
    for phase in range(7):
        for colour in range(COLOURS):
            exchange.finish(phase, colour)
            if phase < 6:
                exchange.start(phase + 1, colour)
    values = total[...]
    norm = jnp.sum(values * values)
    factor = jnp.minimum(1.0, limit / jnp.sqrt(jnp.full((8, LANES), norm, jnp.float32)))[0:1]
    down_ref[...] = total[0:down_rows] * factor
    for block in range(up_blocks):
        here = down_rows + block * LANES
        up_ref[:, block * LANES : (block + 1) * LANES] = total[here : here + LANES] * factor
    base = down_rows + up_blocks * LANES
    for block in range(gate_rows // 8):
        here = base + block * 8
        gate_ref[:, block * LANES : (block + 1) * LANES] = total[here : here + 8] * factor


def reduce_clip(down, up, gate, limit):
    experts = gate.shape[1]
    wide = lambda m: m.reshape(m.shape[0], -1, LANES).transpose(1, 0, 2).reshape(-1, LANES)
    part = jnp.concatenate([down, wide(up), wide(gate.T)], axis=0)
    rows = part.shape[0]
    half = rows // COLOURS // 2
    vmem = pl.BlockSpec(memory_space=pltpu.VMEM)
    clipped = pl.pallas_call(
        functools.partial(
            reduce_kernel, limit, down.shape[0], up.shape[1] // LANES, gate.shape[0] * experts // LANES
        ),
        out_shape=(
            jax.ShapeDtypeStruct(down.shape, jnp.float32),
            jax.ShapeDtypeStruct(up.shape, jnp.float32),
            jax.ShapeDtypeStruct((experts, gate.shape[0]), jnp.float32),
        ),
        in_specs=[vmem],
        out_specs=(vmem, vmem, vmem),
        scratch_shapes=[
            pltpu.VMEM((rows, LANES), jnp.float32),
            pltpu.VMEM((rows, LANES), jnp.float32),
            pltpu.VMEM((COLOURS, half, LANES), jnp.float32),
            pltpu.VMEM((COLOURS, 3, half // 4, LANES), jnp.float32),
            pltpu.VMEM((COLOURS, 3, half // 16, LANES), jnp.float32),
            pltpu.VMEM((COLOURS, 4, half // 16, LANES), jnp.float32),
            pltpu.SemaphoreType.DMA((7, COLOURS, 3)),
            pltpu.SemaphoreType.DMA((7, COLOURS, 3)),
        ],
        compiler_params=pltpu.CompilerParams(collective_id=0, has_side_effects=True),
        name="reduce_clip",
    )(part)
    return clipped[0], clipped[1], clipped[2].T


def on_device(token_ids, tokens, frozen_weight, adapter_down, adapter_up, gate_weight, upstream):
    width = tokens.shape[1]
    experts = gate_weight.shape[1]
    ranks = adapter_down.shape[1]
    rank = ranks // experts
    outputs = frozen_weight.shape[1]
    rows = tokens.shape[0]
    live = (token_ids != 0).astype(jnp.float32)
    base = jnp.dot(tokens, frozen_weight, preferred_element_type=jnp.float32)
    logits = jnp.dot(tokens, gate_weight, preferred_element_type=jnp.float32)
    prob = jax.nn.softmax(logits, axis=1)
    logp = jax.nn.log_softmax(logits, axis=1)
    low = jnp.dot(tokens, adapter_down, preferred_element_type=jnp.float32).astype(jnp.bfloat16)
    spread = jnp.repeat(prob, rank, axis=1)
    weighted = (low.astype(jnp.float32) * spread).astype(jnp.bfloat16)
    projected = (
        base + 2.0 * jnp.dot(weighted, adapter_up, preferred_element_type=jnp.float32)
    ).astype(jnp.bfloat16)
    masked = upstream * live.astype(jnp.bfloat16)[:, None]
    grad_up = 2.0 * left_dot(weighted, masked)
    back = right_dot(masked, adapter_up)
    gate_task = 2.0 * jnp.sum((low.astype(jnp.float32) * back).reshape(rows, experts, rank), axis=2)
    low_grad = (2.0 * spread * back).astype(jnp.bfloat16)
    grad_down = left_dot(tokens, low_grad)
    ent_tok = -jnp.sum(prob * logp, axis=1)
    local_stats = jnp.concatenate(
        [jnp.sum(live[:, None] * prob, axis=0), jnp.stack([jnp.sum(live * ent_tok), jnp.sum(live)])]
    )

    def jac(vector):
        return prob * (vector - jnp.sum(prob * vector, axis=1, keepdims=True))

    plain_z = jac(gate_task) + 50.0 * live[:, None] * prob * (logp + ent_tok[:, None])
    frozen_back = right_dot(masked, frozen_weight) + right_dot(low_grad, adapter_down)
    count = width * ranks + ranks * outputs + width * experts
    limit = math.sqrt(count)
    stats = lax.psum(local_stats, DP)
    load_all, ent_all, live_all = stats[:experts], stats[experts], stats[experts + 1]
    gate_z = plain_z + 2.0 * experts * 100.0 / live_all * live[:, None] * jac(load_all[None, :])
    clipped = reduce_clip(grad_down, grad_up, exact_left(tokens, gate_z), limit)
    input_grad = frozen_back + jnp.dot(
        gate_z, gate_weight.astype(jnp.float32).T, precision=lax.Precision.HIGHEST
    )
    return (
        projected,
        input_grad.astype(jnp.bfloat16),
        clipped[0],
        clipped[1],
        clipped[2],
        load_all / live_all,
        ent_all / live_all,
    )


def solution(mesh):
    torus = Mesh(mesh.devices.reshape(4, 4, 4, 2), DP)
    return jax.shard_map(
        on_device,
        mesh=torus,
        in_specs=(P(DP), P(DP, None), P(), P(), P(), P(), P(DP, None)),
        out_specs=(P(DP, None), P(DP, None), P(), P(), P(), P(), P()),
        check_vma=False,
    )
```

```python
import functools
import math

import jax
import jax.numpy as jnp
from jax import lax
from jax.experimental import pallas as pl
from jax.experimental.pallas import tpu as pltpu
from jax.sharding import Mesh
from jax.sharding import PartitionSpec as P

AXES = ("dp_0", "dp_1", "dp_2")
CORE = "dp_3"
DP = AXES + (CORE,)
MESH = pl.DeviceIdType.MESH
SIDE = 4
LANES = 128
CHUNK = 256
BF16 = jnp.bfloat16
F32 = jnp.float32


def dot(first, second):
    return jnp.dot(first, second, preferred_element_type=F32)


def right_dot(first, second):
    return lax.dot_general(first, second, (((1,), (1,)), ((), ())), preferred_element_type=F32)


def ring_peer(axis, distance):
    return {axis: lax.rem(lax.axis_index(axis) + distance, SIDE)}


def span(start, size, unit=8):
    return pl.ds(pl.multiple_of(start, unit), size)


class Piece:
    def __init__(self, index, base, rows):
        self.index, self.base, self.rows = index, base, rows
        self.half, self.quarter, self.last = rows // 2, rows // 8, rows // 32
        self.first, self.second, self.third = (AXES[(index + step) % 3] for step in range(3))


class Exchange:
    def __init__(self, part, total, halves, firsts, seconds, thirds, send, recv):
        self.part, self.total = part, total
        self.halves, self.firsts, self.seconds, self.thirds = halves, firsts, seconds, thirds
        self.send, self.recv = send, recv
        self.core = lax.axis_index(CORE)

    def half_at(self, piece, core):
        return piece.base + core * piece.half

    def quarter_at(self, piece, place):
        return self.half_at(piece, self.core) + place * piece.quarter

    def last_at(self, piece, place, second):
        return self.quarter_at(piece, place) + second * piece.last

    def copies(self, phase, piece):
        one, two = lax.axis_index(piece.first), lax.axis_index(piece.second)

        def copy(source, target, slot, device):
            return pltpu.make_async_remote_copy(
                src_ref=source,
                dst_ref=target,
                send_sem=self.send.at[phase, piece.index, slot],
                recv_sem=self.recv.at[phase, piece.index, slot],
                device_id=device,
                device_id_type=MESH,
            )

        if phase == 0:
            source = self.part.at[span(self.half_at(piece, 1 - self.core), piece.half)]
            target = self.halves.at[pl.ds(piece.base // 2, piece.half)]
            return [copy(source, target, 0, {CORE: 1 - self.core})]
        if phase == 6:
            here = self.total.at[span(self.half_at(piece, self.core), piece.half)]
            return [copy(here, here, 0, {CORE: 1 - self.core})]
        made = []
        for distance in (1, 2, 3):
            slot = distance - 1
            if phase == 1:
                place = lax.rem(one + distance, SIDE)
                source = self.part.at[span(self.quarter_at(piece, place), piece.quarter)]
                target = self.firsts.at[slot, pl.ds(piece.base // 8, piece.quarter)]
                axis = piece.first
            elif phase == 2:
                place = lax.rem(two + distance, SIDE)
                source = self.part.at[span(self.last_at(piece, one, place), piece.last)]
                target = self.seconds.at[slot, pl.ds(piece.base // 32, piece.last)]
                axis = piece.second
            elif phase == 3:
                source = self.part.at[span(self.last_at(piece, one, two), piece.last)]
                target = self.thirds.at[lax.axis_index(piece.third), pl.ds(piece.base // 32, piece.last)]
                axis = piece.third
            elif phase == 4:
                source = self.total.at[span(self.last_at(piece, one, two), piece.last)]
                target, axis = source, piece.second
            else:
                source = self.total.at[span(self.quarter_at(piece, one), piece.quarter)]
                target, axis = source, piece.first
            made.append(copy(source, target, slot, ring_peer(axis, distance)))
        return made

    def start(self, phase, piece):
        for copy in self.copies(phase, piece):
            copy.start()

    def finish(self, phase, piece):
        for copy in self.copies(phase, piece):
            copy.wait()
        one, two = lax.axis_index(piece.first), lax.axis_index(piece.second)
        if phase == 0:
            here = span(self.half_at(piece, self.core), piece.half)
            self.part[here] = self.part[here] + self.halves[pl.ds(piece.base // 2, piece.half)]
        elif phase == 1:
            here = span(self.quarter_at(piece, one), piece.quarter)
            there = pl.ds(piece.base // 8, piece.quarter)
            got = self.firsts
            self.part[here] = (self.part[here] + got[0, there]) + (got[1, there] + got[2, there])
        elif phase == 2:
            here = span(self.last_at(piece, one, two), piece.last)
            there = pl.ds(piece.base // 32, piece.last)
            got = self.seconds
            self.part[here] = (self.part[here] + got[0, there]) + (got[1, there] + got[2, there])
        elif phase == 3:
            here = span(self.last_at(piece, one, two), piece.last)
            there = pl.ds(piece.base // 32, piece.last)
            got = self.thirds
            got[lax.axis_index(piece.third), there] = self.part[here]
            self.total[here] = (got[0, there] + got[1, there]) + (got[2, there] + got[3, there])

    def step(self, phase, piece):
        self.finish(phase, piece)
        self.start(phase + 1, piece)


class Statistics:
    def __init__(self, tiles, wide, narrow, send, recv):
        self.tiles, self.wide, self.narrow = tiles, wide, narrow
        self.send, self.recv = send, recv

    def copies(self, stage):
        made = []
        for distance in range(1, 8 if stage == 0 else SIDE):
            if stage == 0:
                mine = lax.axis_index(CORE) * SIDE + lax.axis_index(AXES[0])
                other = lax.rem(mine + distance, 8)
                device = {CORE: lax.div(other, SIDE), AXES[0]: lax.rem(other, SIDE)}
                target = self.wide.at[mine]
            else:
                device = ring_peer(AXES[stage], distance)
                target = self.narrow.at[stage - 1, lax.axis_index(AXES[stage])]
            made.append(
                pltpu.make_async_remote_copy(
                    src_ref=self.tiles.at[stage],
                    dst_ref=target,
                    send_sem=self.send.at[stage, distance - 1],
                    recv_sem=self.recv.at[stage, distance - 1],
                    device_id=device,
                    device_id_type=MESH,
                )
            )
        return made

    def start(self, stage):
        for copy in self.copies(stage):
            copy.start()

    def finish(self, stage):
        for copy in self.copies(stage):
            copy.wait()
        if stage == 0:
            self.wide[lax.axis_index(CORE) * SIDE + lax.axis_index(AXES[0])] = self.tiles[0]
            got = [self.wide[place] for place in range(8)]
        else:
            self.narrow[stage - 1, lax.axis_index(AXES[stage])] = self.tiles[stage]
            got = [self.narrow[stage - 1, place] for place in range(SIDE)]
        total = got[0]
        for other in got[1:]:
            total = total + other
        self.tiles[stage + 1] = total


def peers():
    core, x = lax.axis_index(CORE), lax.axis_index(AXES[0])
    found = [{CORE: 1 - core}]
    for distance in (1, 2, 3):
        found.append({CORE: 1 - core, AXES[0]: lax.rem(x + distance, SIDE)})
        found += [ring_peer(axis, distance) for axis in AXES]
    return found


def kernel(
    sizes,
    ids_hbm, tokens_hbm, frozen_hbm, down_hbm, up_hbm, gate_hbm, upstream_hbm,
    projected_ref, input_ref, down_ref, up_ref, gate_ref, stats_ref,
    ids, tokens, frozen, sides, up, gate, masked,
    low, prob, plain, weighted, grads, grads_t, weighted_t, gate_t,
    part, total, halves, firsts, seconds, thirds, tiles, wide, narrow,
    load_sem, token_sem, send, recv, stat_send, stat_recv,
):
    rows, width, outputs, ranks, experts = sizes
    rank = ranks // experts
    scale = 1.0 / rank
    chunks = rows // CHUNK
    up_base = width
    gate_base = width + outputs
    pieces = (Piece(0, 0, 1792), Piece(1, 1792, 1792), Piece(2, 3584, gate_base - 3584), Piece(3, gate_base, width * experts // LANES))
    exchange = Exchange(part, total, halves, firsts, seconds, thirds, send, recv)
    statistics = Statistics(tiles, wide, narrow, stat_send, stat_recv)

    barrier = pltpu.get_barrier_semaphore()
    greeted = peers()
    for peer in greeted:
        pl.semaphore_signal(barrier, inc=1, device_id=peer, device_id_type=MESH)

    def load(source, target, slot):
        return pltpu.make_async_copy(source, target, load_sem.at[slot])

    def token_load(chunk):
        here = span(chunk * CHUNK, CHUNK, CHUNK)
        return pltpu.make_async_copy(tokens_hbm.at[here], tokens.at[here], token_sem.at[chunk])

    gate_load = load(gate_hbm, gate, 0)
    ids_load = load(ids_hbm, ids, 1)
    down_load = load(down_hbm, sides.at[:, pl.ds(0, ranks)], 2)
    up_load = load(up_hbm, up, 3)
    upstream_load = load(upstream_hbm, masked, 4)
    frozen_load = load(frozen_hbm, frozen, 5)
    gate_load.start()
    ids_load.start()
    down_load.start()
    for chunk in range(chunks):
        token_load(chunk).start()
    up_load.start()
    upstream_load.start()
    frozen_load.start()

    gate_load.wait()

    @pl.loop(0, width // 512)
    def _(block):
        here = span(block * 512, 512, 512)
        row = gate[:, here].astype(F32)
        tall = jnp.concatenate([jnp.broadcast_to(row[e : e + 1], (rank, 512)) for e in range(experts)], axis=0)
        sides[here, ranks : 2 * ranks] = tall.T.astype(BF16)

    ids_load.wait()
    live_rows = jnp.sum(jnp.sum((ids[...] != 0).astype(F32), axis=1, keepdims=True), axis=0, keepdims=True)

    def live_of(chunk):
        row = lax.broadcasted_iota(jnp.int32, (CHUNK, LANES), 0) + chunk * CHUNK
        return (row.astype(F32) < live_rows).astype(F32)

    def lane_sum(value):
        return jnp.sum(value, axis=1, keepdims=True)

    tiles[0] = jnp.zeros((8, LANES), F32)
    down_load.wait()

    @pl.loop(0, chunks)
    def _(chunk):
        here = span(chunk * CHUNK, CHUNK, CHUNK)
        token_load(chunk).wait()
        both = dot(tokens[here], sides[...])
        low[here] = both[:, :ranks].astype(BF16)
        logits = both[:, ranks:]
        shifted = logits - jnp.max(logits, axis=1, keepdims=True)
        raised = jnp.exp(shifted)
        mass = lane_sum(raised) * scale
        share = raised / mass
        logp = shifted - jnp.log(mass)
        entropy = -lane_sum(share * logp) * scale
        alive = live_of(chunk)
        prob[here] = share
        plain[here] = 50.0 * alive * share * (logp + entropy)
        tiles[0, 0:1] += jnp.sum(alive * share, axis=0, keepdims=True)
        tiles[0, 1:2] += jnp.sum(alive * entropy, axis=0, keepdims=True)
        tiles[0, 2:3] += jnp.sum(alive, axis=0, keepdims=True)

    pl.semaphore_wait(barrier, len(greeted))
    statistics.start(0)

    up_load.wait()
    upstream_load.wait()
    group = lax.broadcasted_iota(jnp.int32, (2 * ranks, ranks), 0) % ranks // rank
    member = lax.broadcasted_iota(jnp.int32, (2 * ranks, ranks), 1) // rank
    blocks = (group == member).astype(F32).astype(BF16)

    @pl.loop(0, chunks)
    def _(chunk):
        here = span(chunk * CHUNK, CHUNK, CHUNK)
        alive = live_of(chunk)[:, 0:1]
        mine = jnp.where(alive > 0.0, masked[here].astype(F32), 0.0).astype(BF16)
        masked[here] = mine
        back = right_dot(mine, up[...])
        share = prob[here]
        below = low[here].astype(F32)
        heavy = (below * share).astype(BF16).astype(F32) * 2.0
        steep = (2.0 * share * back).astype(BF16)
        weighted[here] = heavy.astype(BF16)
        grads[here, 0:ranks] = steep
        grads_t[:, here] = steep.astype(F32).T.astype(BF16)
        weighted_t[:, here] = heavy.T.astype(BF16)
        product = below * back
        upper = product.astype(BF16)
        lower = (product - upper.astype(F32)).astype(BF16)
        task = 2.0 * dot(jnp.concatenate([upper, lower], axis=1), blocks)
        plain[here] += share * (task - lane_sum(share * task) * scale)

    statistics.finish(0)
    statistics.start(1)

    def down_blocks(first, last):
        @pl.loop(first, last)
        def _(block):
            here = span(block * 256, 256, 256)
            part[here] = dot(grads_t[...], tokens[:, here]).T

    down_blocks(0, 7)
    exchange.start(0, pieces[0])
    statistics.finish(1)
    statistics.start(2)
    down_blocks(7, 14)
    exchange.start(0, pieces[1])
    exchange.step(0, pieces[0])
    down_blocks(14, 16)

    @pl.loop(0, outputs // 256)
    def _(block):
        found = dot(weighted_t[...], masked[:, span(block * 256, 256, 256)])
        part[span(up_base + block * 256, LANES, LANES)] = found[:, :LANES]
        part[span(up_base + block * 256 + LANES, LANES, LANES)] = found[:, LANES:]

    exchange.start(0, pieces[2])
    exchange.step(0, pieces[1])
    statistics.finish(2)
    load_all, live_all = tiles[3, 0:1], tiles[3, 2:3]
    push = (2.0 * experts * 100.0) / live_all
    lane = lax.broadcasted_iota(jnp.int32, (CHUNK, LANES), 1)
    pick_from = lax.broadcasted_iota(jnp.int32, (ranks, ranks), 0)
    pick_to = lax.broadcasted_iota(jnp.int32, (ranks, ranks), 1)
    pick = (pick_from == (pick_to % experts) * rank + pick_to // experts).astype(F32)
    pick = jnp.where(pick_to < 2 * experts, pick, 0.0).astype(BF16)

    @pl.loop(0, chunks)
    def _(chunk):
        here = span(chunk * CHUNK, CHUNK, CHUNK)
        share = prob[here]
        slope = share * (load_all - lane_sum(share * load_all) * scale)
        whole = plain[here] + push * live_of(chunk) * slope
        upper = whole.astype(BF16).astype(F32)
        place = lane % rank
        packed = jnp.where(place == 0, upper, jnp.where(place == 1, whole - upper, 0.0)).astype(BF16)
        grads[here, ranks : 2 * ranks] = packed
        gate_t[:, here] = dot(packed, pick).T[: 2 * experts].astype(BF16)

    @pl.loop(0, width // 512)
    def _(block):
        found = dot(gate_t[...], tokens[:, span(block * 512, 512, 512)])
        found = found[:experts] + found[experts:]
        for piece in range(4):
            here = span(gate_base + (block * 4 + piece) * experts, experts)
            part[here] = found[:, piece * LANES : (piece + 1) * LANES]

    exchange.start(0, pieces[3])
    exchange.step(0, pieces[2])

    def base_blocks(first, last):
        @pl.loop(first, last)
        def _(block):
            tall = span((block % 2) * (rows // 2), rows // 2, rows // 2)
            here = span((block // 2) * 256, 256, 256)
            found = dot(tokens[tall], frozen[:, here]) + dot(weighted[tall], up[:, here])
            projected_ref[tall, here] = found.astype(BF16)

    def input_blocks(first, last):
        @pl.loop(first, last)
        def _(block):
            here = span(block * 256, 256, 256)
            found = right_dot(masked[...], frozen[here]) + right_dot(grads[...], sides[here])
            input_ref[:, here] = found.astype(BF16)

    def step_all(phase):
        for piece in pieces[:3]:
            exchange.step(phase, piece)

    frozen_load.wait()
    base_blocks(0, 2)
    exchange.step(0, pieces[3])
    base_blocks(2, 5)
    step_all(1)
    base_blocks(5, 8)
    exchange.step(1, pieces[3])
    step_all(2)
    input_blocks(0, 4)
    exchange.step(2, pieces[3])
    step_all(3)
    input_blocks(4, 8)
    exchange.step(3, pieces[3])
    step_all(4)
    input_blocks(8, 12)
    exchange.step(4, pieces[3])
    input_blocks(12, 16)
    step_all(5)
    exchange.step(5, pieces[3])
    for piece in pieces:
        exchange.finish(6, piece)

    every = width + outputs + width * experts // LANES
    squares = jnp.zeros((8, LANES), F32)

    def add_squares(block, found):
        for piece in range(4):
            value = total[span((block * 4 + piece) * 8, 8)]
            found = found + value * value
        return found

    squares = lax.fori_loop(0, every // 32, add_squares, squares)
    norm = jnp.sqrt(jnp.sum(lane_sum(squares), axis=0, keepdims=True))
    limit = math.sqrt(every * LANES)
    factor = jnp.minimum(1.0, limit / norm)

    @pl.loop(0, width // 256)
    def _(block):
        here = span(block * 256, 256, 256)
        down_ref[here] = total[here] * factor

    for block in range(outputs // LANES):
        up_ref[:, block * LANES : (block + 1) * LANES] = total[up_base + block * LANES : up_base + (block + 1) * LANES] * factor
    for block in range(width // LANES):
        here = gate_base + block * experts
        gate_ref[:, block * LANES : (block + 1) * LANES] = total[here : here + experts] * factor

    to = lax.broadcasted_iota(jnp.int32, (8, LANES), 1)
    which = lax.broadcasted_iota(jnp.int32, (8, LANES), 0)
    mean = tiles[3] / live_all
    column = lane_sum(jnp.where(to == which * rank, jnp.broadcast_to(mean[0:1], (8, LANES)), 0.0))
    load_row = jnp.sum(jnp.where(to == which, jnp.broadcast_to(column, (8, LANES)), 0.0), axis=0, keepdims=True)
    stats_ref[...] = jnp.where(which == 0, jnp.broadcast_to(load_row, (8, LANES)), jnp.broadcast_to(mean[1:2], (8, LANES)))


def on_device(token_ids, tokens, frozen_weight, adapter_down, adapter_up, gate_weight, upstream):
    rows, width = tokens.shape
    ranks, outputs = adapter_up.shape
    experts = gate_weight.shape[1]
    every = width + outputs + width * experts // LANES
    anywhere = pl.BlockSpec(memory_space=pl.ANY)
    vmem = pl.BlockSpec(memory_space=pltpu.VMEM)
    found = pl.pallas_call(
        functools.partial(kernel, (rows, width, outputs, ranks, experts)),
        out_shape=(
            pltpu.VMEM((rows, outputs), BF16),
            pltpu.VMEM((rows, width), BF16),
            pltpu.VMEM((width, ranks), F32),
            pltpu.VMEM((ranks, outputs), F32),
            pltpu.VMEM((experts, width), F32),
            pltpu.VMEM((8, LANES), F32),
        ),
        in_specs=[anywhere] * 7,
        out_specs=(vmem,) * 6,
        scratch_shapes=[
            pltpu.VMEM((rows // LANES, LANES), jnp.int32),
            pltpu.VMEM((rows, width), BF16),
            pltpu.VMEM((width, outputs), BF16),
            pltpu.VMEM((width, 2 * ranks), BF16),
            pltpu.VMEM((ranks, outputs), BF16),
            pltpu.VMEM((experts, width), BF16),
            pltpu.VMEM((rows, outputs), BF16),
            pltpu.VMEM((rows, ranks), BF16),
            pltpu.VMEM((rows, ranks), F32),
            pltpu.VMEM((rows, ranks), F32),
            pltpu.VMEM((rows, ranks), BF16),
            pltpu.VMEM((rows, 2 * ranks), BF16),
            pltpu.VMEM((ranks, rows), BF16),
            pltpu.VMEM((ranks, rows), BF16),
            pltpu.VMEM((2 * experts, rows), BF16),
            pltpu.VMEM((every, LANES), F32),
            pltpu.VMEM((every, LANES), F32),
            pltpu.VMEM((every // 2, LANES), F32),
            pltpu.VMEM((3, every // 8, LANES), F32),
            pltpu.VMEM((3, every // 32, LANES), F32),
            pltpu.VMEM((4, every // 32, LANES), F32),
            pltpu.VMEM((4, 8, LANES), F32),
            pltpu.VMEM((8, 8, LANES), F32),
            pltpu.VMEM((2, SIDE, 8, LANES), F32),
            pltpu.SemaphoreType.DMA((6,)),
            pltpu.SemaphoreType.DMA((rows // CHUNK,)),
            pltpu.SemaphoreType.DMA((7, 4, 3)),
            pltpu.SemaphoreType.DMA((7, 4, 3)),
            pltpu.SemaphoreType.DMA((3, 7)),
            pltpu.SemaphoreType.DMA((3, 7)),
        ],
        compiler_params=pltpu.CompilerParams(
            collective_id=0, has_side_effects=True, vmem_limit_bytes=48 * 1024 * 1024
        ),
        name="step",
    )(token_ids.reshape(rows // LANES, LANES), tokens, frozen_weight, adapter_down, adapter_up, gate_weight.T, upstream)
    projected, input_grad, down, up, gate, stats = found
    return projected, input_grad, down, up, gate.T, stats[0, :experts], stats[1, 0]


def solution(mesh):
    torus = Mesh(mesh.devices.reshape(4, 4, 4, 2), DP)
    return jax.shard_map(
        on_device,
        mesh=torus,
        in_specs=(P(DP), P(DP, None), P(), P(), P(), P(), P(DP, None)),
        out_specs=(P(DP, None), P(DP, None), P(), P(), P(), P(), P()),
        check_vma=False,
    )
```

```python
import functools
import math

import jax
import jax.numpy as jnp
from jax import lax
from jax.experimental import pallas as pl
from jax.experimental.pallas import tpu as pltpu
from jax.sharding import Mesh
from jax.sharding import PartitionSpec as P

AXES = ("dp_0", "dp_1", "dp_2")
CORE = "dp_3"
DP = AXES + (CORE,)
MESH = pl.DeviceIdType.MESH
SIDE = 4
LANES = 128
CHUNK = 256
BF16 = jnp.bfloat16
F32 = jnp.float32


def dot(first, second):
    return jnp.dot(first, second, preferred_element_type=F32)


def right_dot(first, second):
    return lax.dot_general(first, second, (((1,), (1,)), ((), ())), preferred_element_type=F32)


def ring_peer(axis, distance):
    return {axis: lax.rem(lax.axis_index(axis) + distance, SIDE)}


def span(start, size, unit=8):
    return pl.ds(pl.multiple_of(start, unit), size)


class Piece:
    def __init__(self, index, base, rows):
        self.index, self.base, self.rows = index, base, rows
        self.half, self.quarter, self.last = rows // 2, rows // 8, rows // 32
        self.first, self.second, self.third = (AXES[(index + step) % 3] for step in range(3))


class Exchange:
    def __init__(self, part, total, halves, firsts, seconds, thirds, send, recv):
        self.part, self.total = part, total
        self.halves, self.firsts, self.seconds, self.thirds = halves, firsts, seconds, thirds
        self.send, self.recv = send, recv
        self.core = lax.axis_index(CORE)

    def half_at(self, piece, core):
        return piece.base + core * piece.half

    def quarter_at(self, piece, place):
        return self.half_at(piece, self.core) + place * piece.quarter

    def last_at(self, piece, place, second):
        return self.quarter_at(piece, place) + second * piece.last

    def copies(self, phase, piece):
        one, two = lax.axis_index(piece.first), lax.axis_index(piece.second)

        def copy(source, target, slot, device):
            return pltpu.make_async_remote_copy(
                src_ref=source,
                dst_ref=target,
                send_sem=self.send.at[phase, piece.index, slot],
                recv_sem=self.recv.at[phase, piece.index, slot],
                device_id=device,
                device_id_type=MESH,
            )

        if phase == 0:
            source = self.part.at[span(self.half_at(piece, 1 - self.core), piece.half)]
            target = self.halves.at[pl.ds(piece.base // 2, piece.half)]
            return [copy(source, target, 0, {CORE: 1 - self.core})]
        if phase == 6:
            here = self.total.at[span(self.half_at(piece, self.core), piece.half)]
            return [copy(here, here, 0, {CORE: 1 - self.core})]
        made = []
        for distance in (1, 2, 3):
            slot = distance - 1
            if phase == 1:
                place = lax.rem(one + distance, SIDE)
                source = self.part.at[span(self.quarter_at(piece, place), piece.quarter)]
                target = self.firsts.at[slot, pl.ds(piece.base // 8, piece.quarter)]
                axis = piece.first
            elif phase == 2:
                place = lax.rem(two + distance, SIDE)
                source = self.part.at[span(self.last_at(piece, one, place), piece.last)]
                target = self.seconds.at[slot, pl.ds(piece.base // 32, piece.last)]
                axis = piece.second
            elif phase == 3:
                source = self.part.at[span(self.last_at(piece, one, two), piece.last)]
                target = self.thirds.at[lax.axis_index(piece.third), pl.ds(piece.base // 32, piece.last)]
                axis = piece.third
            elif phase == 4:
                source = self.total.at[span(self.last_at(piece, one, two), piece.last)]
                target, axis = source, piece.second
            else:
                source = self.total.at[span(self.quarter_at(piece, one), piece.quarter)]
                target, axis = source, piece.first
            made.append(copy(source, target, slot, ring_peer(axis, distance)))
        return made

    def start(self, phase, piece):
        for copy in self.copies(phase, piece):
            copy.start()

    def finish(self, phase, piece):
        for copy in self.copies(phase, piece):
            copy.wait()
        one, two = lax.axis_index(piece.first), lax.axis_index(piece.second)
        if phase == 0:
            here = span(self.half_at(piece, self.core), piece.half)
            self.part[here] = self.part[here] + self.halves[pl.ds(piece.base // 2, piece.half)]
        elif phase == 1:
            here = span(self.quarter_at(piece, one), piece.quarter)
            there = pl.ds(piece.base // 8, piece.quarter)
            got = self.firsts
            self.part[here] = (self.part[here] + got[0, there]) + (got[1, there] + got[2, there])
        elif phase == 2:
            here = span(self.last_at(piece, one, two), piece.last)
            there = pl.ds(piece.base // 32, piece.last)
            got = self.seconds
            self.part[here] = (self.part[here] + got[0, there]) + (got[1, there] + got[2, there])
        elif phase == 3:
            here = span(self.last_at(piece, one, two), piece.last)
            there = pl.ds(piece.base // 32, piece.last)
            got = self.thirds
            got[lax.axis_index(piece.third), there] = self.part[here]
            self.total[here] = (got[0, there] + got[1, there]) + (got[2, there] + got[3, there])

    def step(self, phase, piece):
        self.finish(phase, piece)
        self.start(phase + 1, piece)


class Statistics:
    def __init__(self, tiles, wide, narrow, send, recv):
        self.tiles, self.wide, self.narrow = tiles, wide, narrow
        self.send, self.recv = send, recv

    def copies(self, stage):
        made = []
        for distance in range(1, 8 if stage == 0 else SIDE):
            if stage == 0:
                mine = lax.axis_index(CORE) * SIDE + lax.axis_index(AXES[0])
                other = lax.rem(mine + distance, 8)
                device = {CORE: lax.div(other, SIDE), AXES[0]: lax.rem(other, SIDE)}
                target = self.wide.at[mine]
            else:
                device = ring_peer(AXES[stage], distance)
                target = self.narrow.at[stage - 1, lax.axis_index(AXES[stage])]
            made.append(
                pltpu.make_async_remote_copy(
                    src_ref=self.tiles.at[stage],
                    dst_ref=target,
                    send_sem=self.send.at[stage, distance - 1],
                    recv_sem=self.recv.at[stage, distance - 1],
                    device_id=device,
                    device_id_type=MESH,
                )
            )
        return made

    def start(self, stage):
        for copy in self.copies(stage):
            copy.start()

    def finish(self, stage):
        for copy in self.copies(stage):
            copy.wait()
        if stage == 0:
            self.wide[lax.axis_index(CORE) * SIDE + lax.axis_index(AXES[0])] = self.tiles[0]
            got = [self.wide[place] for place in range(8)]
        else:
            self.narrow[stage - 1, lax.axis_index(AXES[stage])] = self.tiles[stage]
            got = [self.narrow[stage - 1, place] for place in range(SIDE)]
        total = got[0]
        for other in got[1:]:
            total = total + other
        self.tiles[stage + 1] = total


def peers():
    core, x = lax.axis_index(CORE), lax.axis_index(AXES[0])
    found = [{CORE: 1 - core}]
    for distance in (1, 2, 3):
        found.append({CORE: 1 - core, AXES[0]: lax.rem(x + distance, SIDE)})
        found += [ring_peer(axis, distance) for axis in AXES]
    return found


def kernel(
    sizes,
    ids_hbm, tokens_hbm, frozen_hbm, down_hbm, up_hbm, gate_hbm, upstream_hbm,
    projected_ref, input_ref, total, tiles,
    ids, tokens, frozen, sides, up, gate, masked,
    low, prob, plain, turned, weighted, grads, grads_t, weighted_t, gate_t,
    part, halves, firsts, seconds, thirds, wide, narrow,
    load_sem, token_sem, send, recv, stat_send, stat_recv,
):
    rows, width, outputs, ranks, experts = sizes
    rank = ranks // experts
    scale = 1.0 / rank
    chunks = rows // CHUNK
    up_base = width
    gate_base = width + outputs
    pieces = (Piece(0, 0, 1792), Piece(1, 1792, 1792), Piece(2, 3584, gate_base - 3584), Piece(3, gate_base, width * experts // LANES))
    exchange = Exchange(part, total, halves, firsts, seconds, thirds, send, recv)
    statistics = Statistics(tiles, wide, narrow, stat_send, stat_recv)

    barrier = pltpu.get_barrier_semaphore()
    greeted = peers()
    for peer in greeted:
        pl.semaphore_signal(barrier, inc=1, device_id=peer, device_id_type=MESH)

    def load(source, target, slot):
        return pltpu.make_async_copy(source, target, load_sem.at[slot])

    def token_load(chunk):
        here = span(chunk * CHUNK, CHUNK, CHUNK)
        return pltpu.make_async_copy(tokens_hbm.at[here], tokens.at[here], token_sem.at[chunk])

    gate_load = load(gate_hbm, gate, 0)
    ids_load = load(ids_hbm, ids, 1)
    down_load = load(down_hbm, sides.at[:, pl.ds(0, ranks)], 2)
    up_load = load(up_hbm, up, 3)
    upstream_load = load(upstream_hbm, masked, 4)
    frozen_load = load(frozen_hbm, frozen, 5)
    gate_load.start()
    ids_load.start()
    down_load.start()
    for chunk in range(chunks):
        token_load(chunk).start()

    gate_load.wait()

    @pl.loop(0, width // 512)
    def _(block):
        here = span(block * 512, 512, 512)
        row = gate[:, here].astype(F32)
        tall = jnp.concatenate([jnp.broadcast_to(row[e : e + 1], (rank, 512)) for e in range(experts)], axis=0)
        sides[here, ranks : 2 * ranks] = tall.T.astype(BF16)

    ids_load.wait()
    live_rows = jnp.sum(jnp.sum((ids[...] != 0).astype(F32), axis=1, keepdims=True), axis=0, keepdims=True)

    def live_of(chunk):
        row = lax.broadcasted_iota(jnp.int32, (CHUNK, LANES), 0) + chunk * CHUNK
        return (row.astype(F32) < live_rows).astype(F32)

    def lane_sum(value):
        return jnp.sum(value, axis=1, keepdims=True)

    tiles[0] = jnp.zeros((8, LANES), F32)
    down_load.wait()

    @pl.loop(0, chunks)
    def _(chunk):
        here = span(chunk * CHUNK, CHUNK, CHUNK)
        token_load(chunk).wait()

        @pl.when(chunk == 1)
        def _():
            up_load.start()
            upstream_load.start()

        @pl.when(chunk == 3)
        def _():
            frozen_load.start()

        both = dot(tokens[here], sides[...])
        low[here] = both[:, :ranks].astype(BF16)
        logits = both[:, ranks:]
        shifted = logits - jnp.max(logits, axis=1, keepdims=True)
        raised = jnp.exp(shifted)
        mass = lane_sum(raised) * scale
        share = raised / mass
        logp = shifted - jnp.log(mass)
        entropy = -lane_sum(share * logp) * scale
        alive = live_of(chunk)
        prob[here] = share
        plain[here] = 50.0 * alive * share * (logp + entropy)
        tiles[0, 0:1] += jnp.sum(alive * share, axis=0, keepdims=True)
        tiles[0, 1:2] += jnp.sum(alive * entropy, axis=0, keepdims=True)
        tiles[0, 2:3] += jnp.sum(alive, axis=0, keepdims=True)

    pl.semaphore_wait(barrier, len(greeted))
    statistics.start(0)

    up_load.wait()
    upstream_load.wait()

    @pl.loop(0, chunks)
    def _(chunk):
        here = span(chunk * CHUNK, CHUNK, CHUNK)
        alive = live_of(chunk)[:, 0:1]
        mine = jnp.where(alive > 0.0, masked[here].astype(F32), 0.0).astype(BF16)
        masked[here] = mine
        back = right_dot(mine, up[...])
        share = prob[here]
        heavy = (low[here].astype(F32) * share).astype(BF16).astype(F32) * 2.0
        steep = (2.0 * share * back).astype(BF16)
        turned[here] = back
        weighted[here] = heavy.astype(BF16)
        grads[here, 0:ranks] = steep
        grads_t[:, here] = steep.astype(F32).T.astype(BF16)
        weighted_t[:, here] = heavy.T.astype(BF16)

    def down_block(start, size):
        here = pl.ds(start, size)
        part[here] = dot(grads_t[...], tokens[:, here]).T

    down_block(0, 896)
    down_block(896, 896)
    exchange.start(0, pieces[0])
    down_block(1792, 896)
    down_block(2688, 896)
    exchange.start(0, pieces[1])
    down_block(3584, 512)
    found = dot(weighted_t[...], masked[...])
    for block in range(outputs // LANES):
        part[up_base + block * LANES : up_base + (block + 1) * LANES] = found[:, block * LANES : (block + 1) * LANES]
    exchange.start(0, pieces[2])
    exchange.step(0, pieces[0])
    statistics.finish(0)
    statistics.start(1)
    group = lax.broadcasted_iota(jnp.int32, (2 * ranks, ranks), 0) % ranks // rank
    member = lax.broadcasted_iota(jnp.int32, (2 * ranks, ranks), 1) // rank
    blocks = (group == member).astype(F32).astype(BF16)

    @pl.loop(0, chunks)
    def _(chunk):
        here = span(chunk * CHUNK, CHUNK, CHUNK)
        share = prob[here]
        product = low[here].astype(F32) * turned[here]
        upper = product.astype(BF16)
        lower = (product - upper.astype(F32)).astype(BF16)
        task = 2.0 * dot(jnp.concatenate([upper, lower], axis=1), blocks)
        plain[here] += share * (task - lane_sum(share * task) * scale)

    exchange.step(0, pieces[1])

    def base_blocks(first, last):
        @pl.loop(first, last)
        def _(block):
            tall = span((block % 2) * (rows // 2), rows // 2, rows // 2)
            here = span((block // 2) * 256, 256, 256)
            found = dot(tokens[tall], frozen[:, here]) + dot(weighted[tall], up[:, here])
            projected_ref[tall, here] = found.astype(BF16)

    def input_blocks(first, last):
        @pl.loop(first, last)
        def _(block):
            here = span(block * 512, 512, 512)
            found = right_dot(masked[...], frozen[here]) + right_dot(grads[...], sides[here])
            input_ref[:, here] = found.astype(BF16)

    def step_all(phase):
        for piece in pieces[:3]:
            exchange.step(phase, piece)

    frozen_load.wait()
    base_blocks(0, 1)
    exchange.step(0, pieces[2])
    statistics.finish(1)
    statistics.start(2)
    base_blocks(1, 3)
    statistics.finish(2)
    load_all, live_all = tiles[3, 0:1], tiles[3, 2:3]
    push = (2.0 * experts * 100.0) / live_all
    lane = lax.broadcasted_iota(jnp.int32, (CHUNK, LANES), 1)
    pick_from = lax.broadcasted_iota(jnp.int32, (ranks, ranks), 0)
    pick_to = lax.broadcasted_iota(jnp.int32, (ranks, ranks), 1)
    pick = (pick_from == (pick_to % experts) * rank + pick_to // experts).astype(F32)
    pick = jnp.where(pick_to < 2 * experts, pick, 0.0).astype(BF16)

    @pl.loop(0, chunks)
    def _(chunk):
        here = span(chunk * CHUNK, CHUNK, CHUNK)
        share = prob[here]
        slope = share * (load_all - lane_sum(share * load_all) * scale)
        whole = plain[here] + push * live_of(chunk) * slope
        upper = whole.astype(BF16).astype(F32)
        place = lane % rank
        packed = jnp.where(place == 0, upper, jnp.where(place == 1, whole - upper, 0.0)).astype(BF16)
        grads[here, ranks : 2 * ranks] = packed
        gate_t[:, here] = dot(packed, pick).T[: 2 * experts].astype(BF16)

    @pl.loop(0, width // 1024)
    def _(block):
        found = dot(gate_t[...], tokens[:, span(block * 1024, 1024, 1024)])
        found = found[:experts] + found[experts:]
        for piece in range(8):
            here = span(gate_base + (block * 8 + piece) * experts, experts)
            part[here] = found[:, piece * LANES : (piece + 1) * LANES]

    exchange.start(0, pieces[3])
    base_blocks(3, 4)
    exchange.step(0, pieces[3])
    step_all(1)
    base_blocks(4, 7)
    exchange.step(1, pieces[3])
    step_all(2)
    base_blocks(7, 8)
    input_blocks(0, 1)
    exchange.step(2, pieces[3])
    step_all(3)
    input_blocks(1, 3)
    exchange.step(3, pieces[3])
    step_all(4)
    input_blocks(3, 5)
    exchange.step(4, pieces[3])
    input_blocks(5, 8)
    step_all(5)
    exchange.step(5, pieces[3])
    for piece in pieces:
        exchange.finish(6, piece)


def finish_kernel(
    sizes,
    projected, inputs, total, tiles,
    projected_hbm, input_hbm, down_hbm, up_hbm, gate_hbm, load_ref, entropy_ref,
    scaled, up, gate, sems,
):
    width, outputs, ranks, experts = sizes
    rank = ranks // experts
    every = total.shape[0]
    quarter = width // 4
    copies = [
        pltpu.make_async_copy(inputs, input_hbm, sems.at[0]),
        pltpu.make_async_copy(projected, projected_hbm, sems.at[1]),
    ]
    for copy in copies:
        copy.start()

    def add_squares(block, found):
        value = total[span(block * 192, 192)]
        return found + jnp.sum((value * value).reshape(6, 32, LANES), axis=0)

    squares = lax.fori_loop(0, every // 192, add_squares, jnp.zeros((32, LANES), F32))
    norm = jnp.sqrt(jnp.sum(jnp.sum(squares, axis=1, keepdims=True), axis=0, keepdims=True))
    factor = jnp.minimum(1.0, math.sqrt(every * LANES) / norm)
    for block in range(4):
        here = pl.ds(block * quarter, quarter)
        scaled[here] = total[here] * factor
        copy = pltpu.make_async_copy(scaled.at[here], down_hbm.at[here], sems.at[2 + block])
        copy.start()
        copies.append(copy)
    for block in range(outputs // LANES):
        here = width + block * LANES
        up[:, block * LANES : (block + 1) * LANES] = total[here : here + LANES] * factor
    copy = pltpu.make_async_copy(up, up_hbm, sems.at[6])
    copy.start()
    copies.append(copy)
    for block in range(width // LANES):
        here = width + outputs + block * experts
        gate[:, block * LANES : (block + 1) * LANES] = total[here : here + experts] * factor
    copy = pltpu.make_async_copy(gate, gate_hbm, sems.at[7])
    copy.start()
    copies.append(copy)
    mean = tiles[3] / tiles[3, 2:3]
    lane = lax.broadcasted_iota(jnp.int32, (1, LANES), 1)
    for expert in range(experts):
        load_ref[expert] = jnp.sum(jnp.where(lane == expert * rank, mean[0:1], 0.0))
    entropy_ref[0] = jnp.sum(jnp.where(lane == 0, mean[1:2], 0.0))
    for copy in copies:
        copy.wait()


def on_device(token_ids, tokens, frozen_weight, adapter_down, adapter_up, gate_weight, upstream):
    rows, width = tokens.shape
    ranks, outputs = adapter_up.shape
    experts = gate_weight.shape[1]
    every = width + outputs + width * experts // LANES
    anywhere = pl.BlockSpec(memory_space=pl.ANY)
    vmem = pl.BlockSpec(memory_space=pltpu.VMEM)
    smem = pl.BlockSpec(memory_space=pltpu.SMEM)
    held = pl.pallas_call(
        functools.partial(kernel, (rows, width, outputs, ranks, experts)),
        out_shape=(
            pltpu.VMEM((rows, outputs), BF16),
            pltpu.VMEM((rows, width), BF16),
            pltpu.VMEM((every, LANES), F32),
            pltpu.VMEM((4, 8, LANES), F32),
        ),
        in_specs=[anywhere] * 7,
        out_specs=(vmem,) * 4,
        scratch_shapes=[
            pltpu.VMEM((rows // LANES, LANES), jnp.int32),
            pltpu.VMEM((rows, width), BF16),
            pltpu.VMEM((width, outputs), BF16),
            pltpu.VMEM((width, 2 * ranks), BF16),
            pltpu.VMEM((ranks, outputs), BF16),
            pltpu.VMEM((experts, width), BF16),
            pltpu.VMEM((rows, outputs), BF16),
            pltpu.VMEM((rows, ranks), BF16),
            pltpu.VMEM((rows, ranks), F32),
            pltpu.VMEM((rows, ranks), F32),
            pltpu.VMEM((rows, ranks), F32),
            pltpu.VMEM((rows, ranks), BF16),
            pltpu.VMEM((rows, 2 * ranks), BF16),
            pltpu.VMEM((ranks, rows), BF16),
            pltpu.VMEM((ranks, rows), BF16),
            pltpu.VMEM((2 * experts, rows), BF16),
            pltpu.VMEM((every, LANES), F32),
            pltpu.VMEM((every // 2, LANES), F32),
            pltpu.VMEM((3, every // 8, LANES), F32),
            pltpu.VMEM((3, every // 32, LANES), F32),
            pltpu.VMEM((4, every // 32, LANES), F32),
            pltpu.VMEM((8, 8, LANES), F32),
            pltpu.VMEM((2, SIDE, 8, LANES), F32),
            pltpu.SemaphoreType.DMA((6,)),
            pltpu.SemaphoreType.DMA((rows // CHUNK,)),
            pltpu.SemaphoreType.DMA((7, 4, 3)),
            pltpu.SemaphoreType.DMA((7, 4, 3)),
            pltpu.SemaphoreType.DMA((3, 7)),
            pltpu.SemaphoreType.DMA((3, 7)),
        ],
        compiler_params=pltpu.CompilerParams(
            collective_id=0, has_side_effects=True, vmem_limit_bytes=46 * 1024 * 1024
        ),
        name="step",
    )(token_ids.reshape(rows // LANES, LANES), tokens, frozen_weight, adapter_down, adapter_up, gate_weight.T, upstream)
    projected, input_grad, down, up, gate, load, entropy = pl.pallas_call(
        functools.partial(finish_kernel, (width, outputs, ranks, experts)),
        out_shape=(
            jax.ShapeDtypeStruct((rows, outputs), BF16),
            jax.ShapeDtypeStruct((rows, width), BF16),
            jax.ShapeDtypeStruct((width, ranks), F32),
            jax.ShapeDtypeStruct((ranks, outputs), F32),
            jax.ShapeDtypeStruct((experts, width), F32),
            jax.ShapeDtypeStruct((experts,), F32),
            jax.ShapeDtypeStruct((1,), F32),
        ),
        in_specs=[vmem] * 4,
        out_specs=(anywhere,) * 5 + (smem,) * 2,
        scratch_shapes=[
            pltpu.VMEM((width, ranks), F32),
            pltpu.VMEM((ranks, outputs), F32),
            pltpu.VMEM((experts, width), F32),
            pltpu.SemaphoreType.DMA((8,)),
        ],
        compiler_params=pltpu.CompilerParams(vmem_limit_bytes=20 * 1024 * 1024),
        name="finish",
    )(*held)
    return projected, input_grad, down, up, gate.T, load, entropy.reshape(())


def solution(mesh):
    torus = Mesh(mesh.devices.reshape(4, 4, 4, 2), DP)
    return jax.shard_map(
        on_device,
        mesh=torus,
        in_specs=(P(DP), P(DP, None), P(), P(), P(), P(), P(DP, None)),
        out_specs=(P(DP, None), P(DP, None), P(), P(), P(), P(), P()),
        check_vma=False,
    )
```

```python
import functools
import math

import jax
import jax.numpy as jnp
from jax import lax
from jax.experimental import pallas as pl
from jax.experimental.pallas import tpu as pltpu
from jax.sharding import Mesh
from jax.sharding import PartitionSpec as P

AXES = ("dp_0", "dp_1", "dp_2")
CORE = "dp_3"
DP = AXES + (CORE,)
MESH = pl.DeviceIdType.MESH
SIDE = 4
LANES = 128
CHUNK = 256
BF16 = jnp.bfloat16
F32 = jnp.float32


def dot(first, second):
    return jnp.dot(first, second, preferred_element_type=F32)


def right_dot(first, second):
    return lax.dot_general(first, second, (((1,), (1,)), ((), ())), preferred_element_type=F32)


def ring_peer(axis, distance):
    return {axis: lax.rem(lax.axis_index(axis) + distance, SIDE)}


def span(start, size, unit=8):
    return pl.ds(pl.multiple_of(start, unit), size)


class Piece:
    def __init__(self, index, base, rows):
        self.index, self.base, self.rows = index, base, rows
        self.half, self.quarter, self.last = rows // 2, rows // 8, rows // 32
        self.first, self.second, self.third = (AXES[(index + step) % 3] for step in range(3))


class Exchange:
    def __init__(self, part, total, halves, firsts, seconds, thirds, send, recv):
        self.part, self.total = part, total
        self.halves, self.firsts, self.seconds, self.thirds = halves, firsts, seconds, thirds
        self.send, self.recv = send, recv
        self.core = lax.axis_index(CORE)

    def half_at(self, piece, core):
        return piece.base + core * piece.half

    def quarter_at(self, piece, place):
        return self.half_at(piece, self.core) + place * piece.quarter

    def last_at(self, piece, place, second):
        return self.quarter_at(piece, place) + second * piece.last

    def send_to(self, source, target, phase, piece, device):
        pltpu.make_async_remote_copy(
            src_ref=source,
            dst_ref=target,
            send_sem=self.send.at[piece.index],
            recv_sem=self.recv.at[phase, piece.index],
            device_id=device,
            device_id_type=MESH,
        ).start()

    def sent(self, piece, rows):
        here = self.part.at[pl.ds(0, rows)]
        pltpu.make_async_copy(here, here, self.send.at[piece.index]).wait()

    def received(self, phase, piece, rows):
        here = self.part.at[pl.ds(0, rows)]
        pltpu.make_async_copy(here, here, self.recv.at[phase, piece.index]).wait()

    def forward(self, piece, distance):
        place = lax.rem(lax.axis_index(piece.first) + distance, SIDE)
        here = self.total.at[span(self.quarter_at(piece, place), piece.quarter)]
        self.send_to(here, here, 6, piece, {CORE: 1 - self.core})

    def start(self, phase, piece):
        one, two = lax.axis_index(piece.first), lax.axis_index(piece.second)
        if phase == 0:
            source = self.part.at[span(self.half_at(piece, 1 - self.core), piece.half)]
            target = self.halves.at[pl.ds(piece.base // 2, piece.half)]
            self.send_to(source, target, 0, piece, {CORE: 1 - self.core})
            return
        if phase == 6:
            for distance in (1, 2, 3):
                self.forward(piece, distance)
            return
        for distance in (2, 1, 3):
            slot = distance - 1
            if phase == 1:
                place = lax.rem(one + distance, SIDE)
                source = self.part.at[span(self.quarter_at(piece, place), piece.quarter)]
                target = self.firsts.at[slot, pl.ds(piece.base // 8, piece.quarter)]
                axis = piece.first
            elif phase == 2:
                place = lax.rem(two + distance, SIDE)
                source = self.part.at[span(self.last_at(piece, one, place), piece.last)]
                target = self.seconds.at[slot, pl.ds(piece.base // 32, piece.last)]
                axis = piece.second
            elif phase == 3:
                source = self.part.at[span(self.last_at(piece, one, two), piece.last)]
                target = self.thirds.at[lax.axis_index(piece.third), pl.ds(piece.base // 32, piece.last)]
                axis = piece.third
            elif phase == 4:
                source = self.total.at[span(self.last_at(piece, one, two), piece.last)]
                target, axis = source, piece.second
            else:
                source = self.total.at[span(self.quarter_at(piece, one), piece.quarter)]
                target, axis = source, piece.first
            self.send_to(source, target, phase, piece, ring_peer(axis, distance))
        if phase == 5:
            self.forward(piece, 0)

    def finish(self, phase, piece):
        sent = {0: piece.half, 1: 3 * piece.quarter, 5: 4 * piece.quarter, 6: 3 * piece.quarter}
        got_rows = {0: piece.half, 1: 3 * piece.quarter, 5: 3 * piece.quarter, 6: piece.half}
        self.sent(piece, sent.get(phase, 3 * piece.last))
        self.received(phase, piece, got_rows.get(phase, 3 * piece.last))
        one, two = lax.axis_index(piece.first), lax.axis_index(piece.second)
        if phase == 0:
            here = span(self.half_at(piece, self.core), piece.half)
            self.part[here] = self.part[here] + self.halves[pl.ds(piece.base // 2, piece.half)]
        elif phase == 1:
            here = span(self.quarter_at(piece, one), piece.quarter)
            there = pl.ds(piece.base // 8, piece.quarter)
            got = self.firsts
            self.part[here] = (self.part[here] + got[0, there]) + (got[1, there] + got[2, there])
        elif phase == 2:
            here = span(self.last_at(piece, one, two), piece.last)
            there = pl.ds(piece.base // 32, piece.last)
            got = self.seconds
            self.part[here] = (self.part[here] + got[0, there]) + (got[1, there] + got[2, there])
        elif phase == 3:
            here = span(self.last_at(piece, one, two), piece.last)
            there = pl.ds(piece.base // 32, piece.last)
            got = self.thirds
            got[lax.axis_index(piece.third), there] = self.part[here]
            self.total[here] = (got[0, there] + got[1, there]) + (got[2, there] + got[3, there])

    def step(self, phase, piece):
        self.finish(phase, piece)
        self.start(phase + 1, piece)


class Statistics:
    def __init__(self, tiles, wide, narrow, send, recv):
        self.tiles, self.wide, self.narrow = tiles, wide, narrow
        self.send, self.recv = send, recv

    def start(self, stage):
        for distance in range(1, 8 if stage == 0 else SIDE):
            if stage == 0:
                mine = lax.axis_index(CORE) * SIDE + lax.axis_index(AXES[0])
                other = lax.rem(mine + distance, 8)
                device = {CORE: lax.div(other, SIDE), AXES[0]: lax.rem(other, SIDE)}
                target = self.wide.at[mine]
            else:
                device = ring_peer(AXES[stage], distance)
                target = self.narrow.at[stage - 1, lax.axis_index(AXES[stage])]
            pltpu.make_async_remote_copy(
                src_ref=self.tiles.at[stage],
                dst_ref=target,
                send_sem=self.send.at[0],
                recv_sem=self.recv.at[stage],
                device_id=device,
                device_id_type=MESH,
            ).start()

    def finish(self, stage):
        several = self.wide.at[pl.ds(0, 7 if stage == 0 else 3)]
        pltpu.make_async_copy(several, several, self.send.at[0]).wait()
        pltpu.make_async_copy(several, several, self.recv.at[stage]).wait()
        if stage == 0:
            self.wide[lax.axis_index(CORE) * SIDE + lax.axis_index(AXES[0])] = self.tiles[0]
            got = [self.wide[place] for place in range(8)]
        else:
            self.narrow[stage - 1, lax.axis_index(AXES[stage])] = self.tiles[stage]
            got = [self.narrow[stage - 1, place] for place in range(SIDE)]
        total = got[0]
        for other in got[1:]:
            total = total + other
        self.tiles[stage + 1] = total


class GateExchange:
    def __init__(self, base, rows, part, total, inward, plane, send, recv):
        self.base, self.share = base, rows // 8
        self.part, self.total = part, total
        self.inward, self.plane = inward, plane
        self.send, self.recv = send, recv
        self.group = lax.axis_index(CORE) * SIDE + lax.axis_index(AXES[0])
        self.spot = lax.axis_index(AXES[1]) * SIDE + lax.axis_index(AXES[2])

    def chunk(self, place):
        return span(self.base + place * self.share, self.share)

    def start(self, stage):
        mine = self.chunk(self.group)
        for distance in range(1, 16 if stage == 1 else 8):
            if stage == 1:
                other = lax.rem(self.spot + distance, 16)
                device = {AXES[1]: lax.div(other, SIDE), AXES[2]: lax.rem(other, SIDE)}
                source, target = self.part.at[mine], self.plane.at[self.spot]
            else:
                other = lax.rem(self.group + distance, 8)
                device = {CORE: lax.div(other, SIDE), AXES[0]: lax.rem(other, SIDE)}
                if stage == 0:
                    source, target = self.part.at[self.chunk(other)], self.inward.at[distance - 1]
                else:
                    source = self.total.at[mine]
                    target = source
            pltpu.make_async_remote_copy(
                src_ref=source,
                dst_ref=target,
                send_sem=self.send.at[3],
                recv_sem=self.recv.at[stage],
                device_id=device,
                device_id_type=MESH,
            ).start()

    def finish(self, stage):
        several = self.plane.at[pl.ds(0, 15 if stage == 1 else 7)]
        pltpu.make_async_copy(several, several, self.send.at[3]).wait()
        pltpu.make_async_copy(several, several, self.recv.at[stage]).wait()
        mine = self.chunk(self.group)
        if stage == 0:
            value = self.part[mine]
            for slot in range(7):
                value = value + self.inward[slot]
            self.part[mine] = value
        elif stage == 1:
            self.plane[self.spot] = self.part[mine]
            value = self.plane[0]
            for slot in range(1, 16):
                value = value + self.plane[slot]
            self.total[mine] = value

    def step(self, stage):
        self.finish(stage)
        self.start(stage + 1)


def peers():
    core, x = lax.axis_index(CORE), lax.axis_index(AXES[0])
    spot = lax.axis_index(AXES[1]) * SIDE + lax.axis_index(AXES[2])
    found = [{CORE: 1 - core}]
    for distance in (1, 2, 3):
        found.append({CORE: 1 - core, AXES[0]: lax.rem(x + distance, SIDE)})
        found.append(ring_peer(AXES[0], distance))
    for distance in range(1, 16):
        other = lax.rem(spot + distance, 16)
        found.append({AXES[1]: lax.div(other, SIDE), AXES[2]: lax.rem(other, SIDE)})
    return found


def kernel(
    sizes,
    ids_hbm, tokens_hbm, frozen_hbm, down_hbm, up_hbm, gate_hbm, upstream_hbm,
    projected_ref, input_ref, total, tiles, frozen, sides, masked, grads,
    ids, tokens, up, gate,
    both, low, prob, plain, turned, weighted, grads_t, weighted_t, gate_t,
    part, halves, firsts, seconds, thirds, wide, narrow, inward, plane,
    load_sem, token_sem, send, recv, stat_send, stat_recv, gate_recv,
):
    rows, width, outputs, ranks, experts = sizes
    rank = ranks // experts
    scale = 1.0 / rank
    chunks = rows // CHUNK
    up_base = width
    gate_base = width + outputs
    pieces = (Piece(0, 0, 1792), Piece(1, 1792, 1792), Piece(2, 3584, gate_base - 3584))
    exchange = Exchange(part, total, halves, firsts, seconds, thirds, send, recv)
    statistics = Statistics(tiles, wide, narrow, stat_send, stat_recv)
    gates = GateExchange(gate_base, width * experts // LANES, part, total, inward, plane, send, gate_recv)

    gate_load = pltpu.make_async_copy(gate_hbm, gate, load_sem.at[0])
    ids_load = pltpu.make_async_copy(ids_hbm, ids, load_sem.at[1])
    gate_load.start()
    ids_load.start()
    barrier = pltpu.get_barrier_semaphore()
    greeted = peers()
    for peer in greeted:
        pl.semaphore_signal(barrier, inc=1, device_id=peer, device_id_type=MESH)

    def load(source, target, slot):
        return pltpu.make_async_copy(source, target, load_sem.at[slot])

    def token_load(chunk):
        here = span(chunk * CHUNK, CHUNK, CHUNK)
        return pltpu.make_async_copy(tokens_hbm.at[here], tokens.at[here], token_sem.at[chunk])

    down_load = load(down_hbm, sides.at[:, pl.ds(0, ranks)], 2)
    up_load = load(up_hbm, up, 3)
    upstream_load = load(upstream_hbm, masked, 4)
    frozen_load = load(frozen_hbm, frozen, 5)
    down_load.start()
    token_load(0).start()

    gate_load.wait()
    token_load(1).start()

    @pl.loop(0, width // 512)
    def _(block):
        here = span(block * 512, 512, 512)
        row = gate[:, here].astype(F32)
        tall = jnp.concatenate([jnp.broadcast_to(row[e : e + 1], (rank, 512)) for e in range(experts)], axis=0)
        sides[here, ranks : 2 * ranks] = tall.T.astype(BF16)

    ids_load.wait()
    live_rows = jnp.sum(jnp.sum((ids[...] != 0).astype(F32), axis=1, keepdims=True), axis=0, keepdims=True)

    def live_of(chunk):
        row = lax.broadcasted_iota(jnp.int32, (CHUNK, LANES), 0) + chunk * CHUNK
        return (row.astype(F32) < live_rows).astype(F32)

    def lane_sum(value):
        return jnp.sum(value, axis=1, keepdims=True)

    tiles[0] = jnp.zeros((8, LANES), F32)
    down_load.wait()

    def shares(chunk):
        here = span(chunk * CHUNK, CHUNK, CHUNK)
        slot = chunk % 2
        low[here] = both[slot, :, :ranks].astype(BF16)
        logits = both[slot, :, ranks:]
        shifted = logits - jnp.max(logits, axis=1, keepdims=True)
        raised = jnp.exp(shifted)
        mass = lane_sum(raised) * scale
        share = raised / mass
        logp = shifted - jnp.log(mass)
        entropy = -lane_sum(share * logp) * scale
        alive = live_of(chunk)
        prob[here] = share
        plain[here] = 50.0 * alive * share * (logp + entropy)
        tiles[0, 0:1] += jnp.sum(alive * share, axis=0, keepdims=True)
        tiles[0, 1:2] += jnp.sum(alive * entropy, axis=0, keepdims=True)
        tiles[0, 2:3] += jnp.sum(alive, axis=0, keepdims=True)

    token_load(2).start()
    token_load(0).wait()
    token_load(3).start()
    both[0] = dot(tokens[0:CHUNK], sides[...])
    up_load.start()
    upstream_load.start()

    @pl.loop(1, chunks)
    def _(chunk):
        token_load(chunk).wait()
        shares(chunk - 1)
        both[chunk % 2] = dot(tokens[span(chunk * CHUNK, CHUNK, CHUNK)], sides[...])

    frozen_load.start()
    shares(chunks - 1)
    pl.semaphore_wait(barrier, len(greeted))
    statistics.start(0)

    up_load.wait()
    upstream_load.wait()

    @pl.loop(0, chunks)
    def _(chunk):
        here = span(chunk * CHUNK, CHUNK, CHUNK)
        alive = live_of(chunk)[:, 0:1]
        mine = jnp.where(alive > 0.0, masked[here].astype(F32), 0.0).astype(BF16)
        masked[here] = mine
        back = right_dot(mine, up[...])
        share = prob[here]
        heavy = (low[here].astype(F32) * share).astype(BF16).astype(F32) * 2.0
        steep = (2.0 * share * back).astype(BF16)
        turned[here] = back
        weighted[here] = heavy.astype(BF16)
        grads[here, 0:ranks] = steep
        grads_t[:, here] = steep.astype(F32).T.astype(BF16)
        weighted_t[:, here] = heavy.T.astype(BF16)

    def down_block(start, size):
        here = pl.ds(start, size)
        part[here] = dot(grads_t[...], tokens[:, here]).T

    down_block(0, 896)
    down_block(896, 896)
    exchange.start(0, pieces[0])
    statistics.finish(0)
    statistics.start(1)
    down_block(1792, 896)
    down_block(2688, 896)
    exchange.start(0, pieces[1])
    down_block(3584, 512)
    found = dot(weighted_t[...], masked[...])
    for block in range(outputs // LANES):
        part[up_base + block * LANES : up_base + (block + 1) * LANES] = found[:, block * LANES : (block + 1) * LANES]
    exchange.start(0, pieces[2])
    statistics.finish(1)
    statistics.start(2)
    exchange.step(0, pieces[0])
    group = lax.broadcasted_iota(jnp.int32, (2 * ranks, ranks), 0) % ranks // rank
    member = lax.broadcasted_iota(jnp.int32, (2 * ranks, ranks), 1) // rank
    blocks = (group == member).astype(F32).astype(BF16)

    def task_part(chunk):
        here = span(chunk * CHUNK, CHUNK, CHUNK)
        share = prob[here]
        product = low[here].astype(F32) * turned[here]
        upper = product.astype(BF16)
        lower = (product - upper.astype(F32)).astype(BF16)
        task = 2.0 * dot(jnp.concatenate([upper, lower], axis=1), blocks)
        plain[here] += share * (task - lane_sum(share * task) * scale)

    exchange.step(0, pieces[1])
    lane = lax.broadcasted_iota(jnp.int32, (CHUNK, LANES), 1)
    pick_from = lax.broadcasted_iota(jnp.int32, (ranks, ranks), 0)
    pick_to = lax.broadcasted_iota(jnp.int32, (ranks, ranks), 1)
    pick = (pick_from == (pick_to % experts) * rank + pick_to // experts).astype(F32)
    pick = jnp.where(pick_to < 2 * experts, pick, 0.0).astype(BF16)

    def slope_part(chunk):
        load_all, live_all = tiles[3, 0:1], tiles[3, 2:3]
        push = (2.0 * experts * 100.0) / live_all
        here = span(chunk * CHUNK, CHUNK, CHUNK)
        share = prob[here]
        slope = share * (load_all - lane_sum(share * load_all) * scale)
        whole = plain[here] + push * live_of(chunk) * slope
        upper = whole.astype(BF16).astype(F32)
        place = lane % rank
        packed = jnp.where(place == 0, upper, jnp.where(place == 1, whole - upper, 0.0)).astype(BF16)
        grads[here, ranks : 2 * ranks] = packed
        gate_t[:, here] = dot(packed, pick).T[: 2 * experts].astype(BF16)

    def base_block(block):
        tall = span((block % 2) * (rows // 2), rows // 2, rows // 2)
        here = span((block // 2) * 256, 256, 256)
        found = dot(tokens[tall], frozen[:, here]) + dot(weighted[tall], up[:, here])
        projected_ref[tall, here] = found.astype(BF16)

    def step_all(phase):
        for piece in pieces[:3]:
            exchange.step(phase, piece)

    frozen_load.wait()
    exchange.step(0, pieces[2])

    @pl.loop(0, 2)
    def _(block):
        task_part(2 * block)
        task_part(2 * block + 1)
        base_block(block)

    statistics.finish(2)

    @pl.loop(2, 4)
    def _(block):
        slope_part(2 * block - 4)
        slope_part(2 * block - 3)
        base_block(block)

    @pl.loop(0, width // 1024)
    def _(block):
        found = dot(gate_t[...], tokens[:, span(block * 1024, 1024, 1024)])
        found = found[:experts] + found[experts:]
        for piece in range(8):
            here = span(gate_base + (block * 8 + piece) * experts, experts)
            part[here] = found[:, piece * LANES : (piece + 1) * LANES]

    gates.start(0)

    @pl.loop(4, 8)
    def _(block):
        @pl.when(block == 4)
        def _():
            exchange.step(1, pieces[0])

        @pl.when(block == 5)
        def _():
            exchange.step(1, pieces[1])
            exchange.step(1, pieces[2])

        @pl.when(block == 7)
        def _():
            step_all(2)
            gates.step(0)

        base_block(block)

    @pl.loop(0, input_ref.shape[1] // 512)
    def _(block):
        @pl.when(block == 1)
        def _():
            step_all(3)

        @pl.when(block == 2)
        def _():
            gates.step(1)

        @pl.when(block == 3)
        def _():
            step_all(4)

        @pl.when(block == 5)
        def _():
            step_all(5)

        here = span(block * 512, 512, 512)
        found = right_dot(masked[...], frozen[here]) + right_dot(grads[...], sides[here])
        input_ref[:, here] = found.astype(BF16)

    gates.finish(2)
    for piece in pieces:
        exchange.finish(6, piece)


def finish_kernel(
    sizes,
    projected, inputs, total, tiles, frozen, sides, masked, grads,
    projected_hbm, input_hbm, down_hbm, up_hbm, gate_hbm, load_ref, entropy_ref,
    scaled, up, gate, rest, sems,
):
    width, outputs, ranks, experts = sizes
    rank = ranks // experts
    every = total.shape[0]
    quarter = width // 4
    copies = [
        pltpu.make_async_copy(inputs, input_hbm.at[:, pl.ds(0, inputs.shape[1])], sems.at[0]),
        pltpu.make_async_copy(projected, projected_hbm, sems.at[1]),
    ]
    for copy in copies:
        copy.start()

    def add_squares(block, found):
        value = total[span(block * 192, 192)]
        return found + jnp.sum((value * value).reshape(6, 32, LANES), axis=0)

    squares = lax.fori_loop(0, every // 192, add_squares, jnp.zeros((32, LANES), F32))
    norm = jnp.sqrt(jnp.sum(jnp.sum(squares, axis=1, keepdims=True), axis=0, keepdims=True))
    factor = jnp.minimum(1.0, math.sqrt(every * LANES) / norm)
    for block in range(4):
        here = pl.ds(block * quarter, quarter)
        scaled[here] = total[here] * factor
        copy = pltpu.make_async_copy(scaled.at[here], down_hbm.at[here], sems.at[2 + block])
        copy.start()
        copies.append(copy)
    for block in range(outputs // LANES):
        here = width + block * LANES
        up[:, block * LANES : (block + 1) * LANES] = total[here : here + LANES] * factor
    copy = pltpu.make_async_copy(up, up_hbm, sems.at[6])
    copy.start()
    copies.append(copy)
    for block in range(width // LANES):
        here = width + outputs + block * experts
        gate[:, block * LANES : (block + 1) * LANES] = total[here : here + experts] * factor
    copy = pltpu.make_async_copy(gate, gate_hbm, sems.at[7])
    copy.start()
    copies.append(copy)
    for block in range(2):
        here = pl.ds(inputs.shape[1] + block * 512, 512)
        found = right_dot(masked[...], frozen[here]) + right_dot(grads[...], sides[here])
        rest[block] = found.astype(BF16)
        copy = pltpu.make_async_copy(rest.at[block], input_hbm.at[:, here], sems.at[8 + block])
        copy.start()
        copies.append(copy)
    mean = tiles[3] / tiles[3, 2:3]
    lane = lax.broadcasted_iota(jnp.int32, (1, LANES), 1)
    for expert in range(experts):
        load_ref[expert] = jnp.sum(jnp.where(lane == expert * rank, mean[0:1], 0.0))
    entropy_ref[0] = jnp.sum(jnp.where(lane == 0, mean[1:2], 0.0))
    for copy in copies:
        copy.wait()


def on_device(token_ids, tokens, frozen_weight, adapter_down, adapter_up, gate_weight, upstream):
    rows, width = tokens.shape
    ranks, outputs = adapter_up.shape
    experts = gate_weight.shape[1]
    every = width + outputs + width * experts // LANES
    anywhere = pl.BlockSpec(memory_space=pl.ANY)
    hbm = pl.BlockSpec(memory_space=pltpu.HBM)
    vmem = pl.BlockSpec(memory_space=pltpu.VMEM)
    smem = pl.BlockSpec(memory_space=pltpu.SMEM)
    held = pl.pallas_call(
        functools.partial(kernel, (rows, width, outputs, ranks, experts)),
        out_shape=(
            pltpu.VMEM((rows, outputs), BF16),
            pltpu.VMEM((rows, width - 1024), BF16),
            pltpu.VMEM((every, LANES), F32),
            pltpu.VMEM((4, 8, LANES), F32),
            pltpu.VMEM((width, outputs), BF16),
            pltpu.VMEM((width, 2 * ranks), BF16),
            pltpu.VMEM((rows, outputs), BF16),
            pltpu.VMEM((rows, 2 * ranks), BF16),
        ),
        in_specs=[hbm] * 7,
        out_specs=(vmem,) * 8,
        scratch_shapes=[
            pltpu.VMEM((rows // LANES, LANES), jnp.int32),
            pltpu.VMEM((rows, width), BF16),
            pltpu.VMEM((ranks, outputs), BF16),
            pltpu.VMEM((experts, width), BF16),
            pltpu.VMEM((2, CHUNK, 2 * ranks), F32),
            pltpu.VMEM((rows, ranks), BF16),
            pltpu.VMEM((rows, ranks), F32),
            pltpu.VMEM((rows, ranks), F32),
            pltpu.VMEM((rows, ranks), F32),
            pltpu.VMEM((rows, ranks), BF16),
            pltpu.VMEM((ranks, rows), BF16),
            pltpu.VMEM((ranks, rows), BF16),
            pltpu.VMEM((2 * experts, rows), BF16),
            pltpu.VMEM((every, LANES), F32),
            pltpu.VMEM((every // 2, LANES), F32),
            pltpu.VMEM((3, every // 8, LANES), F32),
            pltpu.VMEM((3, every // 32, LANES), F32),
            pltpu.VMEM((4, every // 32, LANES), F32),
            pltpu.VMEM((8, 8, LANES), F32),
            pltpu.VMEM((2, SIDE, 8, LANES), F32),
            pltpu.VMEM((7, width * experts // LANES // 8, LANES), F32),
            pltpu.VMEM((16, width * experts // LANES // 8, LANES), F32),
            pltpu.SemaphoreType.DMA((6,)),
            pltpu.SemaphoreType.DMA((rows // CHUNK,)),
            pltpu.SemaphoreType.DMA((4,)),
            pltpu.SemaphoreType.DMA((7, 3)),
            pltpu.SemaphoreType.DMA((1,)),
            pltpu.SemaphoreType.DMA((3,)),
            pltpu.SemaphoreType.DMA((3,)),
        ],
        compiler_params=pltpu.CompilerParams(
            collective_id=0, has_side_effects=True, vmem_limit_bytes=34 * 1024 * 1024
        ),
        name="step",
    )(token_ids.reshape(rows // LANES, LANES), tokens, frozen_weight, adapter_down, adapter_up, gate_weight.T, upstream)
    projected, input_grad, down, up, gate, load, entropy = pl.pallas_call(
        functools.partial(finish_kernel, (width, outputs, ranks, experts)),
        out_shape=(
            jax.ShapeDtypeStruct((rows, outputs), BF16),
            jax.ShapeDtypeStruct((rows, width), BF16),
            jax.ShapeDtypeStruct((width, ranks), F32),
            jax.ShapeDtypeStruct((ranks, outputs), F32),
            jax.ShapeDtypeStruct((experts, width), F32),
            jax.ShapeDtypeStruct((experts,), F32),
            jax.ShapeDtypeStruct((1,), F32),
        ),
        in_specs=[vmem] * 8,
        out_specs=(anywhere,) * 5 + (smem,) * 2,
        scratch_shapes=[
            pltpu.VMEM((width, ranks), F32),
            pltpu.VMEM((ranks, outputs), F32),
            pltpu.VMEM((experts, width), F32),
            pltpu.VMEM((2, rows, 512), BF16),
            pltpu.SemaphoreType.DMA((10,)),
        ],
        compiler_params=pltpu.CompilerParams(vmem_limit_bytes=16 * 1024 * 1024),
        name="finish",
    )(*held)
    return projected, input_grad, down, up, gate.T, load, entropy.reshape(())


def solution(mesh):
    torus = Mesh(mesh.devices.reshape(4, 4, 4, 2), DP)
    return jax.shard_map(
        on_device,
        mesh=torus,
        in_specs=(P(DP), P(DP, None), P(), P(), P(), P(), P(DP, None)),
        out_specs=(P(DP, None), P(DP, None), P(), P(), P(), P(), P()),
        check_vma=False,
    )
```

```python
import functools
import math

import jax
import jax.numpy as jnp
from jax import lax
from jax.experimental import pallas as pl
from jax.experimental.pallas import tpu as pltpu
from jax.sharding import Mesh
from jax.sharding import PartitionSpec as P

AXES = ("dp_0", "dp_1", "dp_2")
CORE = "dp_3"
DP = AXES + (CORE,)
MESH = pl.DeviceIdType.MESH
SIDE = 4
LANES = 128
CHUNK = 256
BF16 = jnp.bfloat16
F32 = jnp.float32


def dot(first, second):
    return jnp.dot(first, second, preferred_element_type=F32)


def right_dot(first, second):
    return lax.dot_general(first, second, (((1,), (1,)), ((), ())), preferred_element_type=F32)


def ring_peer(axis, distance):
    return {axis: lax.rem(lax.axis_index(axis) + distance, SIDE)}


def span(start, size, unit=8):
    return pl.ds(pl.multiple_of(start, unit), size)


class Piece:
    def __init__(self, index, base, rows):
        self.index, self.base, self.rows = index, base, rows
        self.half, self.quarter, self.last = rows // 2, rows // 8, rows // 32
        self.first, self.second, self.third = (AXES[(index + step) % 3] for step in range(3))


class Exchange:
    def __init__(self, part, total, halves, firsts, seconds, thirds, send, recv):
        self.part, self.total = part, total
        self.halves, self.firsts, self.seconds, self.thirds = halves, firsts, seconds, thirds
        self.send, self.recv = send, recv
        self.core = lax.axis_index(CORE)

    def half_at(self, piece, core):
        return piece.base + core * piece.half

    def quarter_at(self, piece, place):
        return self.half_at(piece, self.core) + place * piece.quarter

    def last_at(self, piece, place, second):
        return self.quarter_at(piece, place) + second * piece.last

    def send_to(self, source, target, phase, piece, device):
        pltpu.make_async_remote_copy(
            src_ref=source,
            dst_ref=target,
            send_sem=self.send.at[piece.index],
            recv_sem=self.recv.at[phase, piece.index],
            device_id=device,
            device_id_type=MESH,
        ).start()

    def sent(self, piece, rows):
        here = self.part.at[pl.ds(0, rows)]
        pltpu.make_async_copy(here, here, self.send.at[piece.index]).wait()

    def received(self, phase, piece, rows):
        here = self.part.at[pl.ds(0, rows)]
        pltpu.make_async_copy(here, here, self.recv.at[phase, piece.index]).wait()

    def forward(self, piece, distance):
        place = lax.rem(lax.axis_index(piece.first) + distance, SIDE)
        here = self.total.at[span(self.quarter_at(piece, place), piece.quarter)]
        self.send_to(here, here, 6, piece, {CORE: 1 - self.core})

    def spread_out(self, piece, place):
        here = self.total.at[span(self.last_at(piece, lax.axis_index(piece.first), place), piece.last)]
        for distance in (2, 1, 3):
            self.send_to(here, here, 5, piece, ring_peer(piece.first, distance))
        self.send_to(here, here, 6, piece, {CORE: 1 - self.core})

    def start(self, phase, piece):
        one, two = lax.axis_index(piece.first), lax.axis_index(piece.second)
        if phase == 0:
            source = self.part.at[span(self.half_at(piece, 1 - self.core), piece.half)]
            target = self.halves.at[pl.ds(piece.base // 2, piece.half)]
            self.send_to(source, target, 0, piece, {CORE: 1 - self.core})
            return
        if phase == 1:
            for turn in (1, 2, 3, 0):
                second = lax.rem(two + turn, SIDE)
                for distance in (2, 1, 3):
                    place = lax.rem(one + distance, SIDE)
                    self.send_to(
                        self.part.at[span(self.last_at(piece, place, second), piece.last)],
                        self.firsts.at[distance - 1, span(piece.base // 8 + second * piece.last, piece.last)],
                        7 if turn == 0 else 1,
                        piece,
                        ring_peer(piece.first, distance),
                    )
            return
        if phase == 5:
            for distance in (1, 2, 3):
                self.spread_out(piece, lax.rem(two + distance, SIDE))
            return
        if phase == 6:
            for distance in (1, 2, 3):
                self.forward(piece, distance)
            return
        for distance in (2, 1, 3):
            slot = distance - 1
            if phase == 2:
                place = lax.rem(two + distance, SIDE)
                source = self.part.at[span(self.last_at(piece, one, place), piece.last)]
                target = self.seconds.at[slot, pl.ds(piece.base // 32, piece.last)]
                axis = piece.second
            elif phase == 3:
                source = self.part.at[span(self.last_at(piece, one, two), piece.last)]
                target = self.thirds.at[lax.axis_index(piece.third), pl.ds(piece.base // 32, piece.last)]
                axis = piece.third
            else:
                source = self.total.at[span(self.last_at(piece, one, two), piece.last)]
                target, axis = source, piece.second
            self.send_to(source, target, phase, piece, ring_peer(axis, distance))
        if phase == 4:
            self.spread_out(piece, two)

    def finish(self, phase, piece):
        sent = {0: piece.half, 1: 12 * piece.last, 4: 7 * piece.last, 5: 12 * piece.last, 6: 3 * piece.quarter}
        got_rows = {0: piece.half, 1: 9 * piece.last, 5: 3 * piece.quarter, 6: piece.half}
        self.sent(piece, sent.get(phase, 3 * piece.last))
        self.received(phase, piece, got_rows.get(phase, 3 * piece.last))
        one, two = lax.axis_index(piece.first), lax.axis_index(piece.second)
        if phase == 0:
            here = span(self.half_at(piece, self.core), piece.half)
            self.part[here] = self.part[here] + self.halves[pl.ds(piece.base // 2, piece.half)]
        elif phase == 1:
            for turn in (1, 2, 3):
                self.add_firsts(piece, lax.rem(two + turn, SIDE))
        elif phase == 2:
            self.received(7, piece, 3 * piece.last)
            self.add_firsts(piece, two)
            here = span(self.last_at(piece, one, two), piece.last)
            there = pl.ds(piece.base // 32, piece.last)
            got = self.seconds
            self.part[here] = (self.part[here] + got[0, there]) + (got[1, there] + got[2, there])
        elif phase == 3:
            here = span(self.last_at(piece, one, two), piece.last)
            there = pl.ds(piece.base // 32, piece.last)
            got = self.thirds
            got[lax.axis_index(piece.third), there] = self.part[here]
            self.total[here] = (got[0, there] + got[1, there]) + (got[2, there] + got[3, there])

    def add_firsts(self, piece, second):
        here = span(self.last_at(piece, lax.axis_index(piece.first), second), piece.last)
        there = span(piece.base // 8 + second * piece.last, piece.last)
        got = self.firsts
        self.part[here] = (self.part[here] + got[0, there]) + (got[1, there] + got[2, there])

    def step(self, phase, piece):
        self.finish(phase, piece)
        self.start(phase + 1, piece)


def pair_peer(first, second, size, distance):
    other = lax.rem(lax.axis_index(first) * SIDE + lax.axis_index(second) + distance, size)
    return {first: lax.div(other, SIDE), second: lax.rem(other, SIDE)}


class Statistics:
    def __init__(self, tiles, wide, plane, send, recv):
        self.tiles, self.slots = tiles, (wide, plane)
        self.axes = ((CORE, AXES[2]), (AXES[0], AXES[1]))
        self.send, self.recv = send, recv

    def mine(self, stage):
        first, second = self.axes[stage]
        return lax.axis_index(first) * SIDE + lax.axis_index(second)

    def start(self, stage):
        size = self.slots[stage].shape[0]
        for distance in range(1, size):
            pltpu.make_async_remote_copy(
                src_ref=self.tiles.at[stage],
                dst_ref=self.slots[stage].at[self.mine(stage)],
                send_sem=self.send.at[0],
                recv_sem=self.recv.at[stage],
                device_id=pair_peer(*self.axes[stage], size, distance),
                device_id_type=MESH,
            ).start()

    def finish(self, stage):
        slots = self.slots[stage]
        several = slots.at[pl.ds(0, slots.shape[0] - 1)]
        pltpu.make_async_copy(several, several, self.send.at[0]).wait()
        pltpu.make_async_copy(several, several, self.recv.at[stage]).wait()
        slots[self.mine(stage)] = self.tiles[stage]
        total = slots[0]
        for place in range(1, slots.shape[0]):
            total = total + slots[place]
        self.tiles[stage + 1] = total


class GateExchange:
    def __init__(self, base, rows, part, total, inward, rings, send, recv):
        self.base, self.share = base, rows // 8
        self.part, self.total = part, total
        self.inward, self.rings = inward, rings
        self.send, self.recv = send, recv
        self.group = lax.axis_index(CORE) * SIDE + lax.axis_index(AXES[0])

    def chunk(self, place):
        return span(self.base + place * self.share, self.share)

    def start(self, stage):
        mine = self.chunk(self.group)
        for distance in range(1, SIDE if stage in (1, 2) else 8):
            if stage in (1, 2):
                device = ring_peer(AXES[stage], distance)
                source, target = self.part.at[mine], self.rings.at[stage - 1, lax.axis_index(AXES[stage])]
            else:
                other = lax.rem(self.group + distance, 8)
                device = {CORE: lax.div(other, SIDE), AXES[0]: lax.rem(other, SIDE)}
                if stage == 0:
                    source, target = self.part.at[self.chunk(other)], self.inward.at[distance - 1]
                else:
                    source = self.total.at[mine]
                    target = source
            pltpu.make_async_remote_copy(
                src_ref=source,
                dst_ref=target,
                send_sem=self.send.at[3],
                recv_sem=self.recv.at[stage],
                device_id=device,
                device_id_type=MESH,
            ).start()

    def finish(self, stage):
        several = self.inward.at[pl.ds(0, 3 if stage in (1, 2) else 7)]
        pltpu.make_async_copy(several, several, self.send.at[3]).wait()
        pltpu.make_async_copy(several, several, self.recv.at[stage]).wait()
        mine = self.chunk(self.group)
        if stage == 0:
            value = self.part[mine]
            for slot in range(7):
                value = value + self.inward[slot]
            self.part[mine] = value
        elif stage < 3:
            self.rings[stage - 1, lax.axis_index(AXES[stage])] = self.part[mine]
            value = self.rings[stage - 1, 0]
            for slot in range(1, SIDE):
                value = value + self.rings[stage - 1, slot]
            if stage == 1:
                self.part[mine] = value
            else:
                self.total[mine] = value

    def step(self, stage):
        self.finish(stage)
        self.start(stage + 1)


def peers():
    core = lax.axis_index(CORE)
    found = [{CORE: 1 - core}]
    for distance in (1, 2, 3):
        for axis in (AXES[0], AXES[2]):
            found.append({CORE: 1 - core, **ring_peer(axis, distance)})
        found.append(ring_peer(AXES[2], distance))
    found += [pair_peer(AXES[0], AXES[1], 16, distance) for distance in range(1, 16)]
    return found


def kernel(
    sizes,
    ids_hbm, tokens_hbm, frozen_hbm, down_hbm, up_hbm, gate_hbm, upstream_hbm,
    projected_ref, input_ref, total, tiles, frozen, sides, masked, grads,
    ids, tokens, up, gate,
    both, low, prob, plain, turned, weighted, grads_t, weighted_t, gate_t,
    part, halves, firsts, seconds, thirds, wide, plane, inward, rings,
    load_sem, token_sem, send, recv, stat_send, stat_recv, gate_recv,
):
    rows, width, outputs, ranks, experts = sizes
    rank = ranks // experts
    scale = 1.0 / rank
    chunks = rows // CHUNK
    up_base = width
    gate_base = width + outputs
    pieces = (Piece(0, 0, 1792), Piece(1, 1792, 1792), Piece(2, 3584, gate_base - 3584))
    exchange = Exchange(part, total, halves, firsts, seconds, thirds, send, recv)
    statistics = Statistics(tiles, wide, plane, stat_send, stat_recv)
    gates = GateExchange(gate_base, width * experts // LANES, part, total, inward, rings, send, gate_recv)

    gate_load = pltpu.make_async_copy(gate_hbm, gate, load_sem.at[0])
    ids_load = pltpu.make_async_copy(ids_hbm, ids, load_sem.at[1])
    gate_load.start()
    ids_load.start()
    barrier = pltpu.get_barrier_semaphore()
    greeted = peers()
    for peer in greeted:
        pl.semaphore_signal(barrier, inc=1, device_id=peer, device_id_type=MESH)

    def load(source, target, slot):
        return pltpu.make_async_copy(source, target, load_sem.at[slot])

    def chunk_load(chunk):
        here = span(chunk * CHUNK, CHUNK, CHUNK)
        return (
            pltpu.make_async_copy(tokens_hbm.at[here], tokens.at[here], token_sem.at[chunk, 0]),
            pltpu.make_async_copy(upstream_hbm.at[here], masked.at[here], token_sem.at[chunk, 1]),
        )

    down_load = load(down_hbm, sides.at[:, pl.ds(0, ranks)], 2)
    up_load = load(up_hbm, up, 3)
    frozen_load = load(frozen_hbm, frozen, 4)
    down_load.start()
    chunk_load(0)[0].start()
    up_load.start()
    chunk_load(0)[1].start()

    gate_load.wait()
    for copy in chunk_load(1):
        copy.start()

    @pl.loop(0, width // 512)
    def _(block):
        here = span(block * 512, 512, 512)
        row = gate[:, here].astype(F32)
        tall = jnp.concatenate([jnp.broadcast_to(row[e : e + 1], (rank, 512)) for e in range(experts)], axis=0)
        sides[here, ranks : 2 * ranks] = tall.T.astype(BF16)

    ids_load.wait()
    live_rows = jnp.sum(jnp.sum((ids[...] != 0).astype(F32), axis=1, keepdims=True), axis=0, keepdims=True)

    def live_of(chunk):
        row = lax.broadcasted_iota(jnp.int32, (CHUNK, LANES), 0) + chunk * CHUNK
        return (row.astype(F32) < live_rows).astype(F32)

    def lane_sum(value):
        return jnp.sum(value, axis=1, keepdims=True)

    tiles[0] = jnp.zeros((8, LANES), F32)
    down_load.wait()

    def spread(chunk):
        here = span(chunk * CHUNK, CHUNK, CHUNK)
        slot = chunk % 2
        below = both[slot, :, :ranks].astype(BF16)
        logits = both[slot, :, ranks:]
        shifted = logits - jnp.max(logits, axis=1, keepdims=True)
        raised = jnp.exp(shifted)
        mass = lane_sum(raised) * scale
        share = raised / mass
        logp = shifted - jnp.log(mass)
        entropy = -lane_sum(share * logp) * scale
        alive = live_of(chunk)
        low[here] = below
        prob[here] = share
        plain[here] = 50.0 * alive * share * (logp + entropy)
        tiles[0, 0:1] += jnp.sum(alive * share, axis=0, keepdims=True)
        tiles[0, 1:2] += jnp.sum(alive * entropy, axis=0, keepdims=True)
        tiles[0, 2:3] += jnp.sum(alive, axis=0, keepdims=True)
        mine = jnp.where(alive[:, 0:1] > 0.0, masked[here].astype(F32), 0.0).astype(BF16)
        masked[here] = mine
        back = right_dot(mine, up[...])
        heavy = (below.astype(F32) * share).astype(BF16).astype(F32) * 2.0
        steep = (2.0 * share * back).astype(BF16)
        turned[here] = back
        weighted[here] = heavy.astype(BF16)
        grads[here, 0:ranks] = steep
        grads_t[:, here] = steep.astype(F32).T.astype(BF16)
        weighted_t[:, here] = heavy.T.astype(BF16)

    for copy in chunk_load(2):
        copy.start()
    chunk_load(0)[0].wait()
    for copy in chunk_load(3):
        copy.start()
    both[0] = dot(tokens[0:CHUNK], sides[...])
    up_load.wait()

    @pl.loop(1, chunks)
    def _(chunk):
        chunk_load(chunk - 1)[1].wait()
        chunk_load(chunk)[0].wait()
        spread(chunk - 1)
        both[chunk % 2] = dot(tokens[span(chunk * CHUNK, CHUNK, CHUNK)], sides[...])

    frozen_load.start()
    chunk_load(chunks - 1)[1].wait()
    spread(chunks - 1)
    pl.semaphore_wait(barrier, len(greeted))
    statistics.start(0)

    def down_block(start, size):
        here = pl.ds(start, size)
        part[here] = dot(grads_t[...], tokens[:, here]).T

    down_block(0, 896)
    down_block(896, 896)
    exchange.start(0, pieces[0])
    down_block(1792, 896)
    down_block(2688, 896)
    exchange.start(0, pieces[1])
    down_block(3584, 512)
    found = dot(weighted_t[...], masked[...])
    for block in range(outputs // LANES):
        part[up_base + block * LANES : up_base + (block + 1) * LANES] = found[:, block * LANES : (block + 1) * LANES]
    exchange.start(0, pieces[2])
    statistics.finish(0)
    statistics.start(1)
    exchange.step(0, pieces[0])
    group = lax.broadcasted_iota(jnp.int32, (2 * ranks, ranks), 0) % ranks // rank
    member = lax.broadcasted_iota(jnp.int32, (2 * ranks, ranks), 1) // rank
    blocks = (group == member).astype(F32).astype(BF16)

    def task_part(chunk):
        here = span(chunk * CHUNK, CHUNK, CHUNK)
        share = prob[here]
        product = low[here].astype(F32) * turned[here]
        upper = product.astype(BF16)
        lower = (product - upper.astype(F32)).astype(BF16)
        task = 2.0 * dot(jnp.concatenate([upper, lower], axis=1), blocks)
        plain[here] += share * (task - lane_sum(share * task) * scale)

    task_part(0)
    task_part(1)
    exchange.step(0, pieces[1])
    task_part(2)
    task_part(3)
    exchange.step(0, pieces[2])
    lane = lax.broadcasted_iota(jnp.int32, (CHUNK, LANES), 1)
    pick_from = lax.broadcasted_iota(jnp.int32, (ranks, ranks), 0)
    pick_to = lax.broadcasted_iota(jnp.int32, (ranks, ranks), 1)
    pick = (pick_from == (pick_to % experts) * rank + pick_to // experts).astype(F32)
    pick = jnp.where(pick_to < 2 * experts, pick, 0.0).astype(BF16)

    def slope_part(chunk):
        load_all, live_all = tiles[2, 0:1], tiles[2, 2:3]
        push = (2.0 * experts * 100.0) / live_all
        here = span(chunk * CHUNK, CHUNK, CHUNK)
        share = prob[here]
        slope = share * (load_all - lane_sum(share * load_all) * scale)
        whole = plain[here] + push * live_of(chunk) * slope
        upper = whole.astype(BF16).astype(F32)
        place = lane % rank
        packed = jnp.where(place == 0, upper, jnp.where(place == 1, whole - upper, 0.0)).astype(BF16)
        grads[here, ranks : 2 * ranks] = packed
        gate_t[:, here] = dot(packed, pick).T[: 2 * experts].astype(BF16)

    def base_block(block):
        tall = span((block % 2) * (rows // 2), rows // 2, rows // 2)
        here = span((block // 2) * 256, 256, 256)
        found = dot(tokens[tall], frozen[:, here]) + dot(weighted[tall], up[:, here])
        projected_ref[tall, here] = found.astype(BF16)

    def step_all(phase):
        for piece in pieces[:3]:
            exchange.step(phase, piece)

    def at(block, place):
        return pl.when(block == place)

    frozen_load.wait()

    @pl.loop(0, 3)
    def _(block):
        base_block(block)

    statistics.finish(1)

    @pl.loop(3, 5)
    def _(block):
        @at(block, 4)
        def _():
            exchange.step(1, pieces[0])

        slope_part(2 * block - 6)
        slope_part(2 * block - 5)
        base_block(block)

    exchange.step(1, pieces[1])
    exchange.step(1, pieces[2])

    @pl.loop(0, width // 1024)
    def _(block):
        found = dot(gate_t[...], tokens[:, span(block * 1024, 1024, 1024)])
        found = found[:experts] + found[experts:]
        for piece in range(8):
            here = span(gate_base + (block * 8 + piece) * experts, experts)
            part[here] = found[:, piece * LANES : (piece + 1) * LANES]

    gates.start(0)

    @pl.loop(5, 8)
    def _(block):
        @at(block, 6)
        def _():
            exchange.step(2, pieces[0])

        @at(block, 7)
        def _():
            exchange.step(2, pieces[1])
            exchange.step(2, pieces[2])

        base_block(block)

    @pl.loop(0, input_ref.shape[1] // 512)
    def _(block):
        @at(block, 0)
        def _():
            gates.step(0)

        @at(block, 1)
        def _():
            exchange.step(3, pieces[0])

        @at(block, 2)
        def _():
            gates.step(1)
            exchange.step(3, pieces[1])
            exchange.step(3, pieces[2])

        @at(block, 3)
        def _():
            exchange.step(4, pieces[0])

        @at(block, 4)
        def _():
            gates.step(2)
            exchange.step(4, pieces[1])
            exchange.step(4, pieces[2])

        here = span(block * 512, 512, 512)
        found = right_dot(masked[...], frozen[here]) + right_dot(grads[...], sides[here])
        input_ref[:, here] = found.astype(BF16)

    for piece in pieces:
        exchange.step(5, piece)
    gates.finish(3)
    for piece in pieces:
        exchange.finish(6, piece)


def finish_kernel(
    sizes,
    projected, inputs, total, tiles, frozen, sides, masked, grads,
    projected_hbm, input_hbm, down_hbm, up_hbm, gate_hbm, load_ref, entropy_ref,
    scaled, up, gate, rest, sems,
):
    width, outputs, ranks, experts = sizes
    rank = ranks // experts
    every = total.shape[0]
    quarter = width // 4
    copies = [
        pltpu.make_async_copy(inputs, input_hbm.at[:, pl.ds(0, inputs.shape[1])], sems.at[0]),
        pltpu.make_async_copy(projected, projected_hbm, sems.at[1]),
    ]
    for copy in copies:
        copy.start()

    def add_squares(block, found):
        value = total[span(block * 192, 192)]
        return found + jnp.sum((value * value).reshape(6, 32, LANES), axis=0)

    squares = lax.fori_loop(0, every // 192, add_squares, jnp.zeros((32, LANES), F32))
    norm = jnp.sqrt(jnp.sum(jnp.sum(squares, axis=1, keepdims=True), axis=0, keepdims=True))
    factor = jnp.minimum(1.0, math.sqrt(every * LANES) / norm)
    for block in range(4):
        here = pl.ds(block * quarter, quarter)
        scaled[here] = total[here] * factor
        copy = pltpu.make_async_copy(scaled.at[here], down_hbm.at[here], sems.at[2 + block])
        copy.start()
        copies.append(copy)
    for block in range(outputs // LANES):
        here = width + block * LANES
        up[:, block * LANES : (block + 1) * LANES] = total[here : here + LANES] * factor
    copy = pltpu.make_async_copy(up, up_hbm, sems.at[6])
    copy.start()
    copies.append(copy)
    for block in range(width // LANES):
        here = width + outputs + block * experts
        gate[:, block * LANES : (block + 1) * LANES] = total[here : here + experts] * factor
    copy = pltpu.make_async_copy(gate, gate_hbm, sems.at[7])
    copy.start()
    copies.append(copy)
    for block in range(2):
        here = pl.ds(inputs.shape[1] + block * 512, 512)
        found = right_dot(masked[...], frozen[here]) + right_dot(grads[...], sides[here])
        rest[block] = found.astype(BF16)
        copy = pltpu.make_async_copy(rest.at[block], input_hbm.at[:, here], sems.at[8 + block])
        copy.start()
        copies.append(copy)
    mean = tiles[2] / tiles[2, 2:3]
    lane = lax.broadcasted_iota(jnp.int32, (1, LANES), 1)
    for expert in range(experts):
        load_ref[expert] = jnp.sum(jnp.where(lane == expert * rank, mean[0:1], 0.0))
    entropy_ref[0] = jnp.sum(jnp.where(lane == 0, mean[1:2], 0.0))
    for copy in copies:
        copy.wait()


def on_device(token_ids, tokens, frozen_weight, adapter_down, adapter_up, gate_weight, upstream):
    rows, width = tokens.shape
    ranks, outputs = adapter_up.shape
    experts = gate_weight.shape[1]
    every = width + outputs + width * experts // LANES
    anywhere = pl.BlockSpec(memory_space=pl.ANY)
    hbm = pl.BlockSpec(memory_space=pltpu.HBM)
    vmem = pl.BlockSpec(memory_space=pltpu.VMEM)
    smem = pl.BlockSpec(memory_space=pltpu.SMEM)
    held = pl.pallas_call(
        functools.partial(kernel, (rows, width, outputs, ranks, experts)),
        out_shape=(
            pltpu.VMEM((rows, outputs), BF16),
            pltpu.VMEM((rows, width - 1024), BF16),
            pltpu.VMEM((every, LANES), F32),
            pltpu.VMEM((3, 8, LANES), F32),
            pltpu.VMEM((width, outputs), BF16),
            pltpu.VMEM((width, 2 * ranks), BF16),
            pltpu.VMEM((rows, outputs), BF16),
            pltpu.VMEM((rows, 2 * ranks), BF16),
        ),
        in_specs=[hbm] * 7,
        out_specs=(vmem,) * 8,
        scratch_shapes=[
            pltpu.VMEM((rows // LANES, LANES), jnp.int32),
            pltpu.VMEM((rows, width), BF16),
            pltpu.VMEM((ranks, outputs), BF16),
            pltpu.VMEM((experts, width), BF16),
            pltpu.VMEM((2, CHUNK, 2 * ranks), F32),
            pltpu.VMEM((rows, ranks), BF16),
            pltpu.VMEM((rows, ranks), F32),
            pltpu.VMEM((rows, ranks), F32),
            pltpu.VMEM((rows, ranks), F32),
            pltpu.VMEM((rows, ranks), BF16),
            pltpu.VMEM((ranks, rows), BF16),
            pltpu.VMEM((ranks, rows), BF16),
            pltpu.VMEM((2 * experts, rows), BF16),
            pltpu.VMEM((every, LANES), F32),
            pltpu.VMEM((every // 2, LANES), F32),
            pltpu.VMEM((3, every // 8, LANES), F32),
            pltpu.VMEM((3, every // 32, LANES), F32),
            pltpu.VMEM((4, every // 32, LANES), F32),
            pltpu.VMEM((8, 8, LANES), F32),
            pltpu.VMEM((16, 8, LANES), F32),
            pltpu.VMEM((7, width * experts // LANES // 8, LANES), F32),
            pltpu.VMEM((2, SIDE, width * experts // LANES // 8, LANES), F32),
            pltpu.SemaphoreType.DMA((5,)),
            pltpu.SemaphoreType.DMA((rows // CHUNK, 2)),
            pltpu.SemaphoreType.DMA((4,)),
            pltpu.SemaphoreType.DMA((8, 3)),
            pltpu.SemaphoreType.DMA((1,)),
            pltpu.SemaphoreType.DMA((2,)),
            pltpu.SemaphoreType.DMA((4,)),
        ],
        compiler_params=pltpu.CompilerParams(
            collective_id=0, has_side_effects=True, vmem_limit_bytes=34 * 1024 * 1024
        ),
        name="step",
    )(token_ids.reshape(rows // LANES, LANES), tokens, frozen_weight, adapter_down, adapter_up, gate_weight.T, upstream)
    projected, input_grad, down, up, gate, load, entropy = pl.pallas_call(
        functools.partial(finish_kernel, (width, outputs, ranks, experts)),
        out_shape=(
            jax.ShapeDtypeStruct((rows, outputs), BF16),
            jax.ShapeDtypeStruct((rows, width), BF16),
            jax.ShapeDtypeStruct((width, ranks), F32),
            jax.ShapeDtypeStruct((ranks, outputs), F32),
            jax.ShapeDtypeStruct((experts, width), F32),
            jax.ShapeDtypeStruct((experts,), F32),
            jax.ShapeDtypeStruct((1,), F32),
        ),
        in_specs=[vmem] * 8,
        out_specs=(anywhere,) * 5 + (smem,) * 2,
        scratch_shapes=[
            pltpu.VMEM((width, ranks), F32),
            pltpu.VMEM((ranks, outputs), F32),
            pltpu.VMEM((experts, width), F32),
            pltpu.VMEM((2, rows, 512), BF16),
            pltpu.SemaphoreType.DMA((10,)),
        ],
        compiler_params=pltpu.CompilerParams(vmem_limit_bytes=16 * 1024 * 1024),
        name="finish",
    )(*held)
    return projected, input_grad, down, up, gate.T, load, entropy.reshape(())


def solution(mesh):
    torus = Mesh(mesh.devices.reshape(4, 4, 4, 2), DP)
    return jax.shard_map(
        on_device,
        mesh=torus,
        in_specs=(P(DP), P(DP, None), P(), P(), P(), P(), P(DP, None)),
        out_specs=(P(DP, None), P(DP, None), P(), P(), P(), P(), P()),
        check_vma=False,
    )
```

```python
import functools
import math

import jax
import jax.numpy as jnp
from jax import lax
from jax.experimental import pallas as pl
from jax.experimental.pallas import tpu as pltpu
from jax.sharding import Mesh
from jax.sharding import PartitionSpec as P

AXES = ("dp_0", "dp_1", "dp_2")
CORE = "dp_3"
DP = AXES + (CORE,)
MESH = pl.DeviceIdType.MESH
SIDE = 4
LANES = 128
CHUNK = 256
BF16 = jnp.bfloat16
F32 = jnp.float32


def dot(first, second):
    return jnp.dot(first, second, preferred_element_type=F32)


def right_dot(first, second):
    return lax.dot_general(first, second, (((1,), (1,)), ((), ())), preferred_element_type=F32)


def ring_peer(axis, distance):
    return {axis: lax.rem(lax.axis_index(axis) + distance, SIDE)}


def span(start, size, unit=8):
    return pl.ds(pl.multiple_of(start, unit), size)


class Piece:
    def __init__(self, index, base, rows):
        self.index, self.base, self.rows = index, base, rows
        self.half, self.quarter, self.last = rows // 2, rows // 8, rows // 32
        self.first, self.second, self.third = (AXES[(index + step) % 3] for step in range(3))


class Exchange:
    def __init__(self, part, total, halves, firsts, seconds, thirds, send, recv):
        self.part, self.total = part, total
        self.halves, self.firsts, self.seconds, self.thirds = halves, firsts, seconds, thirds
        self.send, self.recv = send, recv
        self.core = lax.axis_index(CORE)

    def half_at(self, piece, core):
        return piece.base + core * piece.half

    def quarter_at(self, piece, place):
        return self.half_at(piece, self.core) + place * piece.quarter

    def last_at(self, piece, place, second):
        return self.quarter_at(piece, place) + second * piece.last

    def send_to(self, source, target, phase, piece, device):
        pltpu.make_async_remote_copy(
            src_ref=source,
            dst_ref=target,
            send_sem=self.send.at[piece.index],
            recv_sem=self.recv.at[phase, piece.index],
            device_id=device,
            device_id_type=MESH,
        ).start()

    def sent(self, piece, rows):
        here = self.part.at[pl.ds(0, rows)]
        pltpu.make_async_copy(here, here, self.send.at[piece.index]).wait()

    def received(self, phase, piece, rows):
        here = self.part.at[pl.ds(0, rows)]
        pltpu.make_async_copy(here, here, self.recv.at[phase, piece.index]).wait()

    def forward(self, piece, distance):
        place = lax.rem(lax.axis_index(piece.first) + distance, SIDE)
        here = self.total.at[span(self.quarter_at(piece, place), piece.quarter)]
        self.send_to(here, here, 6, piece, {CORE: 1 - self.core})

    def spread_out(self, piece, place):
        here = self.total.at[span(self.last_at(piece, lax.axis_index(piece.first), place), piece.last)]
        for distance in (2, 1, 3):
            self.send_to(here, here, 5, piece, ring_peer(piece.first, distance))
        self.send_to(here, here, 6, piece, {CORE: 1 - self.core})

    def start(self, phase, piece):
        one, two = lax.axis_index(piece.first), lax.axis_index(piece.second)
        if phase == 0:
            source = self.part.at[span(self.half_at(piece, 1 - self.core), piece.half)]
            target = self.halves.at[pl.ds(piece.base // 2, piece.half)]
            self.send_to(source, target, 0, piece, {CORE: 1 - self.core})
            return
        if phase == 1:
            for turn in (1, 2, 3, 0):
                second = lax.rem(two + turn, SIDE)
                for distance in (2, 1, 3):
                    place = lax.rem(one + distance, SIDE)
                    self.send_to(
                        self.part.at[span(self.last_at(piece, place, second), piece.last)],
                        self.firsts.at[distance - 1, span(piece.base // 8 + second * piece.last, piece.last)],
                        7 if turn == 0 else 1,
                        piece,
                        ring_peer(piece.first, distance),
                    )
            return
        if phase == 5:
            for distance in (1, 2, 3):
                self.spread_out(piece, lax.rem(two + distance, SIDE))
            return
        if phase == 6:
            for distance in (1, 2, 3):
                self.forward(piece, distance)
            return
        for distance in (2, 1, 3):
            slot = distance - 1
            if phase == 2:
                place = lax.rem(two + distance, SIDE)
                source = self.part.at[span(self.last_at(piece, one, place), piece.last)]
                target = self.seconds.at[slot, pl.ds(piece.base // 32, piece.last)]
                axis = piece.second
            elif phase == 3:
                source = self.part.at[span(self.last_at(piece, one, two), piece.last)]
                target = self.thirds.at[lax.axis_index(piece.third), pl.ds(piece.base // 32, piece.last)]
                axis = piece.third
            else:
                source = self.total.at[span(self.last_at(piece, one, two), piece.last)]
                target, axis = source, piece.second
            self.send_to(source, target, phase, piece, ring_peer(axis, distance))
        if phase == 4:
            self.spread_out(piece, two)

    def finish(self, phase, piece):
        sent = {0: piece.half, 1: 12 * piece.last, 4: 7 * piece.last, 5: 12 * piece.last, 6: 3 * piece.quarter}
        got_rows = {0: piece.half, 1: 9 * piece.last, 5: 3 * piece.quarter, 6: piece.half}
        self.sent(piece, sent.get(phase, 3 * piece.last))
        self.received(phase, piece, got_rows.get(phase, 3 * piece.last))
        one, two = lax.axis_index(piece.first), lax.axis_index(piece.second)
        if phase == 0:
            here = span(self.half_at(piece, self.core), piece.half)
            self.part[here] = self.part[here] + self.halves[pl.ds(piece.base // 2, piece.half)]
        elif phase == 1:
            for turn in (1, 2, 3):
                self.add_firsts(piece, lax.rem(two + turn, SIDE))
        elif phase == 2:
            self.received(7, piece, 3 * piece.last)
            self.add_firsts(piece, two)
            here = span(self.last_at(piece, one, two), piece.last)
            there = pl.ds(piece.base // 32, piece.last)
            got = self.seconds
            self.part[here] = (self.part[here] + got[0, there]) + (got[1, there] + got[2, there])
        elif phase == 3:
            here = span(self.last_at(piece, one, two), piece.last)
            there = pl.ds(piece.base // 32, piece.last)
            got = self.thirds
            got[lax.axis_index(piece.third), there] = self.part[here]
            self.total[here] = (got[0, there] + got[1, there]) + (got[2, there] + got[3, there])

    def add_firsts(self, piece, second):
        here = span(self.last_at(piece, lax.axis_index(piece.first), second), piece.last)
        there = span(piece.base // 8 + second * piece.last, piece.last)
        got = self.firsts
        self.part[here] = (self.part[here] + got[0, there]) + (got[1, there] + got[2, there])

    def step(self, phase, piece):
        self.finish(phase, piece)
        self.start(phase + 1, piece)


def pair_peer(first, second, size, distance):
    other = lax.rem(lax.axis_index(first) * SIDE + lax.axis_index(second) + distance, size)
    return {first: lax.div(other, SIDE), second: lax.rem(other, SIDE)}


class Statistics:
    def __init__(self, tiles, wide, plane, send, recv):
        self.tiles, self.slots = tiles, (wide, plane)
        self.axes = ((CORE, AXES[2]), (AXES[0], AXES[1]))
        self.send, self.recv = send, recv

    def mine(self, stage):
        first, second = self.axes[stage]
        return lax.axis_index(first) * SIDE + lax.axis_index(second)

    def start(self, stage):
        size = self.slots[stage].shape[0]
        for distance in range(1, size):
            pltpu.make_async_remote_copy(
                src_ref=self.tiles.at[stage],
                dst_ref=self.slots[stage].at[self.mine(stage)],
                send_sem=self.send.at[0],
                recv_sem=self.recv.at[stage],
                device_id=pair_peer(*self.axes[stage], size, distance),
                device_id_type=MESH,
            ).start()

    def finish(self, stage):
        slots = self.slots[stage]
        several = slots.at[pl.ds(0, slots.shape[0] - 1)]
        pltpu.make_async_copy(several, several, self.send.at[0]).wait()
        pltpu.make_async_copy(several, several, self.recv.at[stage]).wait()
        slots[self.mine(stage)] = self.tiles[stage]
        total = slots[0]
        for place in range(1, slots.shape[0]):
            total = total + slots[place]
        self.tiles[stage + 1] = total


class GateExchange:
    def __init__(self, base, rows, part, total, inward, rings, send, recv):
        self.base, self.share = base, rows // 8
        self.part, self.total = part, total
        self.inward, self.rings = inward, rings
        self.send, self.recv = send, recv
        self.group = lax.axis_index(CORE) * SIDE + lax.axis_index(AXES[0])

    def chunk(self, place):
        return span(self.base + place * self.share, self.share)

    def start(self, stage):
        mine = self.chunk(self.group)
        for distance in range(1, SIDE if stage in (1, 2) else 8):
            if stage in (1, 2):
                device = ring_peer(AXES[stage], distance)
                source, target = self.part.at[mine], self.rings.at[stage - 1, lax.axis_index(AXES[stage])]
            else:
                other = lax.rem(self.group + distance, 8)
                device = {CORE: lax.div(other, SIDE), AXES[0]: lax.rem(other, SIDE)}
                if stage == 0:
                    source, target = self.part.at[self.chunk(other)], self.inward.at[distance - 1]
                else:
                    source = self.total.at[mine]
                    target = source
            pltpu.make_async_remote_copy(
                src_ref=source,
                dst_ref=target,
                send_sem=self.send.at[3],
                recv_sem=self.recv.at[stage],
                device_id=device,
                device_id_type=MESH,
            ).start()

    def finish(self, stage):
        several = self.inward.at[pl.ds(0, 3 if stage in (1, 2) else 7)]
        pltpu.make_async_copy(several, several, self.send.at[3]).wait()
        pltpu.make_async_copy(several, several, self.recv.at[stage]).wait()
        mine = self.chunk(self.group)
        if stage == 0:
            value = self.part[mine]
            for slot in range(7):
                value = value + self.inward[slot]
            self.part[mine] = value
        elif stage < 3:
            self.rings[stage - 1, lax.axis_index(AXES[stage])] = self.part[mine]
            value = self.rings[stage - 1, 0]
            for slot in range(1, SIDE):
                value = value + self.rings[stage - 1, slot]
            if stage == 1:
                self.part[mine] = value
            else:
                self.total[mine] = value

    def step(self, stage):
        self.finish(stage)
        self.start(stage + 1)


def peers():
    core = lax.axis_index(CORE)
    found = [{CORE: 1 - core}]
    for distance in (1, 2, 3):
        for axis in (AXES[0], AXES[2]):
            found.append({CORE: 1 - core, **ring_peer(axis, distance)})
        found.append(ring_peer(AXES[2], distance))
    found += [pair_peer(AXES[0], AXES[1], 16, distance) for distance in range(1, 16)]
    return found


def kernel(
    sizes,
    ids_hbm, tokens_hbm, frozen_hbm, down_hbm, up_hbm, gate_hbm, upstream_hbm,
    projected_ref, input_ref, total, tiles, frozen, sides, masked, grads,
    ids, tokens, up, gate,
    both, low, prob, plain, turned, weighted, grads_t, weighted_t, gate_t,
    part, halves, firsts, seconds, thirds, wide, plane, inward, rings,
    load_sem, token_sem, send, recv, stat_send, stat_recv, gate_recv,
):
    rows, width, outputs, ranks, experts = sizes
    rank = ranks // experts
    scale = 1.0 / rank
    chunks = rows // CHUNK
    up_base = width
    gate_base = width + outputs
    pieces = (Piece(0, 0, 1792), Piece(1, 1792, 1792), Piece(2, 3584, gate_base - 3584))
    exchange = Exchange(part, total, halves, firsts, seconds, thirds, send, recv)
    statistics = Statistics(tiles, wide, plane, stat_send, stat_recv)
    gates = GateExchange(gate_base, width * experts // LANES, part, total, inward, rings, send, gate_recv)

    gate_load = pltpu.make_async_copy(gate_hbm, gate, load_sem.at[0])
    ids_load = pltpu.make_async_copy(ids_hbm, ids, load_sem.at[1])
    gate_load.start()
    ids_load.start()
    def load(source, target, slot):
        return pltpu.make_async_copy(source, target, load_sem.at[slot])

    def chunk_load(chunk):
        here = span(chunk * CHUNK, CHUNK, CHUNK)
        return (
            pltpu.make_async_copy(tokens_hbm.at[here], tokens.at[here], token_sem.at[chunk, 0]),
            pltpu.make_async_copy(upstream_hbm.at[here], masked.at[here], token_sem.at[chunk, 1]),
        )

    down_load = load(down_hbm, sides.at[:, pl.ds(0, ranks)], 2)
    up_load = load(up_hbm, up, 3)
    frozen_load = load(frozen_hbm, frozen, 4)
    down_load.start()
    chunk_load(0)[0].start()
    up_load.start()
    chunk_load(0)[1].start()
    barrier = pltpu.get_barrier_semaphore()
    greeted = peers()
    for peer in greeted:
        pl.semaphore_signal(barrier, inc=1, device_id=peer, device_id_type=MESH)

    gate_load.wait()
    for copy in chunk_load(1):
        copy.start()

    @pl.loop(0, width // 512)
    def _(block):
        here = span(block * 512, 512, 512)
        row = gate[:, here].astype(F32)
        tall = jnp.concatenate([jnp.broadcast_to(row[e : e + 1], (rank, 512)) for e in range(experts)], axis=0)
        sides[here, ranks : 2 * ranks] = tall.T.astype(BF16)

    ids_load.wait()
    live_rows = jnp.sum(jnp.sum((ids[...] != 0).astype(F32), axis=1, keepdims=True), axis=0, keepdims=True)

    def live_of(chunk):
        row = lax.broadcasted_iota(jnp.int32, (CHUNK, LANES), 0) + chunk * CHUNK
        return (row.astype(F32) < live_rows).astype(F32)

    def lane_sum(value):
        return jnp.sum(value, axis=1, keepdims=True)

    tiles[0] = jnp.zeros((8, LANES), F32)
    down_load.wait()

    def spread(chunk):
        here = span(chunk * CHUNK, CHUNK, CHUNK)
        slot = chunk % 2
        below = both[slot, :, :ranks].astype(BF16)
        logits = both[slot, :, ranks:]
        shifted = logits - jnp.max(logits, axis=1, keepdims=True)
        raised = jnp.exp(shifted)
        mass = lane_sum(raised) * scale
        share = raised / mass
        logp = shifted - jnp.log(mass)
        entropy = -lane_sum(share * logp) * scale
        alive = live_of(chunk)
        low[here] = below
        prob[here] = share
        plain[here] = 50.0 * alive * share * (logp + entropy)
        tiles[0, 0:1] += jnp.sum(alive * share, axis=0, keepdims=True)
        tiles[0, 1:2] += jnp.sum(alive * entropy, axis=0, keepdims=True)
        tiles[0, 2:3] += jnp.sum(alive, axis=0, keepdims=True)
        mine = jnp.where(alive[:, 0:1] > 0.0, masked[here].astype(F32), 0.0).astype(BF16)
        masked[here] = mine
        back = right_dot(mine, up[...])
        heavy = (below.astype(F32) * share).astype(BF16).astype(F32) * 2.0
        steep = (2.0 * share * back).astype(BF16)
        turned[here] = back
        weighted[here] = heavy.astype(BF16)
        grads[here, 0:ranks] = steep
        grads_t[:, here] = steep.astype(F32).T.astype(BF16)
        weighted_t[:, here] = heavy.T.astype(BF16)

    for copy in chunk_load(2):
        copy.start()
    chunk_load(0)[0].wait()
    for copy in chunk_load(3):
        copy.start()
    both[0] = dot(tokens[0:CHUNK], sides[...])
    up_load.wait()

    @pl.loop(1, chunks)
    def _(chunk):
        chunk_load(chunk - 1)[1].wait()
        chunk_load(chunk)[0].wait()
        spread(chunk - 1)
        both[chunk % 2] = dot(tokens[span(chunk * CHUNK, CHUNK, CHUNK)], sides[...])

    frozen_load.start()
    chunk_load(chunks - 1)[1].wait()
    spread(chunks - 1)
    pl.semaphore_wait(barrier, len(greeted))
    statistics.start(0)

    def down_block(start, size):
        found = dot(grads_t[...], tokens[:, pl.ds(start, size)])
        for block in range(size // LANES):
            here = start + block * LANES
            part[here : here + LANES] = found[:, block * LANES : (block + 1) * LANES]

    down_block(0, 896)
    down_block(896, 896)
    exchange.start(0, pieces[0])
    down_block(1792, 896)
    down_block(2688, 896)
    exchange.start(0, pieces[1])
    down_block(3584, 512)
    found = dot(weighted_t[...], masked[...])
    for block in range(outputs // LANES):
        part[up_base + block * LANES : up_base + (block + 1) * LANES] = found[:, block * LANES : (block + 1) * LANES]
    exchange.start(0, pieces[2])
    statistics.finish(0)
    statistics.start(1)
    exchange.step(0, pieces[0])
    group = lax.broadcasted_iota(jnp.int32, (2 * ranks, ranks), 0) % ranks // rank
    member = lax.broadcasted_iota(jnp.int32, (2 * ranks, ranks), 1) // rank
    blocks = (group == member).astype(F32).astype(BF16)

    def task_part(chunk):
        here = span(chunk * CHUNK, CHUNK, CHUNK)
        share = prob[here]
        product = low[here].astype(F32) * turned[here]
        upper = product.astype(BF16)
        lower = (product - upper.astype(F32)).astype(BF16)
        task = 2.0 * dot(jnp.concatenate([upper, lower], axis=1), blocks)
        plain[here] += share * (task - lane_sum(share * task) * scale)

    task_part(0)
    task_part(1)
    exchange.step(0, pieces[1])
    task_part(2)
    task_part(3)
    exchange.step(0, pieces[2])
    lane = lax.broadcasted_iota(jnp.int32, (CHUNK, LANES), 1)
    pick_from = lax.broadcasted_iota(jnp.int32, (ranks, ranks), 0)
    pick_to = lax.broadcasted_iota(jnp.int32, (ranks, ranks), 1)
    pick = (pick_from == (pick_to % experts) * rank + pick_to // experts).astype(F32)
    pick = jnp.where(pick_to < 2 * experts, pick, 0.0).astype(BF16)

    def slope_part(chunk):
        load_all, live_all = tiles[2, 0:1], tiles[2, 2:3]
        push = (2.0 * experts * 100.0) / live_all
        here = span(chunk * CHUNK, CHUNK, CHUNK)
        share = prob[here]
        slope = share * (load_all - lane_sum(share * load_all) * scale)
        whole = plain[here] + push * live_of(chunk) * slope
        upper = whole.astype(BF16).astype(F32)
        place = lane % rank
        packed = jnp.where(place == 0, upper, jnp.where(place == 1, whole - upper, 0.0)).astype(BF16)
        grads[here, ranks : 2 * ranks] = packed
        gate_t[:, here] = dot(packed, pick).T[: 2 * experts].astype(BF16)

    def base_block(block):
        tall = span((block % 2) * (rows // 2), rows // 2, rows // 2)
        here = span((block // 2) * 256, 256, 256)
        found = dot(tokens[tall], frozen[:, here]) + dot(weighted[tall], up[:, here])
        projected_ref[tall, here] = found.astype(BF16)

    def step_all(phase):
        for piece in pieces[:3]:
            exchange.step(phase, piece)

    def at(block, place):
        return pl.when(block == place)

    frozen_load.wait()

    @pl.loop(0, 3)
    def _(block):
        base_block(block)

    statistics.finish(1)

    @pl.loop(3, 5)
    def _(block):
        @at(block, 4)
        def _():
            exchange.step(1, pieces[0])

        slope_part(2 * block - 6)
        slope_part(2 * block - 5)
        base_block(block)

    exchange.step(1, pieces[1])
    exchange.step(1, pieces[2])

    @pl.loop(0, width // 1024)
    def _(block):
        found = dot(gate_t[...], tokens[:, span(block * 1024, 1024, 1024)])
        found = found[:experts] + found[experts:]
        for piece in range(8):
            here = span(gate_base + (block * 8 + piece) * experts, experts)
            part[here] = found[:, piece * LANES : (piece + 1) * LANES]

    gates.start(0)

    @pl.loop(5, 8)
    def _(block):
        @at(block, 6)
        def _():
            exchange.step(2, pieces[0])

        @at(block, 7)
        def _():
            exchange.step(2, pieces[1])
            exchange.step(2, pieces[2])

        base_block(block)

    @pl.loop(0, input_ref.shape[1] // 512)
    def _(block):
        @at(block, 0)
        def _():
            gates.step(0)

        @at(block, 1)
        def _():
            exchange.step(3, pieces[0])

        @at(block, 2)
        def _():
            exchange.step(3, pieces[1])
            exchange.step(3, pieces[2])
            gates.step(1)

        @at(block, 3)
        def _():
            exchange.step(4, pieces[0])

        @at(block, 4)
        def _():
            exchange.step(4, pieces[1])
            exchange.step(4, pieces[2])

        @at(block, 5)
        def _():
            gates.step(2)

        @at(block, 6)
        def _():
            exchange.step(5, pieces[0])

        here = span(block * 512, 512, 512)
        found = right_dot(masked[...], frozen[here]) + right_dot(grads[...], sides[here])
        input_ref[:, here] = found.astype(BF16)

    exchange.step(5, pieces[1])
    exchange.step(5, pieces[2])
    gates.finish(3)
    for piece in pieces:
        exchange.finish(6, piece)


def finish_kernel(
    sizes,
    projected, inputs, total, tiles, frozen, sides, masked, grads,
    projected_hbm, input_hbm, down_hbm, up_hbm, gate_hbm, load_hbm, entropy_hbm,
    scaled, up, gate, rest, load, entropy, sems,
):
    width, outputs, ranks, experts = sizes
    rank = ranks // experts
    every = total.shape[0]
    done = inputs.shape[1]
    copies = []

    def send(source, target):
        copy = pltpu.make_async_copy(source, target, sems.at[len(copies)])
        copy.start()
        copies.append(copy)

    tall = inputs.shape[0] // 4
    for block in range(4):
        here = pl.ds(block * tall, tall)
        send(inputs.at[here], input_hbm.at[here, pl.ds(0, done)])
    send(projected, projected_hbm)

    def add_squares(block, found):
        value = total[span(block * 192, 192)]
        return found + jnp.sum((value * value).reshape(6, 32, LANES), axis=0)

    squares = lax.fori_loop(0, every // 192, add_squares, jnp.zeros((32, LANES), F32))
    norm = jnp.sqrt(jnp.sum(jnp.sum(squares, axis=1, keepdims=True), axis=0, keepdims=True))
    mean = tiles[2] / tiles[2, 2:3]
    lane = lax.broadcasted_iota(jnp.int32, (1, LANES), 1)
    for expert in range(experts):
        load[expert] = jnp.sum(jnp.where(lane == expert * rank, mean[0:1], 0.0))
    entropy[0] = jnp.sum(jnp.where(lane == 0, mean[1:2], 0.0))
    send(load, load_hbm)
    send(entropy, entropy_hbm)

    here = pl.ds(done, 512)
    found = right_dot(masked[...], frozen[here]) + right_dot(grads[...], sides[here])
    rest[...] = found.astype(BF16)
    factor = jnp.minimum(1.0, math.sqrt(every * LANES) / norm)
    for block in range(width // LANES):
        here = pl.ds(block * LANES, LANES)
        scaled[here] = (total[here] * factor).T
    for block in range(outputs // LANES):
        here = width + block * LANES
        up[:, block * LANES : (block + 1) * LANES] = total[here : here + LANES] * factor
    for block in range(width // LANES):
        here = width + outputs + block * experts
        gate[:, block * LANES : (block + 1) * LANES] = total[here : here + experts] * factor
    send(scaled, down_hbm)
    send(up, up_hbm)
    send(gate, gate_hbm)
    send(rest, input_hbm.at[:, pl.ds(done, 512)])
    for copy in copies:
        copy.wait()


def on_device(token_ids, tokens, frozen_weight, adapter_down, adapter_up, gate_weight, upstream):
    rows, width = tokens.shape
    ranks, outputs = adapter_up.shape
    experts = gate_weight.shape[1]
    every = width + outputs + width * experts // LANES
    anywhere = pl.BlockSpec(memory_space=pl.ANY)
    hbm = pl.BlockSpec(memory_space=pltpu.HBM)
    vmem = pl.BlockSpec(memory_space=pltpu.VMEM)
    held = pl.pallas_call(
        functools.partial(kernel, (rows, width, outputs, ranks, experts)),
        out_shape=(
            pltpu.VMEM((rows, outputs), BF16),
            pltpu.VMEM((rows, width - 512), BF16),
            pltpu.VMEM((every, LANES), F32),
            pltpu.VMEM((3, 8, LANES), F32),
            pltpu.VMEM((width, outputs), BF16),
            pltpu.VMEM((width, 2 * ranks), BF16),
            pltpu.VMEM((rows, outputs), BF16),
            pltpu.VMEM((rows, 2 * ranks), BF16),
        ),
        in_specs=[hbm] * 7,
        out_specs=(vmem,) * 8,
        scratch_shapes=[
            pltpu.VMEM((rows // LANES, LANES), jnp.int32),
            pltpu.VMEM((rows, width), BF16),
            pltpu.VMEM((ranks, outputs), BF16),
            pltpu.VMEM((experts, width), BF16),
            pltpu.VMEM((2, CHUNK, 2 * ranks), F32),
            pltpu.VMEM((rows, ranks), BF16),
            pltpu.VMEM((rows, ranks), F32),
            pltpu.VMEM((rows, ranks), F32),
            pltpu.VMEM((rows, ranks), F32),
            pltpu.VMEM((rows, ranks), BF16),
            pltpu.VMEM((ranks, rows), BF16),
            pltpu.VMEM((ranks, rows), BF16),
            pltpu.VMEM((2 * experts, rows), BF16),
            pltpu.VMEM((every, LANES), F32),
            pltpu.VMEM((every // 2, LANES), F32),
            pltpu.VMEM((3, every // 8, LANES), F32),
            pltpu.VMEM((3, every // 32, LANES), F32),
            pltpu.VMEM((4, every // 32, LANES), F32),
            pltpu.VMEM((8, 8, LANES), F32),
            pltpu.VMEM((16, 8, LANES), F32),
            pltpu.VMEM((7, width * experts // LANES // 8, LANES), F32),
            pltpu.VMEM((2, SIDE, width * experts // LANES // 8, LANES), F32),
            pltpu.SemaphoreType.DMA((5,)),
            pltpu.SemaphoreType.DMA((rows // CHUNK, 2)),
            pltpu.SemaphoreType.DMA((4,)),
            pltpu.SemaphoreType.DMA((8, 3)),
            pltpu.SemaphoreType.DMA((1,)),
            pltpu.SemaphoreType.DMA((2,)),
            pltpu.SemaphoreType.DMA((4,)),
        ],
        compiler_params=pltpu.CompilerParams(
            collective_id=0, has_side_effects=True, vmem_limit_bytes=36 * 1024 * 1024
        ),
        name="step",
    )(token_ids.reshape(rows // LANES, LANES), tokens, frozen_weight, adapter_down, adapter_up, gate_weight.T, upstream)
    projected, input_grad, down, up, gate, load, entropy = pl.pallas_call(
        functools.partial(finish_kernel, (width, outputs, ranks, experts)),
        out_shape=(
            jax.ShapeDtypeStruct((rows, outputs), BF16),
            jax.ShapeDtypeStruct((rows, width), BF16),
            jax.ShapeDtypeStruct((width, ranks), F32),
            jax.ShapeDtypeStruct((ranks, outputs), F32),
            jax.ShapeDtypeStruct((experts, width), F32),
            jax.ShapeDtypeStruct((experts,), F32),
            jax.ShapeDtypeStruct((1,), F32),
        ),
        in_specs=[vmem] * 8,
        out_specs=(anywhere,) * 7,
        scratch_shapes=[
            pltpu.VMEM((width, ranks), F32),
            pltpu.VMEM((ranks, outputs), F32),
            pltpu.VMEM((experts, width), F32),
            pltpu.VMEM((rows, 512), BF16),
            pltpu.SMEM((experts,), F32),
            pltpu.SMEM((1,), F32),
            pltpu.SemaphoreType.DMA((11,)),
        ],
        compiler_params=pltpu.CompilerParams(vmem_limit_bytes=12 * 1024 * 1024),
        name="finish",
    )(*held)
    return projected, input_grad, down, up, gate.T, load, entropy.reshape(())


def solution(mesh):
    torus = Mesh(mesh.devices.reshape(4, 4, 4, 2), DP)
    return jax.shard_map(
        on_device,
        mesh=torus,
        in_specs=(P(DP), P(DP, None), P(), P(), P(), P(), P(DP, None)),
        out_specs=(P(DP, None), P(DP, None), P(), P(), P(), P(), P()),
        check_vma=False,
    )
```

```python
import functools
import math

import jax
import jax.numpy as jnp
from jax import lax
from jax.experimental import pallas as pl
from jax.experimental.pallas import tpu as pltpu
from jax.sharding import Mesh
from jax.sharding import PartitionSpec as P

AXES = ("dp_0", "dp_1", "dp_2")
CORE = "dp_3"
DP = AXES + (CORE,)
MESH = pl.DeviceIdType.MESH
SIDE = 4
LANES = 128
CHUNK = 256
BF16 = jnp.bfloat16
F32 = jnp.float32


def dot(first, second):
    return jnp.dot(first, second, preferred_element_type=F32)


def right_dot(first, second):
    return lax.dot_general(first, second, (((1,), (1,)), ((), ())), preferred_element_type=F32)


def ring_peer(axis, distance):
    return {axis: lax.rem(lax.axis_index(axis) + distance, SIDE)}


def span(start, size, unit=8):
    return pl.ds(pl.multiple_of(start, unit), size)


class Piece:
    def __init__(self, index, base, rows):
        self.index, self.base, self.rows = index, base, rows
        self.half, self.quarter, self.last = rows // 2, rows // 8, rows // 32
        self.first, self.second, self.third = (AXES[(index + step) % 3] for step in range(3))


class Exchange:
    def __init__(self, part, total, halves, firsts, seconds, thirds, send, recv):
        self.part, self.total = part, total
        self.halves, self.firsts, self.seconds, self.thirds = halves, firsts, seconds, thirds
        self.send, self.recv = send, recv
        self.core = lax.axis_index(CORE)

    def half_at(self, piece, core):
        return piece.base + core * piece.half

    def quarter_at(self, piece, place):
        return self.half_at(piece, self.core) + place * piece.quarter

    def last_at(self, piece, place, second):
        return self.quarter_at(piece, place) + second * piece.last

    def send_to(self, source, target, phase, piece, device):
        pltpu.make_async_remote_copy(
            src_ref=source,
            dst_ref=target,
            send_sem=self.send.at[piece.index],
            recv_sem=self.recv.at[phase, piece.index],
            device_id=device,
            device_id_type=MESH,
        ).start()

    def sent(self, piece, rows):
        here = self.part.at[pl.ds(0, rows)]
        pltpu.make_async_copy(here, here, self.send.at[piece.index]).wait()

    def received(self, phase, piece, rows):
        here = self.part.at[pl.ds(0, rows)]
        pltpu.make_async_copy(here, here, self.recv.at[phase, piece.index]).wait()

    def forward(self, piece, distance):
        place = lax.rem(lax.axis_index(piece.first) + distance, SIDE)
        here = self.total.at[span(self.quarter_at(piece, place), piece.quarter)]
        self.send_to(here, here, 6, piece, {CORE: 1 - self.core})

    def spread_out(self, piece, place):
        here = self.total.at[span(self.last_at(piece, lax.axis_index(piece.first), place), piece.last)]
        for distance in (2, 1, 3):
            self.send_to(here, here, 5, piece, ring_peer(piece.first, distance))
        self.send_to(here, here, 6, piece, {CORE: 1 - self.core})

    def start(self, phase, piece):
        one, two = lax.axis_index(piece.first), lax.axis_index(piece.second)
        if phase == 0:
            source = self.part.at[span(self.half_at(piece, 1 - self.core), piece.half)]
            target = self.halves.at[pl.ds(piece.base // 2, piece.half)]
            self.send_to(source, target, 0, piece, {CORE: 1 - self.core})
            return
        if phase == 1:
            for turn in (1, 2, 3, 0):
                second = lax.rem(two + turn, SIDE)
                for distance in (2, 1, 3):
                    place = lax.rem(one + distance, SIDE)
                    self.send_to(
                        self.part.at[span(self.last_at(piece, place, second), piece.last)],
                        self.firsts.at[distance - 1, span(piece.base // 8 + second * piece.last, piece.last)],
                        7 if turn == 0 else 1,
                        piece,
                        ring_peer(piece.first, distance),
                    )
            return
        if phase == 5:
            for distance in (1, 2, 3):
                self.spread_out(piece, lax.rem(two + distance, SIDE))
            return
        if phase == 6:
            for distance in (1, 2, 3):
                self.forward(piece, distance)
            return
        for distance in (2, 1, 3):
            slot = distance - 1
            if phase == 2:
                place = lax.rem(two + distance, SIDE)
                source = self.part.at[span(self.last_at(piece, one, place), piece.last)]
                target = self.seconds.at[slot, pl.ds(piece.base // 32, piece.last)]
                axis = piece.second
            elif phase == 3:
                source = self.part.at[span(self.last_at(piece, one, two), piece.last)]
                target = self.thirds.at[lax.axis_index(piece.third), pl.ds(piece.base // 32, piece.last)]
                axis = piece.third
            else:
                source = self.total.at[span(self.last_at(piece, one, two), piece.last)]
                target, axis = source, piece.second
            self.send_to(source, target, phase, piece, ring_peer(axis, distance))
        if phase == 4:
            self.spread_out(piece, two)

    def finish(self, phase, piece):
        sent = {0: piece.half, 1: 12 * piece.last, 4: 7 * piece.last, 5: 12 * piece.last, 6: 3 * piece.quarter}
        got_rows = {0: piece.half, 1: 9 * piece.last, 5: 3 * piece.quarter, 6: piece.half}
        self.sent(piece, sent.get(phase, 3 * piece.last))
        self.received(phase, piece, got_rows.get(phase, 3 * piece.last))
        one, two = lax.axis_index(piece.first), lax.axis_index(piece.second)
        if phase == 0:
            here = span(self.half_at(piece, self.core), piece.half)
            self.part[here] = self.part[here] + self.halves[pl.ds(piece.base // 2, piece.half)]
        elif phase == 1:
            for turn in (1, 2, 3):
                self.add_firsts(piece, lax.rem(two + turn, SIDE))
        elif phase == 2:
            self.received(7, piece, 3 * piece.last)
            self.add_firsts(piece, two)
            here = span(self.last_at(piece, one, two), piece.last)
            there = pl.ds(piece.base // 32, piece.last)
            got = self.seconds
            self.part[here] = (self.part[here] + got[0, there]) + (got[1, there] + got[2, there])
        elif phase == 3:
            here = span(self.last_at(piece, one, two), piece.last)
            there = pl.ds(piece.base // 32, piece.last)
            got = self.thirds
            got[lax.axis_index(piece.third), there] = self.part[here]
            self.total[here] = (got[0, there] + got[1, there]) + (got[2, there] + got[3, there])

    def add_firsts(self, piece, second):
        here = span(self.last_at(piece, lax.axis_index(piece.first), second), piece.last)
        there = span(piece.base // 8 + second * piece.last, piece.last)
        got = self.firsts
        self.part[here] = (self.part[here] + got[0, there]) + (got[1, there] + got[2, there])

    def step(self, phase, piece):
        self.finish(phase, piece)
        self.start(phase + 1, piece)


def pair_peer(first, second, size, distance):
    other = lax.rem(lax.axis_index(first) * SIDE + lax.axis_index(second) + distance, size)
    return {first: lax.div(other, SIDE), second: lax.rem(other, SIDE)}


class Statistics:
    def __init__(self, tiles, wide, plane, send, recv):
        self.tiles, self.slots = tiles, (wide, plane)
        self.axes = ((CORE, AXES[2]), (AXES[0], AXES[1]))
        self.send, self.recv = send, recv

    def mine(self, stage):
        first, second = self.axes[stage]
        return lax.axis_index(first) * SIDE + lax.axis_index(second)

    def start(self, stage):
        size = self.slots[stage].shape[0]
        for distance in range(1, size):
            pltpu.make_async_remote_copy(
                src_ref=self.tiles.at[stage],
                dst_ref=self.slots[stage].at[self.mine(stage)],
                send_sem=self.send.at[0],
                recv_sem=self.recv.at[stage],
                device_id=pair_peer(*self.axes[stage], size, distance),
                device_id_type=MESH,
            ).start()

    def finish(self, stage):
        slots = self.slots[stage]
        several = slots.at[pl.ds(0, slots.shape[0] - 1)]
        pltpu.make_async_copy(several, several, self.send.at[0]).wait()
        pltpu.make_async_copy(several, several, self.recv.at[stage]).wait()
        slots[self.mine(stage)] = self.tiles[stage]
        total = slots[0]
        for place in range(1, slots.shape[0]):
            total = total + slots[place]
        self.tiles[stage + 1] = total


class GateExchange:
    def __init__(self, base, rows, part, total, inward, rings, send, recv):
        self.base, self.share = base, rows // 8
        self.part, self.total = part, total
        self.inward, self.rings = inward, rings
        self.send, self.recv = send, recv
        self.group = lax.axis_index(CORE) * SIDE + lax.axis_index(AXES[0])

    def chunk(self, place):
        return span(self.base + place * self.share, self.share)

    def start(self, stage):
        mine = self.chunk(self.group)
        for distance in range(1, SIDE if stage in (1, 2) else 8):
            if stage in (1, 2):
                device = ring_peer(AXES[stage], distance)
                source, target = self.part.at[mine], self.rings.at[stage - 1, lax.axis_index(AXES[stage])]
            else:
                other = lax.rem(self.group + distance, 8)
                device = {CORE: lax.div(other, SIDE), AXES[0]: lax.rem(other, SIDE)}
                if stage == 0:
                    source, target = self.part.at[self.chunk(other)], self.inward.at[distance - 1]
                else:
                    source = self.total.at[mine]
                    target = source
            pltpu.make_async_remote_copy(
                src_ref=source,
                dst_ref=target,
                send_sem=self.send.at[3],
                recv_sem=self.recv.at[stage],
                device_id=device,
                device_id_type=MESH,
            ).start()

    def finish(self, stage):
        several = self.inward.at[pl.ds(0, 3 if stage in (1, 2) else 7)]
        pltpu.make_async_copy(several, several, self.send.at[3]).wait()
        pltpu.make_async_copy(several, several, self.recv.at[stage]).wait()
        mine = self.chunk(self.group)
        if stage == 0:
            value = self.part[mine]
            for slot in range(7):
                value = value + self.inward[slot]
            self.part[mine] = value
        elif stage < 3:
            self.rings[stage - 1, lax.axis_index(AXES[stage])] = self.part[mine]
            value = self.rings[stage - 1, 0]
            for slot in range(1, SIDE):
                value = value + self.rings[stage - 1, slot]
            if stage == 1:
                self.part[mine] = value
            else:
                self.total[mine] = value

    def step(self, stage):
        self.finish(stage)
        self.start(stage + 1)


def peers():
    core = lax.axis_index(CORE)
    found = [{CORE: 1 - core}]
    for distance in (1, 2, 3):
        for axis in (AXES[0], AXES[2]):
            found.append({CORE: 1 - core, **ring_peer(axis, distance)})
        found.append(ring_peer(AXES[2], distance))
    found += [pair_peer(AXES[0], AXES[1], 16, distance) for distance in range(1, 16)]
    return found


def kernel(
    sizes,
    ids_hbm, tokens_hbm, frozen_hbm, down_hbm, up_hbm, gate_hbm, upstream_hbm,
    projected_ref, input_ref, total, tiles,
    ids, tokens, frozen, sides, masked, grads, up, gate,
    both, low, prob, plain, turned, weighted, grads_t, weighted_t, gate_t,
    part, halves, firsts, seconds, thirds, wide, plane, inward, rings,
    load_sem, token_sem, send, recv, stat_send, stat_recv, gate_recv,
):
    rows, width, outputs, ranks, experts = sizes
    rank = ranks // experts
    scale = 1.0 / rank
    chunks = rows // CHUNK
    up_base = width
    gate_base = width + outputs
    pieces = (Piece(0, 0, 1792), Piece(1, 1792, 1792), Piece(2, 3584, gate_base - 3584))
    exchange = Exchange(part, total, halves, firsts, seconds, thirds, send, recv)
    statistics = Statistics(tiles, wide, plane, stat_send, stat_recv)
    gates = GateExchange(gate_base, width * experts // LANES, part, total, inward, rings, send, gate_recv)

    gate_load = pltpu.make_async_copy(gate_hbm, gate, load_sem.at[0])
    ids_load = pltpu.make_async_copy(ids_hbm, ids, load_sem.at[1])
    gate_load.start()
    ids_load.start()
    def load(source, target, slot):
        return pltpu.make_async_copy(source, target, load_sem.at[slot])

    def chunk_load(chunk):
        here = span(chunk * CHUNK, CHUNK, CHUNK)
        return (
            pltpu.make_async_copy(tokens_hbm.at[here], tokens.at[here], token_sem.at[chunk, 0]),
            pltpu.make_async_copy(upstream_hbm.at[here], masked.at[here], token_sem.at[chunk, 1]),
        )

    down_load = load(down_hbm, sides.at[:, pl.ds(0, ranks)], 2)
    up_load = load(up_hbm, up, 3)
    frozen_load = load(frozen_hbm, frozen, 4)
    down_load.start()
    chunk_load(0)[0].start()
    up_load.start()
    chunk_load(0)[1].start()
    barrier = pltpu.get_barrier_semaphore()
    greeted = peers()
    for peer in greeted:
        pl.semaphore_signal(barrier, inc=1, device_id=peer, device_id_type=MESH)

    gate_load.wait()
    for copy in chunk_load(1):
        copy.start()

    @pl.loop(0, width // 512)
    def _(block):
        here = span(block * 512, 512, 512)
        row = gate[:, here].astype(F32)
        tall = jnp.concatenate([jnp.broadcast_to(row[e : e + 1], (rank, 512)) for e in range(experts)], axis=0)
        sides[here, ranks : 2 * ranks] = tall.T.astype(BF16)

    ids_load.wait()
    live_rows = jnp.sum(jnp.sum((ids[...] != 0).astype(F32), axis=1, keepdims=True), axis=0, keepdims=True)

    def live_of(chunk):
        row = lax.broadcasted_iota(jnp.int32, (CHUNK, LANES), 0) + chunk * CHUNK
        return (row.astype(F32) < live_rows).astype(F32)

    def lane_sum(value):
        return jnp.sum(value, axis=1, keepdims=True)

    tiles[0] = jnp.zeros((8, LANES), F32)
    down_load.wait()

    def spread(chunk):
        here = span(chunk * CHUNK, CHUNK, CHUNK)
        slot = chunk % 2
        below = both[slot, :, :ranks].astype(BF16)
        logits = both[slot, :, ranks:]
        shifted = logits - jnp.max(logits, axis=1, keepdims=True)
        raised = jnp.exp(shifted)
        mass = lane_sum(raised) * scale
        share = raised / mass
        logp = shifted - jnp.log(mass)
        entropy = -lane_sum(share * logp) * scale
        alive = live_of(chunk)
        low[here] = below
        prob[here] = share
        plain[here] = 50.0 * alive * share * (logp + entropy)
        tiles[0, 0:1] += jnp.sum(alive * share, axis=0, keepdims=True)
        tiles[0, 1:2] += jnp.sum(alive * entropy, axis=0, keepdims=True)
        tiles[0, 2:3] += jnp.sum(alive, axis=0, keepdims=True)
        mine = jnp.where(alive[:, 0:1] > 0.0, masked[here].astype(F32), 0.0).astype(BF16)
        masked[here] = mine
        back = right_dot(mine, up[...])
        heavy = (below.astype(F32) * share).astype(BF16).astype(F32) * 2.0
        steep = (2.0 * share * back).astype(BF16)
        turned[here] = back
        weighted[here] = heavy.astype(BF16)
        grads[here, 0:ranks] = steep
        grads_t[:, here] = steep.astype(F32).T.astype(BF16)
        weighted_t[:, here] = heavy.T.astype(BF16)

    for copy in chunk_load(2):
        copy.start()
    chunk_load(0)[0].wait()
    for copy in chunk_load(3):
        copy.start()
    both[0] = dot(tokens[0:CHUNK], sides[...])
    up_load.wait()

    @pl.loop(1, chunks)
    def _(chunk):
        chunk_load(chunk - 1)[1].wait()
        chunk_load(chunk)[0].wait()
        spread(chunk - 1)
        both[chunk % 2] = dot(tokens[span(chunk * CHUNK, CHUNK, CHUNK)], sides[...])

    frozen_load.start()
    chunk_load(chunks - 1)[1].wait()
    spread(chunks - 1)
    pl.semaphore_wait(barrier, len(greeted))
    statistics.start(0)

    def down_block(start, size):
        found = dot(grads_t[...], tokens[:, pl.ds(start, size)])
        for block in range(size // LANES):
            here = start + block * LANES
            part[here : here + LANES] = found[:, block * LANES : (block + 1) * LANES]

    down_block(0, 1792)
    exchange.start(0, pieces[0])
    down_block(1792, 1792)
    exchange.start(0, pieces[1])
    down_block(3584, 512)
    found = dot(weighted_t[...], masked[...])
    for block in range(outputs // LANES):
        part[up_base + block * LANES : up_base + (block + 1) * LANES] = found[:, block * LANES : (block + 1) * LANES]
    exchange.start(0, pieces[2])
    group = lax.broadcasted_iota(jnp.int32, (2 * ranks, ranks), 0) % ranks // rank
    member = lax.broadcasted_iota(jnp.int32, (2 * ranks, ranks), 1) // rank
    blocks = (group == member).astype(F32).astype(BF16)

    def task_part(chunk):
        here = span(chunk * CHUNK, CHUNK, CHUNK)
        share = prob[here]
        product = low[here].astype(F32) * turned[here]
        upper = product.astype(BF16)
        lower = (product - upper.astype(F32)).astype(BF16)
        task = 2.0 * dot(jnp.concatenate([upper, lower], axis=1), blocks)
        plain[here] += share * (task - lane_sum(share * task) * scale)

    task_part(0)
    task_part(1)
    statistics.finish(0)
    statistics.start(1)
    exchange.step(0, pieces[0])
    task_part(2)
    exchange.step(0, pieces[1])
    task_part(3)
    exchange.step(0, pieces[2])
    lane = lax.broadcasted_iota(jnp.int32, (CHUNK, LANES), 1)
    pick_from = lax.broadcasted_iota(jnp.int32, (ranks, ranks), 0)
    pick_to = lax.broadcasted_iota(jnp.int32, (ranks, ranks), 1)
    pick = (pick_from == (pick_to % experts) * rank + pick_to // experts).astype(F32)
    pick = jnp.where(pick_to < 2 * experts, pick, 0.0).astype(BF16)

    def slope_part(chunk):
        load_all, live_all = tiles[2, 0:1], tiles[2, 2:3]
        push = (2.0 * experts * 100.0) / live_all
        here = span(chunk * CHUNK, CHUNK, CHUNK)
        share = prob[here]
        slope = share * (load_all - lane_sum(share * load_all) * scale)
        whole = plain[here] + push * live_of(chunk) * slope
        upper = whole.astype(BF16).astype(F32)
        place = lane % rank
        packed = jnp.where(place == 0, upper, jnp.where(place == 1, whole - upper, 0.0)).astype(BF16)
        grads[here, ranks : 2 * ranks] = packed
        gate_t[:, here] = dot(packed, pick).T[: 2 * experts].astype(BF16)

    def base_block(block):
        tall = span((block % 2) * (rows // 2), rows // 2, rows // 2)
        here = span((block // 2) * 256, 256, 256)
        found = dot(tokens[tall], frozen[:, here]) + dot(weighted[tall], up[:, here])
        projected_ref[tall, here] = found.astype(BF16)

    def step_all(phase):
        for piece in pieces[:3]:
            exchange.step(phase, piece)

    def at(block, place):
        return pl.when(block == place)

    frozen_load.wait()

    @pl.loop(0, 3)
    def _(block):
        base_block(block)

    statistics.finish(1)

    @pl.loop(3, 5)
    def _(block):
        @at(block, 4)
        def _():
            exchange.step(1, pieces[0])

        slope_part(2 * block - 6)
        slope_part(2 * block - 5)
        base_block(block)

    exchange.step(1, pieces[1])
    exchange.step(1, pieces[2])

    @pl.loop(0, width // 2048)
    def _(block):
        found = dot(gate_t[...], tokens[:, span(block * 2048, 2048, 2048)])
        found = found[:experts] + found[experts:]
        for piece in range(16):
            here = span(gate_base + (block * 16 + piece) * experts, experts)
            part[here] = found[:, piece * LANES : (piece + 1) * LANES]

    gates.start(0)

    @pl.loop(5, 8)
    def _(block):
        @at(block, 6)
        def _():
            exchange.step(2, pieces[0])

        @at(block, 7)
        def _():
            exchange.step(2, pieces[1])
            exchange.step(2, pieces[2])

        base_block(block)

    def input_block(block):
        here = span(block * 512, 512, 512)
        found = right_dot(masked[...], frozen[here]) + right_dot(grads[...], sides[here])
        input_ref[:, here] = found.astype(BF16)

    @pl.loop(0, input_ref.shape[1] // 512 - 1)
    def _(block):
        @at(block, 0)
        def _():
            gates.step(0)

        @at(block, 1)
        def _():
            exchange.step(3, pieces[0])

        @at(block, 2)
        def _():
            exchange.step(3, pieces[1])
            exchange.step(3, pieces[2])
            gates.step(1)

        @at(block, 3)
        def _():
            exchange.step(4, pieces[0])

        @at(block, 4)
        def _():
            exchange.step(4, pieces[1])
            exchange.step(4, pieces[2])

        @at(block, 5)
        def _():
            gates.step(2)

        @at(block, 6)
        def _():
            exchange.step(5, pieces[0])

        input_block(block)

    exchange.step(5, pieces[1])
    exchange.step(5, pieces[2])
    input_block(input_ref.shape[1] // 512 - 1)
    gates.finish(3)
    for piece in pieces:
        exchange.finish(6, piece)


def finish_kernel(
    sizes,
    projected, inputs, total, tiles,
    projected_hbm, input_hbm, down_hbm, up_hbm, gate_hbm, load_hbm, entropy_hbm,
    scaled, up, gate, load, entropy, sems,
):
    width, outputs, ranks, experts = sizes
    rank = ranks // experts
    every = total.shape[0]
    copies = []

    def send(source, target):
        copy = pltpu.make_async_copy(source, target, sems.at[len(copies)])
        copy.start()
        copies.append(copy)

    tall = inputs.shape[0] // 4
    for block in range(4):
        here = pl.ds(block * tall, tall)
        send(inputs.at[here], input_hbm.at[here])
    send(projected, projected_hbm)

    def add_squares(block, found):
        value = total[span(block * 192, 192)]
        return found + jnp.sum((value * value).reshape(6, 32, LANES), axis=0)

    squares = lax.fori_loop(0, every // 192, add_squares, jnp.zeros((32, LANES), F32))
    norm = jnp.sqrt(jnp.sum(jnp.sum(squares, axis=1, keepdims=True), axis=0, keepdims=True))
    mean = tiles[2] / tiles[2, 2:3]
    lane = lax.broadcasted_iota(jnp.int32, (1, LANES), 1)
    for expert in range(experts):
        load[expert] = jnp.sum(jnp.where(lane == expert * rank, mean[0:1], 0.0))
    entropy[0] = jnp.sum(jnp.where(lane == 0, mean[1:2], 0.0))
    send(load, load_hbm)
    send(entropy, entropy_hbm)

    factor = jnp.minimum(1.0, math.sqrt(every * LANES) / norm)
    for block in range(width // LANES):
        here = pl.ds(block * LANES, LANES)
        scaled[here] = (total[here] * factor).T
    for block in range(outputs // LANES):
        here = width + block * LANES
        up[:, block * LANES : (block + 1) * LANES] = total[here : here + LANES] * factor
    for block in range(width // LANES):
        here = width + outputs + block * experts
        gate[:, block * LANES : (block + 1) * LANES] = total[here : here + experts] * factor
    send(scaled, down_hbm)
    send(up, up_hbm)
    send(gate, gate_hbm)
    for copy in copies:
        copy.wait()


def on_device(token_ids, tokens, frozen_weight, adapter_down, adapter_up, gate_weight, upstream):
    rows, width = tokens.shape
    ranks, outputs = adapter_up.shape
    experts = gate_weight.shape[1]
    every = width + outputs + width * experts // LANES
    anywhere = pl.BlockSpec(memory_space=pl.ANY)
    hbm = pl.BlockSpec(memory_space=pltpu.HBM)
    vmem = pl.BlockSpec(memory_space=pltpu.VMEM)
    held = pl.pallas_call(
        functools.partial(kernel, (rows, width, outputs, ranks, experts)),
        out_shape=(
            pltpu.VMEM((rows, outputs), BF16),
            pltpu.VMEM((rows, width), BF16),
            pltpu.VMEM((every, LANES), F32),
            pltpu.VMEM((3, 8, LANES), F32),
        ),
        in_specs=[hbm] * 7,
        out_specs=(vmem,) * 4,
        scratch_shapes=[
            pltpu.VMEM((rows // LANES, LANES), jnp.int32),
            pltpu.VMEM((rows, width), BF16),
            pltpu.VMEM((width, outputs), BF16),
            pltpu.VMEM((width, 2 * ranks), BF16),
            pltpu.VMEM((rows, outputs), BF16),
            pltpu.VMEM((rows, 2 * ranks), BF16),
            pltpu.VMEM((ranks, outputs), BF16),
            pltpu.VMEM((experts, width), BF16),
            pltpu.VMEM((2, CHUNK, 2 * ranks), F32),
            pltpu.VMEM((rows, ranks), BF16),
            pltpu.VMEM((rows, ranks), F32),
            pltpu.VMEM((rows, ranks), F32),
            pltpu.VMEM((rows, ranks), F32),
            pltpu.VMEM((rows, ranks), BF16),
            pltpu.VMEM((ranks, rows), BF16),
            pltpu.VMEM((ranks, rows), BF16),
            pltpu.VMEM((2 * experts, rows), BF16),
            pltpu.VMEM((every, LANES), F32),
            pltpu.VMEM((every // 2, LANES), F32),
            pltpu.VMEM((3, every // 8, LANES), F32),
            pltpu.VMEM((3, every // 32, LANES), F32),
            pltpu.VMEM((4, every // 32, LANES), F32),
            pltpu.VMEM((8, 8, LANES), F32),
            pltpu.VMEM((16, 8, LANES), F32),
            pltpu.VMEM((7, width * experts // LANES // 8, LANES), F32),
            pltpu.VMEM((2, SIDE, width * experts // LANES // 8, LANES), F32),
            pltpu.SemaphoreType.DMA((5,)),
            pltpu.SemaphoreType.DMA((rows // CHUNK, 2)),
            pltpu.SemaphoreType.DMA((4,)),
            pltpu.SemaphoreType.DMA((8, 3)),
            pltpu.SemaphoreType.DMA((1,)),
            pltpu.SemaphoreType.DMA((2,)),
            pltpu.SemaphoreType.DMA((4,)),
        ],
        compiler_params=pltpu.CompilerParams(
            collective_id=0, has_side_effects=True, vmem_limit_bytes=46 * 1024 * 1024
        ),
        name="step",
    )(token_ids.reshape(rows // LANES, LANES), tokens, frozen_weight, adapter_down, adapter_up, gate_weight.T, upstream)
    projected, input_grad, down, up, gate, load, entropy = pl.pallas_call(
        functools.partial(finish_kernel, (width, outputs, ranks, experts)),
        out_shape=(
            jax.ShapeDtypeStruct((rows, outputs), BF16),
            jax.ShapeDtypeStruct((rows, width), BF16),
            jax.ShapeDtypeStruct((width, ranks), F32),
            jax.ShapeDtypeStruct((ranks, outputs), F32),
            jax.ShapeDtypeStruct((experts, width), F32),
            jax.ShapeDtypeStruct((experts,), F32),
            jax.ShapeDtypeStruct((1,), F32),
        ),
        in_specs=[vmem] * 4,
        out_specs=(anywhere,) * 7,
        scratch_shapes=[
            pltpu.VMEM((width, ranks), F32),
            pltpu.VMEM((ranks, outputs), F32),
            pltpu.VMEM((experts, width), F32),
            pltpu.SMEM((experts,), F32),
            pltpu.SMEM((1,), F32),
            pltpu.SemaphoreType.DMA((10,)),
        ],
        compiler_params=pltpu.CompilerParams(vmem_limit_bytes=12 * 1024 * 1024),
        name="finish",
    )(*held)
    return projected, input_grad, down, up, gate.T, load, entropy.reshape(())


def solution(mesh):
    torus = Mesh(mesh.devices.reshape(4, 4, 4, 2), DP)
    return jax.shard_map(
        on_device,
        mesh=torus,
        in_specs=(P(DP), P(DP, None), P(), P(), P(), P(), P(DP, None)),
        out_specs=(P(DP, None), P(DP, None), P(), P(), P(), P(), P()),
        check_vma=False,
    )
```

```python
import functools
import math

import jax
import jax.numpy as jnp
from jax import lax
from jax.experimental import pallas as pl
from jax.experimental.pallas import tpu as pltpu
from jax.sharding import Mesh
from jax.sharding import PartitionSpec as P

AXES = ("dp_0", "dp_1", "dp_2")
CORE = "dp_3"
DP = AXES + (CORE,)
MESH = pl.DeviceIdType.MESH
SIDE = 4
LANES = 128
CHUNK = 256
BF16 = jnp.bfloat16
F32 = jnp.float32


def dot(first, second):
    return jnp.dot(first, second, preferred_element_type=F32)


def right_dot(first, second):
    return lax.dot_general(first, second, (((1,), (1,)), ((), ())), preferred_element_type=F32)


def ring_peer(axis, distance):
    return {axis: lax.rem(lax.axis_index(axis) + distance, SIDE)}


def span(start, size, unit=8):
    return pl.ds(pl.multiple_of(start, unit), size)


class Piece:
    def __init__(self, index, base, rows):
        self.index, self.base, self.rows = index, base, rows
        self.half, self.quarter, self.last = rows // 2, rows // 8, rows // 32
        self.first, self.second, self.third = (AXES[(index + step) % 3] for step in range(3))


class Exchange:
    def __init__(self, part, total, halves, firsts, seconds, thirds, send, recv):
        self.part, self.total = part, total
        self.halves, self.firsts, self.seconds, self.thirds = halves, firsts, seconds, thirds
        self.send, self.recv = send, recv
        self.core = lax.axis_index(CORE)

    def half_at(self, piece, core):
        return piece.base + core * piece.half

    def quarter_at(self, piece, place):
        return self.half_at(piece, self.core) + place * piece.quarter

    def last_at(self, piece, place, second):
        return self.quarter_at(piece, place) + second * piece.last

    def send_to(self, source, target, phase, piece, device):
        pltpu.make_async_remote_copy(
            src_ref=source,
            dst_ref=target,
            send_sem=self.send.at[piece.index],
            recv_sem=self.recv.at[phase, piece.index],
            device_id=device,
            device_id_type=MESH,
        ).start()

    def sent(self, piece, rows):
        here = self.part.at[pl.ds(0, rows)]
        pltpu.make_async_copy(here, here, self.send.at[piece.index]).wait()

    def received(self, phase, piece, rows):
        here = self.part.at[pl.ds(0, rows)]
        pltpu.make_async_copy(here, here, self.recv.at[phase, piece.index]).wait()

    def forward(self, piece, distance):
        place = lax.rem(lax.axis_index(piece.first) + distance, SIDE)
        here = self.total.at[span(self.quarter_at(piece, place), piece.quarter)]
        self.send_to(here, here, 6, piece, {CORE: 1 - self.core})

    def spread_out(self, piece, place):
        here = self.total.at[span(self.last_at(piece, lax.axis_index(piece.first), place), piece.last)]
        for distance in (2, 1, 3):
            self.send_to(here, here, 5, piece, ring_peer(piece.first, distance))
        self.send_to(here, here, 6, piece, {CORE: 1 - self.core})

    def start(self, phase, piece):
        one, two = lax.axis_index(piece.first), lax.axis_index(piece.second)
        if phase == 0:
            source = self.part.at[span(self.half_at(piece, 1 - self.core), piece.half)]
            target = self.halves.at[pl.ds(piece.base // 2, piece.half)]
            self.send_to(source, target, 0, piece, {CORE: 1 - self.core})
            return
        if phase == 1:
            for turn in (1, 2, 3, 0):
                second = lax.rem(two + turn, SIDE)
                for distance in (2, 1, 3):
                    place = lax.rem(one + distance, SIDE)
                    self.send_to(
                        self.part.at[span(self.last_at(piece, place, second), piece.last)],
                        self.firsts.at[distance - 1, span(piece.base // 8 + second * piece.last, piece.last)],
                        7 if turn == 0 else 1,
                        piece,
                        ring_peer(piece.first, distance),
                    )
            return
        if phase == 5:
            for distance in (1, 2, 3):
                self.spread_out(piece, lax.rem(two + distance, SIDE))
            return
        if phase == 6:
            for distance in (1, 2, 3):
                self.forward(piece, distance)
            return
        for distance in (2, 1, 3):
            slot = distance - 1
            if phase == 2:
                place = lax.rem(two + distance, SIDE)
                source = self.part.at[span(self.last_at(piece, one, place), piece.last)]
                target = self.seconds.at[slot, pl.ds(piece.base // 32, piece.last)]
                axis = piece.second
            elif phase == 3:
                source = self.part.at[span(self.last_at(piece, one, two), piece.last)]
                target = self.thirds.at[lax.axis_index(piece.third), pl.ds(piece.base // 32, piece.last)]
                axis = piece.third
            else:
                source = self.total.at[span(self.last_at(piece, one, two), piece.last)]
                target, axis = source, piece.second
            self.send_to(source, target, phase, piece, ring_peer(axis, distance))
        if phase == 4:
            self.spread_out(piece, two)

    def finish(self, phase, piece):
        sent = {0: piece.half, 1: 12 * piece.last, 4: 7 * piece.last, 5: 12 * piece.last, 6: 3 * piece.quarter}
        got_rows = {0: piece.half, 1: 9 * piece.last, 5: 3 * piece.quarter, 6: piece.half}
        self.sent(piece, sent.get(phase, 3 * piece.last))
        self.received(phase, piece, got_rows.get(phase, 3 * piece.last))
        one, two = lax.axis_index(piece.first), lax.axis_index(piece.second)
        if phase == 0:
            here = span(self.half_at(piece, self.core), piece.half)
            self.part[here] = self.part[here] + self.halves[pl.ds(piece.base // 2, piece.half)]
        elif phase == 1:
            for turn in (1, 2, 3):
                self.add_firsts(piece, lax.rem(two + turn, SIDE))
        elif phase == 2:
            self.received(7, piece, 3 * piece.last)
            self.add_firsts(piece, two)
            here = span(self.last_at(piece, one, two), piece.last)
            there = pl.ds(piece.base // 32, piece.last)
            got = self.seconds
            self.part[here] = (self.part[here] + got[0, there]) + (got[1, there] + got[2, there])
        elif phase == 3:
            here = span(self.last_at(piece, one, two), piece.last)
            there = pl.ds(piece.base // 32, piece.last)
            got = self.thirds
            got[lax.axis_index(piece.third), there] = self.part[here]
            self.total[here] = (got[0, there] + got[1, there]) + (got[2, there] + got[3, there])

    def add_firsts(self, piece, second):
        here = span(self.last_at(piece, lax.axis_index(piece.first), second), piece.last)
        there = span(piece.base // 8 + second * piece.last, piece.last)
        got = self.firsts
        self.part[here] = (self.part[here] + got[0, there]) + (got[1, there] + got[2, there])

    def step(self, phase, piece):
        self.finish(phase, piece)
        self.start(phase + 1, piece)


def pair_peer(first, second, size, distance):
    other = lax.rem(lax.axis_index(first) * SIDE + lax.axis_index(second) + distance, size)
    return {first: lax.div(other, SIDE), second: lax.rem(other, SIDE)}


class Statistics:
    def __init__(self, tiles, wide, plane, send, recv):
        self.tiles, self.slots = tiles, (wide, plane)
        self.axes = ((CORE, AXES[2]), (AXES[0], AXES[1]))
        self.send, self.recv = send, recv

    def mine(self, stage):
        first, second = self.axes[stage]
        return lax.axis_index(first) * SIDE + lax.axis_index(second)

    def start(self, stage):
        size = self.slots[stage].shape[0]
        for distance in range(1, size):
            pltpu.make_async_remote_copy(
                src_ref=self.tiles.at[stage],
                dst_ref=self.slots[stage].at[self.mine(stage)],
                send_sem=self.send.at[0],
                recv_sem=self.recv.at[stage],
                device_id=pair_peer(*self.axes[stage], size, distance),
                device_id_type=MESH,
            ).start()

    def finish(self, stage):
        slots = self.slots[stage]
        several = slots.at[pl.ds(0, slots.shape[0] - 1)]
        pltpu.make_async_copy(several, several, self.send.at[0]).wait()
        pltpu.make_async_copy(several, several, self.recv.at[stage]).wait()
        slots[self.mine(stage)] = self.tiles[stage]
        total = slots[0]
        for place in range(1, slots.shape[0]):
            total = total + slots[place]
        self.tiles[stage + 1] = total


class GateExchange:
    def __init__(self, base, rows, part, total, inward, rings, send, recv):
        self.base, self.share = base, rows // 8
        self.part, self.total = part, total
        self.inward, self.rings = inward, rings
        self.send, self.recv = send, recv
        self.group = lax.axis_index(CORE) * SIDE + lax.axis_index(AXES[0])

    def chunk(self, place):
        return span(self.base + place * self.share, self.share)

    def start(self, stage):
        mine = self.chunk(self.group)
        for distance in range(1, SIDE if stage in (1, 2) else 8):
            if stage in (1, 2):
                device = ring_peer(AXES[stage], distance)
                source, target = self.part.at[mine], self.rings.at[stage - 1, lax.axis_index(AXES[stage])]
            else:
                other = lax.rem(self.group + distance, 8)
                device = {CORE: lax.div(other, SIDE), AXES[0]: lax.rem(other, SIDE)}
                if stage == 0:
                    source, target = self.part.at[self.chunk(other)], self.inward.at[distance - 1]
                else:
                    source = self.total.at[mine]
                    target = source
            pltpu.make_async_remote_copy(
                src_ref=source,
                dst_ref=target,
                send_sem=self.send.at[3],
                recv_sem=self.recv.at[stage],
                device_id=device,
                device_id_type=MESH,
            ).start()

    def finish(self, stage):
        several = self.inward.at[pl.ds(0, 3 if stage in (1, 2) else 7)]
        pltpu.make_async_copy(several, several, self.send.at[3]).wait()
        pltpu.make_async_copy(several, several, self.recv.at[stage]).wait()
        mine = self.chunk(self.group)
        if stage == 0:
            value = self.part[mine]
            for slot in range(7):
                value = value + self.inward[slot]
            self.part[mine] = value
        elif stage < 3:
            self.rings[stage - 1, lax.axis_index(AXES[stage])] = self.part[mine]
            value = self.rings[stage - 1, 0]
            for slot in range(1, SIDE):
                value = value + self.rings[stage - 1, slot]
            if stage == 1:
                self.part[mine] = value
            else:
                self.total[mine] = value

    def step(self, stage):
        self.finish(stage)
        self.start(stage + 1)


def peers():
    core = lax.axis_index(CORE)
    found = [{CORE: 1 - core}]
    for distance in (1, 2, 3):
        for axis in (AXES[0], AXES[2]):
            found.append({CORE: 1 - core, **ring_peer(axis, distance)})
        found.append(ring_peer(AXES[2], distance))
    found += [pair_peer(AXES[0], AXES[1], 16, distance) for distance in range(1, 16)]
    return found


def kernel(
    sizes,
    ids_hbm, tokens_hbm, frozen_hbm, down_hbm, up_hbm, gate_hbm, upstream_hbm,
    projected_ref, input_ref, total, tiles,
    ids, tokens, frozen, sides, masked, grads, up, gate,
    both, low, prob, plain, turned, weighted, grads_t, weighted_t, gate_t,
    part, halves, firsts, seconds, thirds, wide, plane, inward, rings,
    load_sem, token_sem, send, recv, stat_send, stat_recv, gate_recv,
):
    rows, width, outputs, ranks, experts = sizes
    rank = ranks // experts
    scale = 1.0 / rank
    chunks = rows // CHUNK
    up_base = width
    gate_base = width + outputs
    pieces = (Piece(0, 0, 1792), Piece(1, 1792, 1792), Piece(2, 3584, gate_base - 3584))
    exchange = Exchange(part, total, halves, firsts, seconds, thirds, send, recv)
    statistics = Statistics(tiles, wide, plane, stat_send, stat_recv)
    gates = GateExchange(gate_base, width * experts // LANES, part, total, inward, rings, send, gate_recv)

    gate_load = pltpu.make_async_copy(gate_hbm, gate, load_sem.at[0])
    ids_load = pltpu.make_async_copy(ids_hbm, ids, load_sem.at[1])
    gate_load.start()
    ids_load.start()
    def load(source, target, slot):
        return pltpu.make_async_copy(source, target, load_sem.at[slot])

    def chunk_load(chunk):
        here = span(chunk * CHUNK, CHUNK, CHUNK)
        return (
            pltpu.make_async_copy(tokens_hbm.at[here], tokens.at[here], token_sem.at[chunk, 0]),
            pltpu.make_async_copy(upstream_hbm.at[here], masked.at[here], token_sem.at[chunk, 1]),
        )

    down_load = load(down_hbm, sides.at[:, pl.ds(0, ranks)], 2)
    up_load = load(up_hbm, up, 3)
    frozen_load = load(frozen_hbm, frozen, 4)
    down_load.start()
    chunk_load(0)[0].start()
    up_load.start()
    chunk_load(0)[1].start()
    barrier = pltpu.get_barrier_semaphore()
    greeted = peers()
    for peer in greeted:
        pl.semaphore_signal(barrier, inc=1, device_id=peer, device_id_type=MESH)

    gate_load.wait()
    for copy in chunk_load(1):
        copy.start()

    @pl.loop(0, width // 512)
    def _(block):
        here = span(block * 512, 512, 512)
        row = gate[:, here].astype(F32)
        tall = jnp.concatenate([jnp.broadcast_to(row[e : e + 1], (rank, 512)) for e in range(experts)], axis=0)
        sides[here, ranks : 2 * ranks] = tall.T.astype(BF16)

    ids_load.wait()
    live_rows = jnp.sum(jnp.sum((ids[...] != 0).astype(F32), axis=1, keepdims=True), axis=0, keepdims=True)

    def live_of(chunk):
        row = lax.broadcasted_iota(jnp.int32, (CHUNK, LANES), 0) + chunk * CHUNK
        return (row.astype(F32) < live_rows).astype(F32)

    def lane_sum(value):
        return jnp.sum(value, axis=1, keepdims=True)

    tiles[0] = jnp.zeros((8, LANES), F32)
    down_load.wait()

    def spread(chunk):
        here = span(chunk * CHUNK, CHUNK, CHUNK)
        slot = chunk % 2
        below = both[slot, :, :ranks].astype(BF16)
        logits = both[slot, :, ranks:]
        shifted = logits - jnp.max(logits, axis=1, keepdims=True)
        raised = jnp.exp(shifted)
        mass = lane_sum(raised) * scale
        share = raised / mass
        logp = shifted - jnp.log(mass)
        entropy = -lane_sum(share * logp) * scale
        alive = live_of(chunk)
        low[here] = below
        prob[here] = share
        plain[here] = 50.0 * alive * share * (logp + entropy)
        tiles[0, 0:1] += jnp.sum(alive * share, axis=0, keepdims=True)
        tiles[0, 1:2] += jnp.sum(alive * entropy, axis=0, keepdims=True)
        tiles[0, 2:3] += jnp.sum(alive, axis=0, keepdims=True)
        mine = jnp.where(alive[:, 0:1] > 0.0, masked[here].astype(F32), 0.0).astype(BF16)
        masked[here] = mine
        back = right_dot(mine, up[...])
        heavy = (below.astype(F32) * share).astype(BF16).astype(F32) * 2.0
        steep = (2.0 * share * back).astype(BF16)
        turned[here] = back
        weighted[here] = heavy.astype(BF16)
        grads[here, 0:ranks] = steep
        grads_t[:, here] = steep.astype(F32).T.astype(BF16)
        weighted_t[:, here] = heavy.T.astype(BF16)

    for copy in chunk_load(2):
        copy.start()
    chunk_load(0)[0].wait()
    for copy in chunk_load(3):
        copy.start()
    both[0] = dot(tokens[0:CHUNK], sides[...])
    up_load.wait()

    @pl.loop(1, chunks)
    def _(chunk):
        chunk_load(chunk - 1)[1].wait()
        chunk_load(chunk)[0].wait()
        spread(chunk - 1)
        both[chunk % 2] = dot(tokens[span(chunk * CHUNK, CHUNK, CHUNK)], sides[...])

    frozen_load.start()
    chunk_load(chunks - 1)[1].wait()
    spread(chunks - 1)
    pl.semaphore_wait(barrier, len(greeted))
    statistics.start(0)

    def down_block(start, size):
        found = dot(grads_t[...], tokens[:, pl.ds(start, size)])
        for block in range(size // LANES):
            here = start + block * LANES
            part[here : here + LANES] = found[:, block * LANES : (block + 1) * LANES]

    down_block(0, 1792)
    exchange.start(0, pieces[0])
    down_block(1792, 1792)
    exchange.start(0, pieces[1])
    down_block(3584, 512)
    found = dot(weighted_t[...], masked[...])
    for block in range(outputs // LANES):
        part[up_base + block * LANES : up_base + (block + 1) * LANES] = found[:, block * LANES : (block + 1) * LANES]
    exchange.start(0, pieces[2])
    group = lax.broadcasted_iota(jnp.int32, (2 * ranks, ranks), 0) % ranks // rank
    member = lax.broadcasted_iota(jnp.int32, (2 * ranks, ranks), 1) // rank
    blocks = (group == member).astype(F32).astype(BF16)

    def task_part(chunk):
        here = span(chunk * CHUNK, CHUNK, CHUNK)
        share = prob[here]
        product = low[here].astype(F32) * turned[here]
        upper = product.astype(BF16)
        lower = (product - upper.astype(F32)).astype(BF16)
        task = 2.0 * dot(jnp.concatenate([upper, lower], axis=1), blocks)
        plain[here] += share * (task - lane_sum(share * task) * scale)

    task_part(0)
    task_part(1)
    statistics.finish(0)
    statistics.start(1)
    exchange.step(0, pieces[0])
    task_part(2)
    exchange.step(0, pieces[1])
    task_part(3)
    exchange.step(0, pieces[2])
    lane = lax.broadcasted_iota(jnp.int32, (CHUNK, LANES), 1)
    pick_from = lax.broadcasted_iota(jnp.int32, (ranks, ranks), 0)
    pick_to = lax.broadcasted_iota(jnp.int32, (ranks, ranks), 1)
    pick = (pick_from == (pick_to % experts) * rank + pick_to // experts).astype(F32)
    pick = jnp.where(pick_to < 2 * experts, pick, 0.0).astype(BF16)

    def slope_part(chunk):
        load_all, live_all = tiles[2, 0:1], tiles[2, 2:3]
        push = (2.0 * experts * 100.0) / live_all
        here = span(chunk * CHUNK, CHUNK, CHUNK)
        share = prob[here]
        slope = share * (load_all - lane_sum(share * load_all) * scale)
        whole = plain[here] + push * live_of(chunk) * slope
        upper = whole.astype(BF16).astype(F32)
        place = lane % rank
        packed = jnp.where(place == 0, upper, jnp.where(place == 1, whole - upper, 0.0)).astype(BF16)
        grads[here, ranks : 2 * ranks] = packed
        gate_t[:, here] = dot(packed, pick).T[: 2 * experts].astype(BF16)

    def base_block(block):
        tall = span((block % 2) * (rows // 2), rows // 2, rows // 2)
        here = span((block // 2) * 256, 256, 256)
        found = dot(tokens[tall], frozen[:, here]) + dot(weighted[tall], up[:, here])
        projected_ref[tall, here] = found.astype(BF16)

    def step_all(phase):
        for piece in pieces[:3]:
            exchange.step(phase, piece)

    def at(block, place):
        return pl.when(block == place)

    frozen_load.wait()

    first = pl.ds(0, 256)
    found = dot(tokens[...], frozen[:, first]) + dot(weighted[...], up[:, first])
    projected_ref[:, first] = found.astype(BF16)
    base_block(2)

    statistics.finish(1)

    @pl.loop(3, 5)
    def _(block):
        slope_part(2 * block - 6)
        slope_part(2 * block - 5)
        base_block(block)

    for piece in pieces:
        exchange.step(1, piece)

    @pl.loop(0, width // 2048)
    def _(block):
        found = dot(gate_t[...], tokens[:, span(block * 2048, 2048, 2048)])
        found = found[:experts] + found[experts:]
        for piece in range(16):
            here = span(gate_base + (block * 16 + piece) * experts, experts)
            part[here] = found[:, piece * LANES : (piece + 1) * LANES]

    gates.start(0)

    @pl.loop(5, 8)
    def _(block):
        @at(block, 6)
        def _():
            exchange.step(2, pieces[0])

        @at(block, 7)
        def _():
            exchange.step(2, pieces[1])
            exchange.step(2, pieces[2])

        base_block(block)

    def input_block(block):
        here = span(block * 512, 512, 512)
        found = right_dot(masked[...], frozen[here]) + right_dot(grads[...], sides[here])
        input_ref[:, here] = found.astype(BF16)

    @pl.loop(0, input_ref.shape[1] // 512 - 1)
    def _(block):
        @at(block, 0)
        def _():
            gates.step(0)

        @at(block, 1)
        def _():
            exchange.step(3, pieces[0])

        @at(block, 2)
        def _():
            exchange.step(3, pieces[1])
            exchange.step(3, pieces[2])
            gates.step(1)

        @at(block, 3)
        def _():
            exchange.step(4, pieces[0])

        @at(block, 4)
        def _():
            exchange.step(4, pieces[1])
            exchange.step(4, pieces[2])

        @at(block, 5)
        def _():
            gates.step(2)

        @at(block, 6)
        def _():
            exchange.step(5, pieces[0])

        input_block(block)

    exchange.step(5, pieces[1])
    exchange.step(5, pieces[2])
    input_block(input_ref.shape[1] // 512 - 1)
    gates.finish(3)
    for piece in pieces:
        exchange.finish(6, piece)


def finish_kernel(
    sizes,
    projected, inputs, total, tiles,
    projected_hbm, input_hbm, down_hbm, up_hbm, gate_hbm, load_hbm, entropy_hbm,
    scaled, up, gate, load, entropy, sems,
):
    width, outputs, ranks, experts = sizes
    rank = ranks // experts
    every = total.shape[0]
    copies = []

    def send(source, target):
        copy = pltpu.make_async_copy(source, target, sems.at[len(copies)])
        copy.start()
        copies.append(copy)

    tall = inputs.shape[0] // 4
    for block in range(4):
        here = pl.ds(block * tall, tall)
        send(inputs.at[here], input_hbm.at[here])
    send(projected, projected_hbm)

    def add_squares(block, found):
        value = total[span(block * 192, 192)]
        return found + jnp.sum((value * value).reshape(6, 32, LANES), axis=0)

    squares = lax.fori_loop(0, every // 192, add_squares, jnp.zeros((32, LANES), F32))
    norm = jnp.sqrt(jnp.sum(jnp.sum(squares, axis=1, keepdims=True), axis=0, keepdims=True))
    mean = tiles[2] / tiles[2, 2:3]
    lane = lax.broadcasted_iota(jnp.int32, (1, LANES), 1)
    for expert in range(experts):
        load[expert] = jnp.sum(jnp.where(lane == expert * rank, mean[0:1], 0.0))
    entropy[0] = jnp.sum(jnp.where(lane == 0, mean[1:2], 0.0))
    send(load, load_hbm)
    send(entropy, entropy_hbm)

    factor = jnp.minimum(1.0, math.sqrt(every * LANES) / norm)
    for block in range(width // LANES):
        here = pl.ds(block * LANES, LANES)
        scaled[here] = (total[here] * factor).T
    for block in range(outputs // LANES):
        here = width + block * LANES
        up[:, block * LANES : (block + 1) * LANES] = total[here : here + LANES] * factor
    for block in range(width // LANES):
        here = width + outputs + block * experts
        gate[:, block * LANES : (block + 1) * LANES] = total[here : here + experts] * factor
    send(scaled, down_hbm)
    send(up, up_hbm)
    send(gate, gate_hbm)
    for copy in copies:
        copy.wait()


def on_device(token_ids, tokens, frozen_weight, adapter_down, adapter_up, gate_weight, upstream):
    rows, width = tokens.shape
    ranks, outputs = adapter_up.shape
    experts = gate_weight.shape[1]
    every = width + outputs + width * experts // LANES
    anywhere = pl.BlockSpec(memory_space=pl.ANY)
    hbm = pl.BlockSpec(memory_space=pltpu.HBM)
    vmem = pl.BlockSpec(memory_space=pltpu.VMEM)
    held = pl.pallas_call(
        functools.partial(kernel, (rows, width, outputs, ranks, experts)),
        out_shape=(
            pltpu.VMEM((rows, outputs), BF16),
            pltpu.VMEM((rows, width), BF16),
            pltpu.VMEM((every, LANES), F32),
            pltpu.VMEM((3, 8, LANES), F32),
        ),
        in_specs=[hbm] * 7,
        out_specs=(vmem,) * 4,
        scratch_shapes=[
            pltpu.VMEM((rows // LANES, LANES), jnp.int32),
            pltpu.VMEM((rows, width), BF16),
            pltpu.VMEM((width, outputs), BF16),
            pltpu.VMEM((width, 2 * ranks), BF16),
            pltpu.VMEM((rows, outputs), BF16),
            pltpu.VMEM((rows, 2 * ranks), BF16),
            pltpu.VMEM((ranks, outputs), BF16),
            pltpu.VMEM((experts, width), BF16),
            pltpu.VMEM((2, CHUNK, 2 * ranks), F32),
            pltpu.VMEM((rows, ranks), BF16),
            pltpu.VMEM((rows, ranks), F32),
            pltpu.VMEM((rows, ranks), F32),
            pltpu.VMEM((rows, ranks), F32),
            pltpu.VMEM((rows, ranks), BF16),
            pltpu.VMEM((ranks, rows), BF16),
            pltpu.VMEM((ranks, rows), BF16),
            pltpu.VMEM((2 * experts, rows), BF16),
            pltpu.VMEM((every, LANES), F32),
            pltpu.VMEM((every // 2, LANES), F32),
            pltpu.VMEM((3, every // 8, LANES), F32),
            pltpu.VMEM((3, every // 32, LANES), F32),
            pltpu.VMEM((4, every // 32, LANES), F32),
            pltpu.VMEM((8, 8, LANES), F32),
            pltpu.VMEM((16, 8, LANES), F32),
            pltpu.VMEM((7, width * experts // LANES // 8, LANES), F32),
            pltpu.VMEM((2, SIDE, width * experts // LANES // 8, LANES), F32),
            pltpu.SemaphoreType.DMA((5,)),
            pltpu.SemaphoreType.DMA((rows // CHUNK, 2)),
            pltpu.SemaphoreType.DMA((4,)),
            pltpu.SemaphoreType.DMA((8, 3)),
            pltpu.SemaphoreType.DMA((1,)),
            pltpu.SemaphoreType.DMA((2,)),
            pltpu.SemaphoreType.DMA((4,)),
        ],
        compiler_params=pltpu.CompilerParams(
            collective_id=0, has_side_effects=True, vmem_limit_bytes=46 * 1024 * 1024
        ),
        name="step",
    )(token_ids.reshape(rows // LANES, LANES), tokens, frozen_weight, adapter_down, adapter_up, gate_weight.T, upstream)
    projected, input_grad, down, up, gate, load, entropy = pl.pallas_call(
        functools.partial(finish_kernel, (width, outputs, ranks, experts)),
        out_shape=(
            jax.ShapeDtypeStruct((rows, outputs), BF16),
            jax.ShapeDtypeStruct((rows, width), BF16),
            jax.ShapeDtypeStruct((width, ranks), F32),
            jax.ShapeDtypeStruct((ranks, outputs), F32),
            jax.ShapeDtypeStruct((experts, width), F32),
            jax.ShapeDtypeStruct((experts,), F32),
            jax.ShapeDtypeStruct((1,), F32),
        ),
        in_specs=[vmem] * 4,
        out_specs=(anywhere,) * 7,
        scratch_shapes=[
            pltpu.VMEM((width, ranks), F32),
            pltpu.VMEM((ranks, outputs), F32),
            pltpu.VMEM((experts, width), F32),
            pltpu.SMEM((experts,), F32),
            pltpu.SMEM((1,), F32),
            pltpu.SemaphoreType.DMA((10,)),
        ],
        compiler_params=pltpu.CompilerParams(vmem_limit_bytes=12 * 1024 * 1024),
        name="finish",
    )(*held)
    return projected, input_grad, down, up, gate.T, load, entropy.reshape(())


def solution(mesh):
    torus = Mesh(mesh.devices.reshape(4, 4, 4, 2), DP)
    return jax.shard_map(
        on_device,
        mesh=torus,
        in_specs=(P(DP), P(DP, None), P(), P(), P(), P(), P(DP, None)),
        out_specs=(P(DP, None), P(DP, None), P(), P(), P(), P(), P()),
        check_vma=False,
    )
```
